32 devices in a mesh: replica: 16 (over z, x, core), spatial: 2 (over y).
Axes of the slice: x: 2, y: 2, z: 4, core: 2. Of those that a mesh axis runs over, the one named last changes fastest.
Arguments:
- grads: bfloat16 [16, 2, 852992], P('replica', 'spatial'), may hold values from -6 to 6
- master: float32 [852992], P(('replica', 'spatial')), may hold values from -0.06 to 0.06
- velocity: float32 [852992], P(('replica', 'spatial')), may hold values from -0.3 to 0.3
- layer_offsets: int32 [6], replicated, may hold values from 0 to 852736, as said below
- layer_sizes: int32 [6], replicated, may hold values from 256 to 589824
- lars_skip: int32 [6], replicated, may hold values from 0 to 1
Outputs:
- new_weights: bfloat16 [852992], replicated
- new_master: float32 [852992], P(('replica', 'spatial'))
- new_velocity: float32 [852992], P(('replica', 'spatial'))
The draws below stay inside these ranges and needn't reach their ends.
Inputs may be any that keep to these rules, and one draw needn't show every extreme that they name: layer_offsets, layer_sizes and lars_skip describe the six tensors (a 256 x 1024 convolution, a 256 x 256 x 9 convolution, and two gains and two shifts of 256 entries) laid end to end in some order without gaps, the last of them always a gain or a shift; lars_skip is 1 exactly for the gains and shifts.
All inputs are finite; a program needn't handle non-finite values.
Results may differ from the reference program's by a relative error of at most 0.001.
Values may be sent and summed in bfloat16 or wider, within the bound.
A program may use at most 64 MiB of HBM per device.

```python
import jax
import jax.numpy as jnp
from jax import lax

CIN = 1024
MID = 256
KSQ = 9
LAYERS = 6
PARAMS = 852992
N_REPLICA = 16
N_SPATIAL = 2


def layout_tables(key):
    scores = jax.random.permutation(jax.random.fold_in(key, 71), LAYERS).astype(jnp.int32)
    small_list = jnp.array([1, 2, 4, 5], jnp.int32)
    pick = jax.random.randint(jax.random.fold_in(key, 73), (), 0, 4)
    chosen = small_list[pick]
    scores = jnp.where(jnp.arange(LAYERS, dtype=jnp.int32) == chosen, LAYERS, scores)
    order = jnp.argsort(scores, stable=True)
    base_sizes = jnp.array([MID * CIN, MID, MID, MID * MID * KSQ, MID, MID], jnp.int32)
    base_skip = jnp.array([0, 1, 1, 0, 1, 1], jnp.int32)
    sizes = base_sizes[order]
    offsets = jnp.cumsum(sizes) - sizes
    return (offsets.astype(jnp.int32), sizes.astype(jnp.int32), base_skip[order])


def draw_layer_offsets(key, part):
    return layout_tables(key)[0]


def draw_layer_sizes(key, part):
    return layout_tables(key)[1]


def draw_lars_skip(key, part):
    return layout_tables(key)[2]


def raised(values, rng, source, target, blocks, factor):
    owner, partner = [(jnp.arange(values.shape[dim]) // (values.shape[dim] // blocks)).reshape([-1 if axis == dim else 1 for axis in range(values.ndim)]) for dim in (source, target)]
    chosen = jax.random.permutation(rng, blocks)[partner]
    strong = (owner == chosen) | (owner == (partner + blocks // 2) % blocks)
    return jnp.where(strong, factor * values, values)


def levels(stream_key, extent, split, smallest, high):
    loudness, own = 1.0, jax.random.fold_in(stream_key, 6)
    for axis_at, blocks in split:
        heights = jnp.exp(jax.random.uniform(jax.random.fold_in(own, axis_at), (blocks,), jnp.float32, smallest / len(split), high / len(split)))
        loudness = loudness * jnp.repeat(heights, extent[axis_at] // blocks).reshape([-1 if axis == axis_at else 1 for axis in range(len(extent))])
    return loudness


def gaussian(stream_key, extent, scale, limit, cuts=(), held_as=jnp.bfloat16):
    values = jax.random.normal(stream_key, extent, jnp.float32) * scale
    if len(cuts) > 0:
        values = levels(stream_key, extent, cuts, -0.22, 0.18) * values
    return jnp.clip(values, min=-limit, max=limit).astype(held_as)


def gaussian_with(key, shape, scale, bound, pieces, heavy, kind=jnp.bfloat16):
    values = scale * jax.random.normal(key, shape, jnp.float32)
    if pieces:
        values = values * levels(key, shape, pieces, -0.22, 0.18)
    return jnp.clip(raised(values, jax.random.fold_in(key, 3), *heavy), -bound, bound).astype(kind)


def setup_inputs(seed: int = 0) -> dict:
    keys = jax.random.split(jax.random.key(seed), 7)
    grads = gaussian_with(keys[0], (N_REPLICA, N_SPATIAL, PARAMS), 1.0, 6.0, ((0, 16), (1, 2)), (0, 2, 16, 2.0))
    master = jnp.clip(jax.random.uniform(keys[1], (PARAMS,), jnp.float32, -0.06, 0.06) * levels(keys[1], (PARAMS,), ((0, 32),), -0.4, 0.0), -0.06, 0.06)
    velocity = gaussian(keys[2], (PARAMS,), 0.05, 0.3, ((0, 32),), jnp.float32)
    layer_offsets = draw_layer_offsets(jax.random.fold_in(keys[6], 71), 0)
    layer_sizes = draw_layer_sizes(jax.random.fold_in(keys[6], 71), 0)
    lars_skip = draw_lars_skip(jax.random.fold_in(keys[6], 71), 0)
    return dict(grads=grads, master=master, velocity=velocity, layer_offsets=layer_offsets, layer_sizes=layer_sizes, lars_skip=lars_skip)


def reference(grads, master, velocity, layer_offsets, layer_sizes, lars_skip):
    grad = lax.optimization_barrier(jnp.sum(grads.astype(jnp.float32), axis=(0, 1))) / (N_REPLICA * N_SPATIAL)
    position = jnp.arange(PARAMS, dtype=jnp.int32)
    inside = (position[None, :] >= layer_offsets[:, None]) & (position[None, :] < (layer_offsets + layer_sizes)[:, None])
    onehot = inside.astype(jnp.float32)
    wsq = jnp.dot(onehot, master * master, precision=lax.Precision.HIGHEST)
    gsq = jnp.dot(onehot, grad * grad, precision=lax.Precision.HIGHEST)
    wnorm = jnp.sqrt(wsq)
    gnorm = jnp.sqrt(gsq)
    skipped = lars_skip.astype(jnp.float32)
    ratio = 0.02 * wnorm / (gnorm + 0.001 * wnorm + 1e-06)
    trust = skipped + (1.0 - skipped) * ratio
    decay = (1.0 - skipped) * 0.001
    trust_pos = jnp.dot(trust, onehot, precision=lax.Precision.HIGHEST)
    decay_pos = jnp.dot(decay, onehot, precision=lax.Precision.HIGHEST)
    new_velocity = 0.9 * velocity + 8.0 * trust_pos * (grad + decay_pos * master)
    new_master = master - new_velocity
    return (new_master.astype(jnp.bfloat16), new_master, new_velocity)
```

```python
import functools

import jax
import jax.numpy as jnp
from jax import lax
from jax.experimental import pallas as pl
from jax.experimental.pallas import tpu as pltpu
from jax.sharding import PartitionSpec as P

MESH = pl.DeviceIdType.MESH
TILE = 1024
AHEAD = 2


def flip(i, k):
    out, bit = 0, 1
    while bit <= k:
        b = (i // bit) % 2
        out = out + bit * (1 - 2 * b) * ((k // bit) % 2)
        bit *= 2
    return i + out


def kernel(
    plan,
    grads_ref,
    m_ref,
    v_ref,
    offsets_ref,
    sizes_ref,
    skip_ref,
    ags,
    nmw,
    nvw,
    m_in,
    v_in,
    gin,
    packed,
    r1x,
    r1y,
    sx,
    sy,
    r2x,
    r2y,
    part,
    recv3,
    mv,
    halo,
    grad_buf,
    wrow,
    stats,
    in_sem,
    mv_sem,
    ready,
    send1x,
    got1x,
    send1y,
    got1y,
    send2x,
    got2x,
    send2y,
    got2y,
    send3,
    got3,
    halo_sem,
    send_s,
    got_s,
    send4,
    got4,
):
    n_out, shard, step, span, layers = plan
    plane = 8
    n = n_out * plane
    chunk = (plane - 1) * step + span
    rows = span * 8
    hx = (span + 1) // 2
    hy = span - hx
    wx = step + 2 * hx - span
    gap = wx - hx
    r = lax.axis_index("replica")
    y = lax.axis_index("spatial")
    d = r * 2 + y
    z = d // plane
    p = d % plane
    x = p // 4
    c = (p // 2) % 2
    base = d * (step * TILE)
    off = d * (shard - step * TILE)

    def dev(flat):
        return (flat // 2, flat % 2)

    def at(zz, xx, cc, yy):
        return ((zz * 2 + xx) * 2 + cc, yy)

    barrier = pltpu.get_barrier_semaphore()

    def load(zt):
        start = pl.multiple_of(zt * (plane * step * TILE), TILE)
        return pltpu.make_async_copy(
            grads_ref.at[0, :, pl.ds(start, chunk * TILE)], gin.at[zt], in_sem.at[zt]
        )

    order = [(z + k) % n_out for k in range(1, n_out + 1)]
    for zt in order:
        load(zt).start()
    mv_loads = [
        pltpu.make_async_copy(ref, buf, mv_sem.at[j])
        for j, (ref, buf) in enumerate(((m_ref, m_in), (v_ref, v_in)))
    ]
    for copy in mv_loads:
        copy.start()

    def signal(sem, device):
        pl.semaphore_signal(sem, inc=1, device_id=device, device_id_type=MESH)

    def signal_z(sem):
        @pl.when(z > 0)
        def _():
            signal(sem, at(z - 1, x, c, y))

        @pl.when(z < n_out - 1)
        def _():
            signal(sem, at(z + 1, x, c, y))

    n_z = jnp.where(z > 0, 1, 0) + jnp.where(z < n_out - 1, 1, 0)
    for device in (
        at(z, x, 1 - c, y),
        at(z, 1 - x, c, y),
        at(z, x, c, 1 - y),
        at(z, 1 - x, 1 - c, y),
        at(z, x, 1 - c, 1 - y),
    ):
        signal(barrier, device)
    signal_z(barrier)

    group = max(g for g in range(1, 33) if chunk % g == 0)

    def pack(zt):
        load(zt).wait()

        @pl.loop(0, chunk // group)
        def _(i):
            first = pl.multiple_of(i * (group * TILE), group * TILE)
            v = gin[zt, :, pl.ds(first, group * TILE)].astype(jnp.float32)
            packed[zt, pl.ds(i * group, group)] = v.reshape(group, 8, 128).astype(jnp.bfloat16)

    def remote(src, dst, send, recv, device):
        return pltpu.make_async_remote_copy(
            src_ref=src,
            dst_ref=dst,
            send_sem=send,
            recv_sem=recv,
            device_id=device,
            device_id_type=MESH,
        )

    def landed(ref, sem):
        pltpu.make_async_copy(ref, ref, sem).wait()

    def first_x(xx, cc):
        return (xx * 2 + cc) * (2 * step) + span - hx

    def first_y(xx, cc, yy):
        return (xx * 4 + cc * 2 + yy) * step + yy * hx

    def send_raw(zt):
        for m in (3, 2, 1):
            xx, cc = (1 - x if m >= 2 else x), (1 - c if m % 2 else c)
            remote(
                packed.at[zt, pl.ds(first_x(xx, cc), wx)],
                r1x.at[zt, m - 1],
                send1x,
                got1x.at[zt],
                at(z, xx, cc, y),
            ).start()
            yy = 1 - y if m >= 2 else y
            for xb in range(2):
                remote(
                    packed.at[zt, pl.ds(first_y(xb, cc, yy), hy)],
                    r1y.at[zt, m - 1, xb],
                    send1y,
                    got1y.at[zt],
                    at(z, x, cc, yy),
                ).start()

    def sum_raw(zt):
        landed(r1x.at[zt], got1x.at[zt])
        own = first_x(x, c)

        @pl.loop(0, wx, unroll=3)
        def _(t):
            acc = packed[zt, own + t].astype(jnp.float32) + r1x[zt, 0, t].astype(jnp.float32)
            rest = r1x[zt, 1, t].astype(jnp.float32) + r1x[zt, 2, t].astype(jnp.float32)
            sx[zt, t] = acc + rest

        remote(
            sx.at[zt, pl.ds((1 - y) * gap, hx)],
            r2x.at[zt],
            send2x,
            got2x.at[zt],
            at(z, x, c, 1 - y),
        ).start()
        landed(r1y.at[zt], got1y.at[zt])
        for xb in range(2):
            own = first_y(xb, c, y)

            @pl.loop(0, hy, unroll=3)
            def _(t):
                acc = packed[zt, own + t].astype(jnp.float32)
                acc = acc + r1y[zt, 0, xb, t].astype(jnp.float32)
                rest = r1y[zt, 1, xb, t].astype(jnp.float32)
                rest = rest + r1y[zt, 2, xb, t].astype(jnp.float32)
                sy[zt, xb, t] = acc + rest

        remote(
            sy.at[zt, 1 - x],
            r2y.at[zt],
            send2y,
            got2y.at[zt],
            at(z, 1 - x, c, y),
        ).start()

    def copy3(zt, src):
        return remote(part.at[zt], recv3.at[src], send3, got3, at(zt, x, c, y))

    def sum_plane(zt):
        landed(r2x.at[zt], got2x.at[zt])

        @pl.loop(0, hx, unroll=2)
        def _(t):
            part[zt, (1 - y) * hy + t] = sx[zt, y * gap + t] + r2x[zt, t]

        landed(r2y.at[zt], got2y.at[zt])

        @pl.loop(0, hy, unroll=2)
        def _(t):
            part[zt, y * hx + t] = sy[zt, x, t] + r2y[zt, t]

    pack(order[0])
    pl.semaphore_wait(barrier, 5 + n_z)
    send_raw(order[0])
    signal_z(ready.at[0])
    for k in range(1, n_out):
        pack(order[k])
        if k < AHEAD:
            send_raw(order[k])
    for i in range(n_out - 2):
        pl.semaphore_wait(ready.at[i], n_z)
        if i < n_out - 3:
            signal_z(ready.at[i + 1])

    lane = lax.broadcasted_iota(jnp.int32, (rows, 128), 1)
    shift_l = off % 128
    shift_r = off // 128
    whole = step * TILE
    for j, ref in enumerate((m_in, v_in)):
        mv_loads[j].wait()
        edge = jnp.pad(ref[pl.ds(whole, shard - whole)], (0, 128 - (shard - whole)))
        edge = jnp.broadcast_to(edge.reshape(1, 128), (8, 128))
        w = jnp.concatenate([ref[pl.ds(0, whole)].reshape(step * 8, 128), edge], 0)
        w = pltpu.roll(w, shift_l, 1)
        w = jnp.where(lane < shift_l, pltpu.roll(w, 1, 0), w)
        w = pltpu.roll(w, shift_r, 0)
        mv[:, j] = w.reshape(span, 8, 128)

    place = lax.broadcasted_iota(jnp.int32, (8, 128), 0) * 128 + lax.broadcasted_iota(
        jnp.int32, (8, 128), 1
    )
    low = [offsets_ref[l] - base for l in range(layers)]
    high = [offsets_ref[l] + sizes_ref[l] - base for l in range(layers)]
    own_low = [jnp.maximum(v, off) for v in low]
    own_high = [jnp.minimum(v, off + shard) for v in high]
    lane1 = lax.broadcasted_iota(jnp.int32, (1, 128), 1)

    def squares(value, first):
        def add(t, accs):
            pos = place + t * TILE
            v = value(t)
            v = v * v
            return tuple(
                acc + jnp.where((pos >= lo) & (pos < hi), v, 0.0)
                for acc, lo, hi in zip(accs, own_low, own_high)
            )

        accs = lax.fori_loop(
            0, span, add, tuple(jnp.zeros((8, 128), jnp.float32) for _ in range(layers))
        )
        row = jnp.zeros((1, 128), jnp.float32)
        for l, acc in enumerate(accs):
            row = jnp.where(lane1 == first + l, jnp.sum(acc, axis=(0, 1), keepdims=True), row)
        return row

    wrow[...] = squares(lambda t: mv[t, 0], 0)

    for k in range(n_out):
        sum_raw(order[k])
        if k + AHEAD < n_out:
            send_raw(order[k + AHEAD])
        if k > 0:
            sum_plane(order[k - 1])
            copy3(order[k - 1], z).start()
    sum_plane(z)

    landed(recv3.at[pl.ds(0, n_out - 1)], got3)

    @pl.loop(0, span)
    def _(t):
        acc = part[z, t]
        for k in range(1, n_out):
            acc = acc + recv3[(z + k) % n_out, t]
        grad_buf[t] = acc / n

    stats[d] = squares(lambda t: grad_buf[t], layers) + wrow[...]

    @pl.loop(1, n, unroll=True)
    def _(q):
        remote(stats.at[d], stats.at[d], send_s, got_s, dev((d + q) % n)).start()

    halo_copy = remote(mv.at[span - 1], halo, halo_sem.at[0], halo_sem.at[1], dev((d + 1) % n))
    halo_copy.start()

    landed(stats.at[pl.ds(0, n - 1)], got_s)
    total = jnp.sum(stats[...], axis=0)
    trust, decay = [], []
    for l in range(layers):
        wsq = jnp.sum(jnp.where(lane1 == l, total, 0.0), axis=(0, 1), keepdims=True)
        gsq = jnp.sum(jnp.where(lane1 == layers + l, total, 0.0), axis=(0, 1), keepdims=True)
        wnorm = jnp.sqrt(jnp.broadcast_to(wsq, (8, 128)))
        gnorm = jnp.sqrt(jnp.broadcast_to(gsq, (8, 128)))
        skipped = skip_ref[l].astype(jnp.float32)
        ratio = 0.02 * wnorm / (gnorm + 0.001 * wnorm + 1e-06)
        trust.append(skipped + (1.0 - skipped) * ratio)
        decay.append((1.0 - skipped) * 0.001)

    halo_copy.wait()
    for j in range(2):
        mv[0, j] = jnp.where(place < off, halo[j], mv[0, j])

    @pl.loop(0, span)
    def _(t):
        pos = place + t * TILE
        trust_pos = jnp.zeros((8, 128), jnp.float32)
        decay_pos = jnp.zeros((8, 128), jnp.float32)
        for l in range(layers):
            inside = (pos >= low[l]) & (pos < high[l])
            trust_pos = jnp.where(inside, trust[l], trust_pos)
            decay_pos = jnp.where(inside, decay[l], decay_pos)
        m = mv[t, 0]
        nv = 0.9 * mv[t, 1] + 8.0 * trust_pos * (grad_buf[t] + decay_pos * m)
        nm = m - nv
        nvw[t] = nv
        nmw[t] = nm
        ags[d, t] = nm.astype(jnp.bfloat16)

    def block(zz, xx, cc, yy):
        return zz * plane + xx * 4 + cc * 2 + yy

    def forward(b, device, lo=0, size=span):
        piece = ags.at[b, pl.ds(lo, size)]
        remote(piece, piece, send4, got4.at[b], device).start()

    def arrived(b):
        landed(ags.at[b], got4.at[b])

    x_side = at(z, 1 - x, c, y)
    y_side = at(z, x, c, 1 - y)
    partner = at(z, x, 1 - c, y)
    for k in range(1, n_out):
        forward(d, at(flip(z, k), x, c, y))

    def column(k):
        b = block(flip(z, k), x, c, y)
        if k > 0:
            arrived(b)
        forward(b, x_side)
        forward(b, y_side)
        forward(b, partner)

    column(0)
    for k in range(n_out):
        zz = flip(z, k)
        if k + 1 < n_out:
            column(k + 1)
        b = block(zz, x, c, 1 - y)
        arrived(b)
        forward(b, x_side, 0, hx)
        forward(b, partner)
        b = block(zz, 1 - x, c, y)
        arrived(b)
        forward(b, y_side, hx, hy)
        forward(b, partner)
        if k > 0:
            b = block(flip(z, k - 1), 1 - x, c, 1 - y)
            arrived(b)
            forward(b, partner)
    b = block(flip(z, n_out - 1), 1 - x, c, 1 - y)
    arrived(b)
    forward(b, partner)

    @pl.loop(0, n_out)
    def _(k):
        for xx in range(2):
            for yy in range(2):
                arrived(block(k, xx, 1 - c, yy))

    for ref, sem in (
        (r1x, send1x),
        (r1y, send1y),
        (r2x, send2x),
        (r2y, send2y),
        (recv3.at[pl.ds(0, n_out - 1)], send3),
        (stats.at[pl.ds(0, n - 1)], send_s),
        (ags.at[pl.ds(0, n - 1)], send4),
    ):
        landed(ref, sem)


def finish(plan, ags, nmw, nvw, out_ref, nm_ref, nv_ref, nm_out, nv_out, out_sem, own_sem):
    n, n_spa, shard, step, span = plan
    rows = span * 8
    whole = step * TILE
    copies = [
        pltpu.make_async_copy(
            ags.at[b, pl.ds(0, step)], out_ref.at[pl.ds(b * step, step)], out_sem.at[b]
        )
        for b in range(n)
    ]
    copies.append(
        pltpu.make_async_copy(
            ags.at[n - 1, pl.ds(step, span - step)],
            out_ref.at[pl.ds(n * step, span - step)],
            out_sem.at[n],
        )
    )
    for copy in copies:
        copy.start()
    d = lax.axis_index("replica") * n_spa + lax.axis_index("spatial")
    off = d * (shard - whole)
    shift_l = off % 128
    shift_r = off // 128
    back_l = 128 - shift_l
    lane = lax.broadcasted_iota(jnp.int32, (rows, 128), 1)
    for j, (src, buf, ref) in enumerate(((nmw, nm_out, nm_ref), (nvw, nv_out, nv_ref))):
        x = src[...].reshape(rows, 128)
        x = pltpu.roll(x, (rows - shift_r) % rows, 0)
        x = pltpu.roll(x, back_l % 128, 1)
        x = jnp.where(lane < back_l, x, pltpu.roll(x, rows - 1, 0))
        buf[pl.ds(0, whole)] = x[: step * 8].reshape(whole)
        buf[pl.ds(whole, shard - whole)] = x[step * 8, : shard - whole].reshape(shard - whole)
        copy = pltpu.make_async_copy(buf, ref, own_sem.at[j])
        copy.start()
        copies.append(copy)
    for copy in copies:
        copy.wait()


def windowed(n_rep, n_spa, grads, master, velocity, layer_offsets, layer_sizes, lars_skip):
    shard = master.shape[0]
    params = grads.shape[2]
    layers = layer_offsets.shape[0]
    plane = 8
    n = n_rep * n_spa
    n_out = n // plane
    step = shard // TILE
    span = params // TILE - (n - 1) * step
    chunk = (plane - 1) * step + span
    tiles = params // TILE
    hx = (span + 1) // 2
    hy = span - hx
    wx = step + 2 * hx - span
    plan = (n_out, shard, step, span, layers)
    vmem = pl.BlockSpec(memory_space=pltpu.VMEM)
    smem = pl.BlockSpec(memory_space=pltpu.SMEM)
    anywhere = pl.BlockSpec(memory_space=pltpu.HBM)
    f32, bf16 = jnp.float32, jnp.bfloat16
    dma = pltpu.SemaphoreType.DMA
    ags, nmw, nvw = pl.pallas_call(
        functools.partial(kernel, plan),
        out_shape=(
            pltpu.VMEM((n, span, 8, 128), bf16),
            pltpu.VMEM((span, 8, 128), f32),
            pltpu.VMEM((span, 8, 128), f32),
        ),
        in_specs=[anywhere, anywhere, anywhere, smem, smem, smem],
        out_specs=(vmem, vmem, vmem),
        scratch_shapes=[
            pltpu.VMEM((shard,), f32),
            pltpu.VMEM((shard,), f32),
            pltpu.VMEM((n_out, 1, chunk * TILE), bf16),
            pltpu.VMEM((n_out, chunk, 8, 128), bf16),
            pltpu.VMEM((n_out, 3, wx, 8, 128), bf16),
            pltpu.VMEM((n_out, 3, 2, hy, 8, 128), bf16),
            pltpu.VMEM((n_out, wx, 8, 128), f32),
            pltpu.VMEM((n_out, 2, hy, 8, 128), f32),
            pltpu.VMEM((n_out, hx, 8, 128), f32),
            pltpu.VMEM((n_out, hy, 8, 128), f32),
            pltpu.VMEM((n_out, span, 8, 128), f32),
            pltpu.VMEM((n_out, span, 8, 128), f32),
            pltpu.VMEM((span, 2, 8, 128), f32),
            pltpu.VMEM((2, 8, 128), f32),
            pltpu.VMEM((span, 8, 128), f32),
            pltpu.VMEM((1, 128), f32),
            pltpu.VMEM((n, 1, 128), f32),
            dma((n_out,)),
            dma((2,)),
            pltpu.SemaphoreType.REGULAR((n_out,)),
            dma(()),
            dma((n_out,)),
            dma(()),
            dma((n_out,)),
            dma(()),
            dma((n_out,)),
            dma(()),
            dma((n_out,)),
            dma(()),
            dma(()),
            dma((2,)),
            dma(()),
            dma(()),
            dma(()),
            dma((n,)),
        ],
        compiler_params=pltpu.CompilerParams(
            collective_id=0, has_side_effects=True, vmem_limit_bytes=61 * 2**20
        ),
    )(grads, master, velocity, layer_offsets, layer_sizes, lars_skip)
    weights, nm, nv = pl.pallas_call(
        functools.partial(finish, (n, n_spa, shard, step, span)),
        out_shape=(
            jax.ShapeDtypeStruct((tiles, 8, 128), bf16),
            jax.ShapeDtypeStruct((shard,), f32),
            jax.ShapeDtypeStruct((shard,), f32),
        ),
        in_specs=[vmem, vmem, vmem],
        out_specs=(anywhere, anywhere, anywhere),
        scratch_shapes=[
            pltpu.VMEM((shard,), f32),
            pltpu.VMEM((shard,), f32),
            dma((n + 1,)),
            dma((2,)),
        ],
        compiler_params=pltpu.CompilerParams(vmem_limit_bytes=16 * 2**20),
    )(ags, nmw, nvw)
    return weights.reshape(params), nm, nv


def tiled(n_rep, n_spa, params):
    n = n_rep * n_spa
    shard = params // n
    rest = shard % TILE
    n_out = n_rep // 4
    return (
        n_spa == 2
        and n_rep % 4 == 0
        and n_out >= 2
        and n_out & (n_out - 1) == 0
        and params % TILE == 0
        and shard >= TILE
        and 0 < n * rest <= TILE
        and rest <= 128
    )


def step_fn(n_rep, n_spa, grads, *rest):
    if tiled(n_rep, n_spa, grads.shape[2]):
        return windowed(n_rep, n_spa, grads, *rest)
    return shards(grads, *rest)


def shards(grads, master, velocity, layer_offsets, layer_sizes, lars_skip):
    n_rep = lax.axis_size("replica")
    n_spa = lax.axis_size("spatial")
    shard = master.shape[0]
    position = lax.axis_index(("replica", "spatial")) * shard + jnp.arange(shard, dtype=jnp.int32)
    inside = (position[None, :] >= layer_offsets[:, None]) & (
        position[None, :] < (layer_offsets + layer_sizes)[:, None]
    )
    onehot = inside.astype(jnp.float32)
    received = lax.all_to_all(
        grads[0, 0].reshape(n_rep, n_spa * shard),
        "replica",
        split_axis=0,
        concat_axis=0,
        tiled=True,
    )
    first = jnp.sum(received.astype(jnp.float32), axis=0)
    summed = lax.psum_scatter(
        first.reshape(n_spa, shard), "spatial", scatter_dimension=0, tiled=True
    )
    grad = summed.reshape(shard) / (n_rep * n_spa)
    gsq_local = jnp.dot(onehot, grad * grad, precision=lax.Precision.HIGHEST)
    wsq_local = jnp.dot(onehot, master * master, precision=lax.Precision.HIGHEST)
    wsq, gsq = lax.psum((wsq_local, gsq_local), ("replica", "spatial"))
    wnorm = jnp.sqrt(wsq)
    gnorm = jnp.sqrt(gsq)
    skipped = lars_skip.astype(jnp.float32)
    ratio = 0.02 * wnorm / (gnorm + 0.001 * wnorm + 1e-06)
    trust = skipped + (1.0 - skipped) * ratio
    decay = (1.0 - skipped) * 0.001
    trust_pos = jnp.dot(trust, onehot, precision=lax.Precision.HIGHEST)
    decay_pos = jnp.dot(decay, onehot, precision=lax.Precision.HIGHEST)
    new_velocity = 0.9 * velocity + 8.0 * trust_pos * (grad + decay_pos * master)
    new_master = master - new_velocity
    new_weights = lax.all_gather(
        new_master.astype(jnp.bfloat16), ("replica", "spatial"), axis=0, tiled=True
    )
    return (new_weights, new_master, new_velocity)


def solution(mesh):
    return jax.shard_map(
        functools.partial(step_fn, mesh.shape["replica"], mesh.shape["spatial"]),
        mesh=mesh,
        in_specs=(
            P("replica", "spatial", None),
            P(("replica", "spatial")),
            P(("replica", "spatial")),
            P(),
            P(),
            P(),
        ),
        out_specs=(P(), P(("replica", "spatial")), P(("replica", "spatial"))),
        check_vma=False,
    )
```

```python
import functools

import jax
import jax.numpy as jnp
from jax import lax
from jax.experimental import pallas as pl
from jax.experimental.pallas import tpu as pltpu
from jax.sharding import PartitionSpec as P

MESH = pl.DeviceIdType.MESH
TILE = 1024
ZTILES = 4
RS = "k1 bar A1 B1 k2 A2 k3 k4 z1 z2 z3 mv s1 B2 A3 s2 p1 B3 A4 s3 p2 B4 Z s4 p3 p4"
ZSEND = (1, 2, 3)
ZWAIT = (1, 2, 3)
DIRECT = (0, 3)


def flip(i, k):
    out, bit = 0, 1
    while bit <= k:
        b = (i // bit) % 2
        out = out + bit * (1 - 2 * b) * ((k // bit) % 2)
        bit *= 2
    return i + out


def kernel(
    plan,
    grads_ref,
    m_ref,
    v_ref,
    offsets_ref,
    sizes_ref,
    skip_ref,
    ags,
    nmw,
    nvw,
    m_in,
    v_in,
    gin,
    packed,
    r1x,
    r1y,
    sx,
    sy,
    r2x,
    r2y,
    rz1,
    zs,
    rz2,
    part,
    recv3,
    mv,
    halo,
    grad_buf,
    wrow,
    stats,
    in_sem,
    mv_sem,
    ready,
    send1x,
    got1x,
    send1y,
    got1y,
    send2x,
    got2x,
    send2y,
    got2y,
    sendz1,
    gotz1,
    sendz2,
    gotz2,
    send3,
    got3,
    halo_sem,
    send_s,
    got_s,
    send4,
    got4,
):
    n_out, shard, step, span, layers, hx, hy, hz = plan
    plane = 8
    n = n_out * plane
    chunk = (plane - 1) * step + span
    rows = span * 8
    hxy = hx + hy
    half_a = (span + 1) // 2
    half_b = span - half_a
    r = lax.axis_index("replica")
    y = lax.axis_index("spatial")
    d = r * 2 + y
    z = d // plane
    p = d % plane
    x = p // 4
    c = (p // 2) % 2
    base = d * (step * TILE)
    off = d * (shard - step * TILE)

    def dev(flat):
        return (flat // 2, flat % 2)

    def at(zz, xx, cc, yy):
        return ((zz * 2 + xx) * 2 + cc, yy)

    barrier = pltpu.get_barrier_semaphore()

    def load(zt):
        start = pl.multiple_of(zt * (plane * step * TILE), TILE)
        return pltpu.make_async_copy(
            grads_ref.at[0, :, pl.ds(start, chunk * TILE)], gin.at[zt], in_sem.at[zt]
        )

    order = [(z + k) % n_out for k in range(1, n_out + 1)]
    for zt in order:
        load(zt).start()
    mv_loads = [
        pltpu.make_async_copy(ref, buf, mv_sem.at[j])
        for j, (ref, buf) in enumerate(((m_ref, m_in), (v_ref, v_in)))
    ]
    for copy in mv_loads:
        copy.start()

    def signal(sem, device):
        pl.semaphore_signal(sem, inc=1, device_id=device, device_id_type=MESH)

    def signal_z(sem, cores):
        @pl.when(z > 0)
        def _():
            for cc in cores:
                signal(sem, at(z - 1, x, cc, y))

        @pl.when(z < n_out - 1)
        def _():
            for cc in cores:
                signal(sem, at(z + 1, x, cc, y))

    n_z = jnp.where(z > 0, 1, 0) + jnp.where(z < n_out - 1, 1, 0)
    for device in (
        at(z, x, 1 - c, y),
        at(z, 1 - x, c, y),
        at(z, x, c, 1 - y),
        at(z, 1 - x, 1 - c, y),
        at(z, x, 1 - c, 1 - y),
    ):
        signal(barrier, device)
    signal_z(barrier, (c, 1 - c))

    group = max(g for g in range(1, 33) if chunk % g == 0)

    def pack(zt):
        load(zt).wait()

        @pl.loop(0, chunk // group)
        def _(i):
            first = pl.multiple_of(i * (group * TILE), group * TILE)
            v = gin[zt, :, pl.ds(first, group * TILE)].astype(jnp.float32)
            packed[zt, pl.ds(i * group, group)] = v.reshape(group, 8, 128).astype(jnp.bfloat16)

    def remote(src, dst, send, recv, device):
        return pltpu.make_async_remote_copy(
            src_ref=src,
            dst_ref=dst,
            send_sem=send,
            recv_sem=recv,
            device_id=device,
            device_id_type=MESH,
        )

    def landed(ref, sem):
        pltpu.make_async_copy(ref, ref, sem).wait()

    def first(xx, cc, yy):
        return (xx * 4 + cc * 2 + yy) * step

    def send_raw(zt, h):
        yb, xb = (y, x) if h else (1 - y, 1 - x)
        for m in (3, 2, 1):
            xx, cc = (1 - x if m >= 2 else x), (1 - c if m % 2 else c)
            remote(
                packed.at[zt, pl.ds(first(xx, cc, yb), hx)],
                r1x.at[h, zt, m - 1],
                send1x,
                got1x.at[h, zt],
                at(z, xx, cc, y),
            ).start()
            yy = 1 - y if m >= 2 else y
            remote(
                packed.at[zt, pl.ds(first(xb, cc, yy) + hx, hy)],
                r1y.at[h, zt, m - 1],
                send1y,
                got1y.at[h, zt],
                at(z, x, cc, yy),
            ).start()

    def raws(zt, h, t, r1, own):
        v = packed[zt, own + t].astype(jnp.float32) + r1[h, zt, 0, t].astype(jnp.float32)
        return v + (r1[h, zt, 1, t].astype(jnp.float32) + r1[h, zt, 2, t].astype(jnp.float32))

    def sum_raw(zt):
        landed(r1x.at[0, zt], got1x.at[0, zt])
        own = first(x, c, 1 - y)

        @pl.loop(0, hx, unroll=2)
        def _(t):
            sx[zt, t] = raws(zt, 0, t, r1x, own)

        remote(sx.at[zt], r2x.at[zt], send2x, got2x.at[zt], at(z, x, c, 1 - y)).start()
        landed(r1y.at[0, zt], got1y.at[0, zt])
        own2 = first(1 - x, c, y) + hx

        @pl.loop(0, hy, unroll=2)
        def _(t):
            sy[zt, t] = raws(zt, 0, t, r1y, own2)

        remote(sy.at[zt], r2y.at[zt], send2y, got2y.at[zt], at(z, 1 - x, c, y)).start()

    def copy3(zt, src):
        return remote(part.at[zt], recv3.at[src], send3, got3, at(zt, x, c, y))

    def sum_plane(zt):
        own = first(x, c, y)
        landed(r1x.at[1, zt], got1x.at[1, zt])
        landed(r2x.at[zt], got2x.at[zt])

        @pl.loop(0, hx, unroll=2)
        def _(t):
            part[zt, t] = raws(zt, 1, t, r1x, own) + r2x[zt, t]

        landed(r1y.at[1, zt], got1y.at[1, zt])
        landed(r2y.at[zt], got2y.at[zt])

        @pl.loop(0, hy, unroll=2)
        def _(t):
            part[zt, hx + t] = raws(zt, 1, t, r1y, own + hx) + r2y[zt, t]

    def send_far(zt, other):
        cc = 1 - c if other else c
        for j in range(4):
            remote(
                packed.at[zt, pl.ds(first(j // 2, cc, j % 2) + hxy, hz)],
                rz1.at[other * n_out + z, j],
                sendz1,
                gotz1,
                at(zt, x, cc, y),
            ).start()

    def send_distance(j):
        @pl.when(z >= j)
        def _():
            for other in (0, 1):
                send_far(z - j, other)

        @pl.when(z < n_out - j)
        def _():
            for other in (0, 1):
                send_far(z + j, other)

    def sum_far():
        landed(rz1.at[pl.ds(0, 2 * n_out - 1)], gotz1)

        @pl.loop(0, 4)
        def _(j):
            own = first(j // 2, c, j % 2) + hxy
            for t in range(hz):
                acc = packed[z, own + t].astype(jnp.float32)
                acc = acc + rz1[n_out + z, j, t].astype(jnp.float32)
                for k in range(1, n_out):
                    zz = (z + k) % n_out
                    two = rz1[zz, j, t].astype(jnp.float32)
                    acc = acc + (two + rz1[n_out + zz, j, t].astype(jnp.float32))
                zs[j, t] = acc

        for m in (3, 2, 1):
            xx, yy = (1 - x if m >= 2 else x), (1 - y if m % 2 else y)
            remote(zs.at[xx * 2 + yy], rz2.at[m - 1], sendz2, gotz2, at(z, xx, c, yy)).start()

    lane = lax.broadcasted_iota(jnp.int32, (rows, 128), 1)
    shift_l = off % 128
    shift_r = off // 128
    whole = step * TILE

    def window(j, ref):
        mv_loads[j].wait()
        edge = jnp.pad(ref[pl.ds(whole, shard - whole)], (0, 128 - (shard - whole)))
        edge = jnp.broadcast_to(edge.reshape(1, 128), (8, 128))
        w = jnp.concatenate([ref[pl.ds(0, whole)].reshape(step * 8, 128), edge], 0)
        w = pltpu.roll(w, shift_l, 1)
        w = jnp.where(lane < shift_l, pltpu.roll(w, 1, 0), w)
        w = pltpu.roll(w, shift_r, 0)
        mv[:, j] = w.reshape(span, 8, 128)

    place = lax.broadcasted_iota(jnp.int32, (8, 128), 0) * 128 + lax.broadcasted_iota(
        jnp.int32, (8, 128), 1
    )
    low = [offsets_ref[l] - base for l in range(layers)]
    high = [offsets_ref[l] + sizes_ref[l] - base for l in range(layers)]
    own_low = [jnp.maximum(v, off) for v in low]
    own_high = [jnp.minimum(v, off + shard) for v in high]
    lane1 = lax.broadcasted_iota(jnp.int32, (1, 128), 1)

    def squares(value, first):
        def add(t, accs):
            pos = place + t * TILE
            v = value(t)
            v = v * v
            return tuple(
                acc + jnp.where((pos >= lo) & (pos < hi), v, 0.0)
                for acc, lo, hi in zip(accs, own_low, own_high)
            )

        accs = lax.fori_loop(
            0, span, add, tuple(jnp.zeros((8, 128), jnp.float32) for _ in range(layers))
        )
        row = jnp.zeros((1, 128), jnp.float32)
        for l, acc in enumerate(accs):
            row = jnp.where(lane1 == first + l, jnp.sum(acc, axis=(0, 1), keepdims=True), row)
        return row

    def step_z(j):
        if j == 1:
            send_distance(1)
            send_far(z, 1)
            return
        pl.semaphore_wait(ready.at[j - 2], n_z)
        if j < n_out - 1:
            signal_z(ready.at[j - 1], (c,))
        send_distance(j)

    for op in RS.split():
        i = int(op[1:] or 0) if op != "bar" and op != "mv" else 0
        zt = order[i - 1]
        if op == "bar":
            pl.semaphore_wait(barrier, 5 + 2 * n_z)
            signal_z(ready.at[0], (c,))
        elif op == "mv":
            for j, ref in enumerate((m_in, v_in)):
                window(j, ref)
            wrow[...] = squares(lambda t: mv[t, 0], 0)
        elif op[0] == "k":
            pack(zt)
        elif op[0] == "A":
            send_raw(zt, 0)
        elif op[0] == "B":
            send_raw(zt, 1)
        elif op[0] == "z":
            step_z(i)
        elif op[0] == "Z":
            sum_far()
        elif op[0] == "s":
            sum_raw(zt)
        elif op[0] == "p":
            sum_plane(zt)
            if i < n_out:
                copy3(zt, z).start()

    landed(recv3.at[pl.ds(0, n_out - 1)], got3)

    @pl.loop(0, hxy)
    def _(t):
        acc = part[z, t]
        for k in range(1, n_out):
            acc = acc + recv3[(z + k) % n_out, t]
        grad_buf[t] = acc / n

    landed(rz2, gotz2)
    for t in range(hz):
        acc = zs[x * 2 + y, t] + rz2[0, t]
        grad_buf[hxy + t] = (acc + (rz2[1, t] + rz2[2, t])) / n

    stats[d] = squares(lambda t: grad_buf[t], layers) + wrow[...]

    @pl.loop(1, n, unroll=True)
    def _(q):
        remote(stats.at[d], stats.at[d], send_s, got_s, dev((d + q) % n)).start()

    halo_copy = remote(mv.at[span - 1], halo, halo_sem.at[0], halo_sem.at[1], dev((d + 1) % n))
    halo_copy.start()

    landed(stats.at[pl.ds(0, n - 1)], got_s)
    total = jnp.sum(stats[...], axis=0)
    trust, decay = [], []
    for l in range(layers):
        wsq = jnp.sum(jnp.where(lane1 == l, total, 0.0), axis=(0, 1), keepdims=True)
        gsq = jnp.sum(jnp.where(lane1 == layers + l, total, 0.0), axis=(0, 1), keepdims=True)
        wnorm = jnp.sqrt(jnp.broadcast_to(wsq, (8, 128)))
        gnorm = jnp.sqrt(jnp.broadcast_to(gsq, (8, 128)))
        skipped = skip_ref[l].astype(jnp.float32)
        ratio = 0.02 * wnorm / (gnorm + 0.001 * wnorm + 1e-06)
        trust.append(skipped + (1.0 - skipped) * ratio)
        decay.append((1.0 - skipped) * 0.001)

    halo_copy.wait()
    for j in range(2):
        mv[0, j] = jnp.where(place < off, halo[j], mv[0, j])

    @pl.loop(0, span)
    def _(t):
        pos = place + t * TILE
        trust_pos = jnp.zeros((8, 128), jnp.float32)
        decay_pos = jnp.zeros((8, 128), jnp.float32)
        for l in range(layers):
            inside = (pos >= low[l]) & (pos < high[l])
            trust_pos = jnp.where(inside, trust[l], trust_pos)
            decay_pos = jnp.where(inside, decay[l], decay_pos)
        m = mv[t, 0]
        nv = 0.9 * mv[t, 1] + 8.0 * trust_pos * (grad_buf[t] + decay_pos * m)
        nm = m - nv
        nvw[t] = nv
        nmw[t] = nm
        ags[d, t] = nm.astype(jnp.bfloat16)

    def block(zz, xx, cc, yy):
        return zz * plane + xx * 4 + cc * 2 + yy

    def forward(b, device, lo=0, size=span):
        piece = ags.at[b, pl.ds(lo, size)]
        remote(piece, piece, send4, got4.at[b], device).start()

    def arrived(b):
        landed(ags.at[b], got4.at[b])

    x_side = at(z, 1 - x, c, y)
    y_side = at(z, x, c, 1 - y)
    across = at(z, 1 - x, c, 1 - y)
    partner = at(z, x, 1 - c, y)
    for k in ZSEND:
        forward(d, at(flip(z, k), x, c, y))

    def column(k):
        b = block(flip(z, k), x, c, y)
        if k > 0:
            arrived(b)
        forward(b, x_side)
        forward(b, y_side)
        if k in DIRECT:
            forward(b, across)
        forward(b, partner)

    def sides(k):
        zz = flip(z, k)
        b = block(zz, x, c, 1 - y)
        arrived(b)
        if k not in DIRECT:
            forward(b, x_side, 0, half_a)
        forward(b, partner)
        b = block(zz, 1 - x, c, y)
        arrived(b)
        if k not in DIRECT:
            forward(b, y_side, half_a, half_b)
        forward(b, partner)

    def corner(k):
        b = block(flip(z, k), 1 - x, c, 1 - y)
        arrived(b)
        forward(b, partner)

    visits = (0,) + ZWAIT
    column(0)
    for i, k in enumerate(visits):
        if i + 1 < n_out:
            column(visits[i + 1])
        sides(k)
        if i > 0:
            corner(visits[i - 1])
    corner(visits[-1])

    @pl.loop(0, n_out)
    def _(k):
        for xx in range(2):
            for yy in range(2):
                arrived(block(k, xx, 1 - c, yy))

    for ref, sem in (
        (r1x, send1x),
        (r1y, send1y),
        (r2x, send2x),
        (r2y, send2y),
        (rz1.at[pl.ds(0, 2 * n_out - 1)], sendz1),
        (rz2, sendz2),
        (recv3.at[pl.ds(0, n_out - 1)], send3),
        (stats.at[pl.ds(0, n - 1)], send_s),
        (ags.at[pl.ds(0, n - 1)], send4),
    ):
        landed(ref, sem)


def finish(plan, ags, nmw, nvw, out_ref, nm_ref, nv_ref, nm_out, nv_out, out_sem, own_sem):
    n, n_spa, shard, step, span = plan
    rows = span * 8
    whole = step * TILE
    copies = [
        pltpu.make_async_copy(
            ags.at[b, pl.ds(0, step)], out_ref.at[pl.ds(b * step, step)], out_sem.at[b]
        )
        for b in range(n)
    ]
    copies.append(
        pltpu.make_async_copy(
            ags.at[n - 1, pl.ds(step, span - step)],
            out_ref.at[pl.ds(n * step, span - step)],
            out_sem.at[n],
        )
    )
    for copy in copies:
        copy.start()
    d = lax.axis_index("replica") * n_spa + lax.axis_index("spatial")
    off = d * (shard - whole)
    shift_l = off % 128
    shift_r = off // 128
    back_l = 128 - shift_l
    lane = lax.broadcasted_iota(jnp.int32, (rows, 128), 1)
    for j, (src, buf, ref) in enumerate(((nmw, nm_out, nm_ref), (nvw, nv_out, nv_ref))):
        x = src[...].reshape(rows, 128)
        x = pltpu.roll(x, (rows - shift_r) % rows, 0)
        x = pltpu.roll(x, back_l % 128, 1)
        x = jnp.where(lane < back_l, x, pltpu.roll(x, rows - 1, 0))
        buf[pl.ds(0, whole)] = x[: step * 8].reshape(whole)
        buf[pl.ds(whole, shard - whole)] = x[step * 8, : shard - whole].reshape(shard - whole)
        copy = pltpu.make_async_copy(buf, ref, own_sem.at[j])
        copy.start()
        copies.append(copy)
    for copy in copies:
        copy.wait()


def windowed(n_rep, n_spa, grads, master, velocity, layer_offsets, layer_sizes, lars_skip):
    shard = master.shape[0]
    params = grads.shape[2]
    layers = layer_offsets.shape[0]
    plane = 8
    n = n_rep * n_spa
    n_out = n // plane
    step = shard // TILE
    span = params // TILE - (n - 1) * step
    chunk = (plane - 1) * step + span
    tiles = params // TILE
    hz = ZTILES
    hx = (span - hz + 1) // 2
    hy = span - hz - hx
    plan = (n_out, shard, step, span, layers, hx, hy, hz)
    vmem = pl.BlockSpec(memory_space=pltpu.VMEM)
    smem = pl.BlockSpec(memory_space=pltpu.SMEM)
    anywhere = pl.BlockSpec(memory_space=pltpu.HBM)
    f32, bf16 = jnp.float32, jnp.bfloat16
    dma = pltpu.SemaphoreType.DMA
    ags, nmw, nvw = pl.pallas_call(
        functools.partial(kernel, plan),
        out_shape=(
            pltpu.VMEM((n, span, 8, 128), bf16),
            pltpu.VMEM((span, 8, 128), f32),
            pltpu.VMEM((span, 8, 128), f32),
        ),
        in_specs=[anywhere, anywhere, anywhere, smem, smem, smem],
        out_specs=(vmem, vmem, vmem),
        scratch_shapes=[
            pltpu.VMEM((shard,), f32),
            pltpu.VMEM((shard,), f32),
            pltpu.VMEM((n_out, 1, chunk * TILE), bf16),
            pltpu.VMEM((n_out, chunk, 8, 128), bf16),
            pltpu.VMEM((2, n_out, 3, hx, 8, 128), bf16),
            pltpu.VMEM((2, n_out, 3, hy, 8, 128), bf16),
            pltpu.VMEM((n_out, hx, 8, 128), f32),
            pltpu.VMEM((n_out, hy, 8, 128), f32),
            pltpu.VMEM((n_out, hx, 8, 128), f32),
            pltpu.VMEM((n_out, hy, 8, 128), f32),
            pltpu.VMEM((2 * n_out, 4, hz, 8, 128), bf16),
            pltpu.VMEM((4, hz, 8, 128), f32),
            pltpu.VMEM((3, hz, 8, 128), f32),
            pltpu.VMEM((n_out, hx + hy, 8, 128), f32),
            pltpu.VMEM((n_out, hx + hy, 8, 128), f32),
            pltpu.VMEM((span, 2, 8, 128), f32),
            pltpu.VMEM((2, 8, 128), f32),
            pltpu.VMEM((span, 8, 128), f32),
            pltpu.VMEM((1, 128), f32),
            pltpu.VMEM((n, 1, 128), f32),
            dma((n_out,)),
            dma((2,)),
            pltpu.SemaphoreType.REGULAR((n_out,)),
            dma(()),
            dma((2, n_out)),
            dma(()),
            dma((2, n_out)),
            dma(()),
            dma((n_out,)),
            dma(()),
            dma((n_out,)),
            dma(()),
            dma(()),
            dma(()),
            dma(()),
            dma(()),
            dma(()),
            dma((2,)),
            dma(()),
            dma(()),
            dma(()),
            dma((n,)),
        ],
        compiler_params=pltpu.CompilerParams(
            collective_id=0, has_side_effects=True, vmem_limit_bytes=61 * 2**20
        ),
    )(grads, master, velocity, layer_offsets, layer_sizes, lars_skip)
    weights, nm, nv = pl.pallas_call(
        functools.partial(finish, (n, n_spa, shard, step, span)),
        out_shape=(
            jax.ShapeDtypeStruct((tiles, 8, 128), bf16),
            jax.ShapeDtypeStruct((shard,), f32),
            jax.ShapeDtypeStruct((shard,), f32),
        ),
        in_specs=[vmem, vmem, vmem],
        out_specs=(anywhere, anywhere, anywhere),
        scratch_shapes=[
            pltpu.VMEM((shard,), f32),
            pltpu.VMEM((shard,), f32),
            dma((n + 1,)),
            dma((2,)),
        ],
        compiler_params=pltpu.CompilerParams(vmem_limit_bytes=16 * 2**20),
    )(ags, nmw, nvw)
    return weights.reshape(params), nm, nv


def tiled(n_rep, n_spa, params):
    n = n_rep * n_spa
    shard = params // n
    rest = shard % TILE
    n_out = n_rep // 4
    return (
        n_spa == 2
        and n_rep % 4 == 0
        and n_out >= 2
        and n_out & (n_out - 1) == 0
        and params % TILE == 0
        and shard >= TILE
        and 0 < n * rest <= TILE
        and rest <= 128
    )


def step_fn(n_rep, n_spa, grads, *rest):
    if tiled(n_rep, n_spa, grads.shape[2]):
        return windowed(n_rep, n_spa, grads, *rest)
    return shards(grads, *rest)


def shards(grads, master, velocity, layer_offsets, layer_sizes, lars_skip):
    n_rep = lax.axis_size("replica")
    n_spa = lax.axis_size("spatial")
    shard = master.shape[0]
    position = lax.axis_index(("replica", "spatial")) * shard + jnp.arange(shard, dtype=jnp.int32)
    inside = (position[None, :] >= layer_offsets[:, None]) & (
        position[None, :] < (layer_offsets + layer_sizes)[:, None]
    )
    onehot = inside.astype(jnp.float32)
    received = lax.all_to_all(
        grads[0, 0].reshape(n_rep, n_spa * shard),
        "replica",
        split_axis=0,
        concat_axis=0,
        tiled=True,
    )
    first = jnp.sum(received.astype(jnp.float32), axis=0)
    summed = lax.psum_scatter(
        first.reshape(n_spa, shard), "spatial", scatter_dimension=0, tiled=True
    )
    grad = summed.reshape(shard) / (n_rep * n_spa)
    gsq_local = jnp.dot(onehot, grad * grad, precision=lax.Precision.HIGHEST)
    wsq_local = jnp.dot(onehot, master * master, precision=lax.Precision.HIGHEST)
    wsq, gsq = lax.psum((wsq_local, gsq_local), ("replica", "spatial"))
    wnorm = jnp.sqrt(wsq)
    gnorm = jnp.sqrt(gsq)
    skipped = lars_skip.astype(jnp.float32)
    ratio = 0.02 * wnorm / (gnorm + 0.001 * wnorm + 1e-06)
    trust = skipped + (1.0 - skipped) * ratio
    decay = (1.0 - skipped) * 0.001
    trust_pos = jnp.dot(trust, onehot, precision=lax.Precision.HIGHEST)
    decay_pos = jnp.dot(decay, onehot, precision=lax.Precision.HIGHEST)
    new_velocity = 0.9 * velocity + 8.0 * trust_pos * (grad + decay_pos * master)
    new_master = master - new_velocity
    new_weights = lax.all_gather(
        new_master.astype(jnp.bfloat16), ("replica", "spatial"), axis=0, tiled=True
    )
    return (new_weights, new_master, new_velocity)


def solution(mesh):
    return jax.shard_map(
        functools.partial(step_fn, mesh.shape["replica"], mesh.shape["spatial"]),
        mesh=mesh,
        in_specs=(
            P("replica", "spatial", None),
            P(("replica", "spatial")),
            P(("replica", "spatial")),
            P(),
            P(),
            P(),
        ),
        out_specs=(P(), P(("replica", "spatial")), P(("replica", "spatial"))),
        check_vma=False,
    )
```

```python
import functools

import jax
import jax.numpy as jnp
from jax import lax
from jax.experimental import pallas as pl
from jax.experimental.pallas import tpu as pltpu
from jax.sharding import PartitionSpec as P

MESH = pl.DeviceIdType.MESH
TILE = 1024
ZTILES = 5
XOR = (2, 3, 1, 0)
RS = (
    "k1", "bar", "A1", "B1", "k2", "A2", "k3", "k4", "z1", "z2", "z3", "mv", "s1", "B2", "A3",
    "s2", "p1", "B3", "A4", "s3", "p2", "B4", "Z", "s4", "p3", "p4",
)
ZSEND = (1, 2, 3)
AG = (
    "c0", "c1", "g0", "x0", "y0", "c2", "e0", "c3", "x1", "y1", "d0", "x2", "y2", "d1", "h1",
    "h2", "h3", "x3", "y3", "d2", "d3",
)
DIRECT = (0, 3)


def flip(i, k):
    out, bit = 0, 1
    while bit <= k:
        b = (i // bit) % 2
        out = out + bit * (1 - 2 * b) * ((k // bit) % 2)
        bit *= 2
    return i + out


def kernel(
    plan,
    grads_ref,
    m_ref,
    v_ref,
    offsets_in,
    sizes_in,
    skip_in,
    ags,
    agz,
    age,
    nmw,
    nvw,
    offsets_ref,
    sizes_ref,
    skip_ref,
    m_in,
    v_in,
    gin,
    packed,
    r1x,
    r1y,
    sx,
    sy,
    r2x,
    r2y,
    rz1,
    zs,
    rz2,
    re1,
    ze,
    re2,
    part,
    recv3,
    mv,
    halo,
    grad_buf,
    wrow,
    stats,
    in_sem,
    mv_sem,
    table_sem,
    ready,
    send1x,
    got1x,
    send1y,
    got1y,
    send2x,
    got2x,
    send2y,
    got2y,
    sendz1,
    gotz1,
    sendz2,
    gotz2,
    send_e1,
    got_e1,
    send_e2,
    got_e2,
    send3,
    got3,
    halo_sem,
    send_s,
    got_s,
    send4,
    got4,
    send_g,
    got_in,
    got_gz,
    got_gc,
    send_e,
    got_e,
    back_sem,
):
    n_out, shard, step, span, layers, hx, hy, hz = plan
    plane = 8
    n = n_out * plane
    chunk = (plane - 1) * step + span
    rows = span * 8
    hxy = hx + hy
    last = n_out - 1
    half_a = (hxy + 1) // 2
    half_b = hxy - half_a
    r = lax.axis_index("replica")
    y = lax.axis_index("spatial")
    d = r * 2 + y
    z = d // plane
    p = d % plane
    x = p // 4
    c = (p // 2) % 2
    base = d * (step * TILE)
    off = d * (shard - step * TILE)

    def dev(flat):
        return (flat // 2, flat % 2)

    def at(zz, xx, cc, yy):
        return ((zz * 2 + xx) * 2 + cc, yy)

    barrier = pltpu.get_barrier_semaphore()

    def load(zt):
        start = pl.multiple_of(zt * (plane * step * TILE), TILE)
        return pltpu.make_async_copy(
            grads_ref.at[0, :, pl.ds(start, chunk * TILE)], gin.at[zt], in_sem.at[zt]
        )

    order = [(z + k) % n_out for k in range(1, n_out + 1)]
    if XOR:
        order = [flip(z, k) for k in XOR]
    for zt in order:
        load(zt).start()
    mv_loads = [
        pltpu.make_async_copy(ref, buf, mv_sem.at[j])
        for j, (ref, buf) in enumerate(((m_ref, m_in), (v_ref, v_in)))
    ]
    tables = [
        pltpu.make_async_copy(ref, buf, table_sem.at[j])
        for j, (ref, buf) in enumerate(
            ((offsets_in, offsets_ref), (sizes_in, sizes_ref), (skip_in, skip_ref))
        )
    ]
    for copy in mv_loads + tables:
        copy.start()

    def signal(sem, device):
        pl.semaphore_signal(sem, inc=1, device_id=device, device_id_type=MESH)

    def signal_z(sem, cores):
        @pl.when(z > 0)
        def _():
            for cc in cores:
                signal(sem, at(z - 1, x, cc, y))

        @pl.when(z < n_out - 1)
        def _():
            for cc in cores:
                signal(sem, at(z + 1, x, cc, y))

    n_z = jnp.where(z > 0, 1, 0) + jnp.where(z < n_out - 1, 1, 0)
    for device in (
        at(z, x, 1 - c, y),
        at(z, 1 - x, c, y),
        at(z, x, c, 1 - y),
        at(z, 1 - x, 1 - c, y),
        at(z, x, 1 - c, 1 - y),
    ):
        signal(barrier, device)
    signal_z(barrier, (c, 1 - c))

    group = max(g for g in range(1, 33) if chunk % g == 0)

    def pack(k):
        zt = order[k - 1]
        load(zt).wait()
        @pl.loop(0, chunk // group)
        def _(i):
            first = pl.multiple_of(i * (group * TILE), group * TILE)
            v = gin[zt, :, pl.ds(first, group * TILE)].astype(jnp.float32)
            packed[zt, pl.ds(i * group, group)] = v.reshape(group, 8, 128).astype(jnp.bfloat16)

    def remote(src, dst, send, recv, device):
        return pltpu.make_async_remote_copy(
            src_ref=src,
            dst_ref=dst,
            send_sem=send,
            recv_sem=recv,
            device_id=device,
            device_id_type=MESH,
        )

    def landed(ref, sem):
        pltpu.make_async_copy(ref, ref, sem).wait()

    def first(xx, cc, yy):
        return (xx * 4 + cc * 2 + yy) * step

    def send_raw(zt, h):
        yb, xb = (y, x) if h else (1 - y, 1 - x)
        for m in (3, 2, 1):
            xx, cc = (1 - x if m >= 2 else x), (1 - c if m % 2 else c)
            remote(
                packed.at[zt, pl.ds(first(xx, cc, yb), hx)],
                r1x.at[h, zt, m - 1],
                send1x,
                got1x.at[h, zt],
                at(z, xx, cc, y),
            ).start()
            yy = 1 - y if m >= 2 else y
            remote(
                packed.at[zt, pl.ds(first(xb, cc, yy) + hx, hy)],
                r1y.at[h, zt, m - 1],
                send1y,
                got1y.at[h, zt],
                at(z, x, cc, yy),
            ).start()

    def raws(zt, h, t, r1, own):
        v = packed[zt, own + t].astype(jnp.float32) + r1[h, zt, 0, t].astype(jnp.float32)
        return v + (r1[h, zt, 1, t].astype(jnp.float32) + r1[h, zt, 2, t].astype(jnp.float32))

    def sum_raw(zt):
        landed(r1x.at[0, zt], got1x.at[0, zt])
        own = first(x, c, 1 - y)

        @pl.loop(0, hx, unroll=2)
        def _(t):
            sx[zt, t] = raws(zt, 0, t, r1x, own)

        remote(sx.at[zt], r2x.at[zt], send2x, got2x.at[zt], at(z, x, c, 1 - y)).start()
        landed(r1y.at[0, zt], got1y.at[0, zt])
        own2 = first(1 - x, c, y) + hx

        @pl.loop(0, hy, unroll=2)
        def _(t):
            sy[zt, t] = raws(zt, 0, t, r1y, own2)

        remote(sy.at[zt], r2y.at[zt], send2y, got2y.at[zt], at(z, 1 - x, c, y)).start()

    def copy3(zt, src):
        return remote(part.at[zt], recv3.at[src], send3, got3, at(zt, x, c, y))

    def sum_plane(zt):
        own = first(x, c, y)
        landed(r1x.at[1, zt], got1x.at[1, zt])
        landed(r2x.at[zt], got2x.at[zt])

        @pl.loop(0, hx, unroll=2)
        def _(t):
            part[zt, t] = raws(zt, 1, t, r1x, own) + r2x[zt, t]

        landed(r1y.at[1, zt], got1y.at[1, zt])
        landed(r2y.at[zt], got2y.at[zt])

        @pl.loop(0, hy, unroll=2)
        def _(t):
            part[zt, hx + t] = raws(zt, 1, t, r1y, own + hx) + r2y[zt, t]

    def send_far(zt, other):
        cc = 1 - c if other else c
        for j in range(4):
            remote(
                packed.at[zt, pl.ds(first(j // 2, cc, j % 2) + hxy, hz)],
                rz1.at[other * n_out + z, j],
                sendz1,
                gotz1,
                at(zt, x, cc, y),
            ).start()

        @pl.when((zt == last) & (cc == 1))
        def _():
            remote(
                packed.at[last, pl.ds(chunk - 1, 1)],
                re1.at[pl.ds(z * 2 + c, 1)],
                send_e1,
                got_e1,
                at(zt, x, cc, y),
            ).start()

    def send_distance(j):
        @pl.when(z >= j)
        def _():
            for other in (0, 1):
                send_far(z - j, other)

        @pl.when(z < n_out - j)
        def _():
            for other in (0, 1):
                send_far(z + j, other)

    def sum_far():
        landed(rz1.at[pl.ds(0, 2 * n_out - 1)], gotz1)

        @pl.loop(0, 4)
        def _(j):
            own = first(j // 2, c, j % 2) + hxy
            for t in range(hz):
                acc = packed[z, own + t].astype(jnp.float32)
                acc = acc + rz1[n_out + z, j, t].astype(jnp.float32)
                for k in range(1, n_out):
                    zz = (z + k) % n_out
                    two = rz1[zz, j, t].astype(jnp.float32)
                    acc = acc + (two + rz1[n_out + zz, j, t].astype(jnp.float32))
                zs[j, t] = acc

        for m in (3, 2, 1):
            xx, yy = (1 - x if m >= 2 else x), (1 - y if m % 2 else y)
            remote(zs.at[xx * 2 + yy], rz2.at[m - 1], sendz2, gotz2, at(z, xx, c, yy)).start()

        @pl.when((z == last) & (c == 1))
        def _():
            landed(re1.at[pl.ds(0, 2 * n_out - 1)], got_e1)
            acc = packed[last, chunk - 1].astype(jnp.float32)
            for j in range(2 * n_out - 1):
                acc = acc + re1[j].astype(jnp.float32)
            ze[0] = acc

            @pl.when(x * 2 + y < 3)
            def _():
                remote(
                    ze, re2.at[pl.ds(x * 2 + y, 1)], send_e2, got_e2, at(z, 1, 1, 1)
                ).start()

    lane = lax.broadcasted_iota(jnp.int32, (rows, 128), 1)
    shift_l = off % 128
    shift_r = off // 128
    whole = step * TILE

    def window(j, ref):
        mv_loads[j].wait()
        edge = jnp.pad(ref[pl.ds(whole, shard - whole)], (0, 128 - (shard - whole)))
        edge = jnp.broadcast_to(edge.reshape(1, 128), (8, 128))
        w = jnp.concatenate([ref[pl.ds(0, whole)].reshape(step * 8, 128), edge], 0)
        w = pltpu.roll(w, shift_l, 1)
        w = jnp.where(lane < shift_l, pltpu.roll(w, 1, 0), w)
        w = pltpu.roll(w, shift_r, 0)
        mv[:, j] = w.reshape(span, 8, 128)

    place = lax.broadcasted_iota(jnp.int32, (8, 128), 0) * 128 + lax.broadcasted_iota(
        jnp.int32, (8, 128), 1
    )
    low, high, own_low, own_high = [], [], [], []

    def bounds():
        for copy in tables:
            copy.wait()
        for l in range(layers):
            low.append(offsets_ref[l] - base)
            high.append(offsets_ref[l] + sizes_ref[l] - base)
            own_low.append(jnp.maximum(low[l], off))
            own_high.append(jnp.minimum(high[l], off + shard))

    lane1 = lax.broadcasted_iota(jnp.int32, (1, 128), 1)

    def squares(value, first, lows, highs):
        def add(t, accs):
            pos = place + t * TILE
            v = value(t)
            v = v * v
            return tuple(
                acc + jnp.where((pos >= lo) & (pos < hi), v, 0.0)
                for acc, lo, hi in zip(accs, lows, highs)
            )

        accs = lax.fori_loop(
            0, span, add, tuple(jnp.zeros((8, 128), jnp.float32) for _ in range(layers))
        )
        row = jnp.zeros((1, 128), jnp.float32)
        for l, acc in enumerate(accs):
            row = jnp.where(lane1 == first + l, jnp.sum(acc, axis=(0, 1), keepdims=True), row)
        return row

    def step_z(j):
        if j == 1:
            send_distance(1)
            send_far(z, 1)
            return
        pl.semaphore_wait(ready.at[j - 2], n_z)
        if j < n_out - 1:
            signal_z(ready.at[j - 1], (c,))
        send_distance(j)

    for op in RS:
        i = int(op[1:] or 0) if op != "bar" and op != "mv" else 0
        zt = order[i - 1]
        if op == "bar":
            pl.semaphore_wait(barrier, 5 + 2 * n_z)
            signal_z(ready.at[0], (c,))
        elif op == "mv":
            bounds()
            for j, ref in enumerate((m_in, v_in)):
                window(j, ref)
            wrow[...] = squares(lambda t: mv[t, 0], 0, own_low, own_high)
        elif op[0] == "k":
            pack(i)
        elif op[0] == "A":
            send_raw(zt, 0)
        elif op[0] == "B":
            send_raw(zt, 1)
        elif op[0] == "z":
            step_z(i)
        elif op[0] == "Z":
            sum_far()
        elif op[0] == "s":
            sum_raw(zt)
        elif op[0] == "p":
            sum_plane(zt)
            if i < n_out:
                copy3(zt, z).start()

    landed(recv3.at[pl.ds(0, n_out - 1)], got3)

    @pl.loop(0, hxy)
    def _(t):
        acc = part[z, t]
        for k in range(1, n_out):
            acc = acc + recv3[(z + k) % n_out, t]
        grad_buf[t] = acc / n

    landed(rz2, gotz2)
    for t in range(hz):
        acc = zs[x * 2 + y, t] + rz2[0, t]
        grad_buf[hxy + t] = (acc + (rz2[1, t] + rz2[2, t])) / n
    grad_buf[step] = jnp.zeros((8, 128), jnp.float32)

    @pl.when(d == n - 1)
    def _():
        landed(re2, got_e2)
        grad_buf[step] = (ze[0] + re2[0] + (re2[1] + re2[2])) / n

    stats[d] = squares(lambda t: grad_buf[t], layers, low, high) + wrow[...]

    for k in range(n_out - 1, -1, -1):
        for q in range(plane - 1, -1, -1):
            if k + q > 0:
                peer = flip(z, k) * plane + flip(p, q)
                remote(stats.at[d], stats.at[d], send_s, got_s, dev(peer)).start()

    halo_copy = remote(mv.at[span - 1], halo, halo_sem.at[0], halo_sem.at[1], dev((d + 1) % n))
    halo_copy.start()

    landed(stats.at[pl.ds(0, n - 1)], got_s)
    total = jnp.sum(stats[...], axis=0)
    trust, decay = [], []
    for l in range(layers):
        wsq = jnp.sum(jnp.where(lane1 == l, total, 0.0), axis=(0, 1), keepdims=True)
        gsq = jnp.sum(jnp.where(lane1 == layers + l, total, 0.0), axis=(0, 1), keepdims=True)
        wnorm = jnp.sqrt(jnp.broadcast_to(wsq, (8, 128)))
        gnorm = jnp.sqrt(jnp.broadcast_to(gsq, (8, 128)))
        skipped = skip_ref[l].astype(jnp.float32)
        ratio = 0.02 * wnorm / (gnorm + 0.001 * wnorm + 1e-06)
        trust.append(skipped + (1.0 - skipped) * ratio)
        decay.append((1.0 - skipped) * 0.001)

    halo_copy.wait()
    for j in range(2):
        mv[0, j] = jnp.where(place < off, halo[j], mv[0, j])

    def update(t):
        pos = place + t * TILE
        trust_pos = jnp.zeros((8, 128), jnp.float32)
        decay_pos = jnp.zeros((8, 128), jnp.float32)
        for l in range(layers):
            inside = (pos >= low[l]) & (pos < high[l])
            trust_pos = jnp.where(inside, trust[l], trust_pos)
            decay_pos = jnp.where(inside, decay[l], decay_pos)
        m = mv[t, 0]
        nv = 0.9 * mv[t, 1] + 8.0 * trust_pos * (grad_buf[t] + decay_pos * m)
        nm = m - nv
        nvw[t] = nv
        nmw[t] = nm
        return nm.astype(jnp.bfloat16)

    def zslot(zz, xx, cc, yy):
        return (cc * n_out + zz) * 4 + xx * 2 + yy

    x_side = at(z, 1 - x, c, y)
    y_side = at(z, x, c, 1 - y)
    across = at(z, 1 - x, c, 1 - y)
    partner = at(z, x, 1 - c, y)
    mine = zslot(z, x, c, y)
    for t in range(hz):
        agz[mine, t] = update(hxy + t)
    for device in (across, x_side, y_side):
        remote(agz.at[mine], agz.at[mine], send_g, got_in, device).start()

    @pl.loop(0, hxy)
    def _(t):
        ags[d, t] = update(t)

    def send_edge():
        for i, ref in enumerate((nmw, nvw)):
            remote(ref.at[0], ref.at[step], back_sem.at[i], back_sem.at[2 + i], dev(d - 1)).start()

    def block(zz, xx, cc, yy):
        return zz * plane + xx * 4 + cc * 2 + yy

    def forward(b, device, lo=0, size=hxy):
        piece = ags.at[b, pl.ds(lo, size)]
        remote(piece, piece, send4, got4.at[b], device).start()

    def arrived(b):
        landed(ags.at[b], got4.at[b])

    def group(cc, zz):
        return agz.at[pl.ds((cc * n_out + zz) * 4, 4)]

    def z_share():
        landed(agz.at[pl.ds(0, 3)], got_in)
        row = group(c, z)
        for k in ZSEND:
            remote(row, row, send_g, got_gz.at[z], at(flip(z, k), x, c, y)).start()
        remote(row, row, send_g, got_gc, partner).start()

    def z_arrived(k):
        row = group(c, flip(z, k))
        landed(row, got_gz.at[flip(z, k)])
        remote(row, row, send_g, got_gc, partner).start()

    for k in ZSEND:
        forward(d, at(flip(z, k), x, c, y))

    def column(k):
        b = block(flip(z, k), x, c, y)
        if k > 0:
            arrived(b)
        forward(b, x_side)
        forward(b, y_side)
        if k in DIRECT:
            forward(b, across)
        forward(b, partner)

    def from_y(k):
        b = block(flip(z, k), x, c, 1 - y)
        arrived(b)
        if k not in DIRECT:
            forward(b, x_side, 0, half_a)
        forward(b, partner)

    def from_x(k):
        b = block(flip(z, k), 1 - x, c, y)
        arrived(b)
        if k not in DIRECT:
            forward(b, y_side, half_a, half_b)
        forward(b, partner)

    def corner(k):
        b = block(flip(z, k), 1 - x, c, 1 - y)
        arrived(b)
        forward(b, partner)

    def edges():
        @pl.when(d > 0)
        def _():
            send_edge()

        @pl.when(d == n - 1)
        def _():
            age[0] = update(step)
            for q in range(1, n):
                remote(age, age, send_e, got_e, dev(d - q)).start()

    for op in AG:
        i = int(op[1:])
        if op[0] == "c":
            column(i)
        elif op[0] == "x":
            from_x(i)
        elif op[0] == "y":
            from_y(i)
        elif op[0] == "d":
            corner(i)
        elif op[0] == "g":
            z_share()
        elif op[0] == "h":
            z_arrived(i)
        elif op[0] == "e":
            edges()

    @pl.loop(0, n_out)
    def _(k):
        for xx in range(2):
            for yy in range(2):
                arrived(block(k, xx, 1 - c, yy))

    landed(agz.at[pl.ds((1 - c) * (4 * n_out), 4 * n_out)], got_gc)

    @pl.when(d < n - 1)
    def _():
        landed(age, got_e)
        for i, ref in enumerate((nmw, nvw)):
            landed(ref.at[step], back_sem.at[2 + i])

    @pl.when(d == n - 1)
    def _():
        landed(ags.at[pl.ds(0, n - 1), 0], send_e)

    @pl.when(d > 0)
    def _():
        for i, ref in enumerate((nmw, nvw)):
            landed(ref.at[step], back_sem.at[i])

    @pl.when((z != last) | (c != 1))
    def _():
        landed(re1.at[pl.ds(0, 1)], send_e1)

    @pl.when((z == last) & (c == 1) & (x * 2 + y < 3))
    def _():
        landed(ze, send_e2)

    for ref, sem in (
        (r1x, send1x),
        (r1y, send1y),
        (r2x, send2x),
        (r2y, send2y),
        (rz1.at[pl.ds(0, 2 * n_out - 1)], sendz1),
        (rz2, sendz2),
        (recv3.at[pl.ds(0, n_out - 1)], send3),
        (stats.at[pl.ds(0, n - 1)], send_s),
        (ags.at[pl.ds(0, n - 1)], send4),
        (agz.at[pl.ds(0, n - 1)], send_g),
    ):
        landed(ref, sem)


def finish(
    plan,
    ags,
    agz,
    age,
    nmw,
    nvw,
    out_ref,
    nm_ref,
    nv_ref,
    nm_out,
    nv_out,
    out_sem,
    own_sem,
):
    n, n_spa, shard, step, span, hz = plan
    rows = span * 8
    whole = step * TILE
    hxy = step - hz
    pieces = []
    for b in range(n):
        zz, xx, cc, yy = b // 8, b // 4 % 2, b // 2 % 2, b % 2
        slot = (cc * (n // 8) + zz) * 4 + xx * 2 + yy
        pieces.append((ags.at[b], b * step, hxy))
        pieces.append((agz.at[slot], b * step + hxy, hz))
    pieces.append((age, n * step, 1))
    copies = [
        pltpu.make_async_copy(src, out_ref.at[pl.ds(first, size)], out_sem.at[i])
        for i, (src, first, size) in enumerate(pieces)
    ]
    for copy in copies:
        copy.start()
    d = lax.axis_index("replica") * n_spa + lax.axis_index("spatial")
    off = d * (shard - whole)
    shift_l = off % 128
    shift_r = off // 128
    back_l = 128 - shift_l
    lane = lax.broadcasted_iota(jnp.int32, (rows, 128), 1)
    for j, (src, buf, ref) in enumerate(((nmw, nm_out, nm_ref), (nvw, nv_out, nv_ref))):
        x = src[...].reshape(rows, 128)
        x = pltpu.roll(x, (rows - shift_r) % rows, 0)
        x = pltpu.roll(x, back_l % 128, 1)
        x = jnp.where(lane < back_l, x, pltpu.roll(x, rows - 1, 0))
        buf[pl.ds(0, whole)] = x[: step * 8].reshape(whole)
        buf[pl.ds(whole, shard - whole)] = x[step * 8, : shard - whole].reshape(shard - whole)
        copy = pltpu.make_async_copy(buf, ref, own_sem.at[j])
        copy.start()
        copies.append(copy)
    for copy in copies:
        copy.wait()


def windowed(n_rep, n_spa, grads, master, velocity, layer_offsets, layer_sizes, lars_skip):
    shard = master.shape[0]
    params = grads.shape[2]
    layers = layer_offsets.shape[0]
    plane = 8
    n = n_rep * n_spa
    n_out = n // plane
    step = shard // TILE
    span = params // TILE - (n - 1) * step
    chunk = (plane - 1) * step + span
    tiles = params // TILE
    hz = ZTILES
    hx = (step - hz + 1) // 2
    hy = step - hz - hx
    plan = (n_out, shard, step, span, layers, hx, hy, hz)
    vmem = pl.BlockSpec(memory_space=pltpu.VMEM)
    anywhere = pl.BlockSpec(memory_space=pltpu.HBM)
    f32, bf16 = jnp.float32, jnp.bfloat16
    dma = pltpu.SemaphoreType.DMA
    ags, agz, age, nmw, nvw = pl.pallas_call(
        functools.partial(kernel, plan),
        out_shape=(
            pltpu.VMEM((n, hx + hy, 8, 128), bf16),
            pltpu.VMEM((n, hz, 8, 128), bf16),
            pltpu.VMEM((1, 8, 128), bf16),
            pltpu.VMEM((span, 8, 128), f32),
            pltpu.VMEM((span, 8, 128), f32),
        ),
        in_specs=[anywhere] * 6,
        out_specs=(vmem,) * 5,
        scratch_shapes=[
            pltpu.SMEM((layers,), jnp.int32),
            pltpu.SMEM((layers,), jnp.int32),
            pltpu.SMEM((layers,), jnp.int32),
            pltpu.VMEM((shard,), f32),
            pltpu.VMEM((shard,), f32),
            pltpu.VMEM((n_out, 1, chunk * TILE), bf16),
            pltpu.VMEM((n_out, chunk, 8, 128), bf16),
            pltpu.VMEM((2, n_out, 3, hx, 8, 128), bf16),
            pltpu.VMEM((2, n_out, 3, hy, 8, 128), bf16),
            pltpu.VMEM((n_out, hx, 8, 128), f32),
            pltpu.VMEM((n_out, hy, 8, 128), f32),
            pltpu.VMEM((n_out, hx, 8, 128), f32),
            pltpu.VMEM((n_out, hy, 8, 128), f32),
            pltpu.VMEM((2 * n_out, 4, hz, 8, 128), bf16),
            pltpu.VMEM((4, hz, 8, 128), f32),
            pltpu.VMEM((3, hz, 8, 128), f32),
            pltpu.VMEM((2 * n_out, 8, 128), bf16),
            pltpu.VMEM((1, 8, 128), f32),
            pltpu.VMEM((3, 8, 128), f32),
            pltpu.VMEM((n_out, hx + hy, 8, 128), f32),
            pltpu.VMEM((n_out, hx + hy, 8, 128), f32),
            pltpu.VMEM((span, 2, 8, 128), f32),
            pltpu.VMEM((2, 8, 128), f32),
            pltpu.VMEM((span, 8, 128), f32),
            pltpu.VMEM((1, 128), f32),
            pltpu.VMEM((n, 1, 128), f32),
            dma((n_out,)),
            dma((2,)),
            dma((3,)),
            pltpu.SemaphoreType.REGULAR((n_out,)),
            dma(()),
            dma((2, n_out)),
            dma(()),
            dma((2, n_out)),
            dma(()),
            dma((n_out,)),
            dma(()),
            dma((n_out,)),
            dma(()),
            dma(()),
            dma(()),
            dma(()),
            dma(()),
            dma(()),
            dma(()),
            dma(()),
            dma(()),
            dma(()),
            dma((2,)),
            dma(()),
            dma(()),
            dma(()),
            dma((n,)),
            dma(()),
            dma(()),
            dma((n_out,)),
            dma(()),
            dma(()),
            dma(()),
            dma((4,)),
        ],
        compiler_params=pltpu.CompilerParams(
            collective_id=0, has_side_effects=True, vmem_limit_bytes=61 * 2**20
        ),
    )(grads, master, velocity, layer_offsets, layer_sizes, lars_skip)
    weights, nm, nv = pl.pallas_call(
        functools.partial(finish, (n, n_spa, shard, step, span, hz)),
        out_shape=(
            jax.ShapeDtypeStruct((tiles, 8, 128), bf16),
            jax.ShapeDtypeStruct((shard,), f32),
            jax.ShapeDtypeStruct((shard,), f32),
        ),
        in_specs=[vmem] * 5,
        out_specs=(anywhere, anywhere, anywhere),
        scratch_shapes=[
            pltpu.VMEM((shard,), f32),
            pltpu.VMEM((shard,), f32),
            dma((2 * n + 1,)),
            dma((2,)),
        ],
        compiler_params=pltpu.CompilerParams(vmem_limit_bytes=16 * 2**20),
    )(ags, agz, age, nmw, nvw)
    return weights.reshape(params), nm, nv


def tiled(n_rep, n_spa, params):
    n = n_rep * n_spa
    shard = params // n
    rest = shard % TILE
    n_out = n_rep // 4
    return (
        n_spa == 2
        and n_rep % 4 == 0
        and n_out >= 2
        and n_out & (n_out - 1) == 0
        and params % TILE == 0
        and shard >= TILE
        and 0 < n * rest <= TILE
        and rest <= 128
    )


def step_fn(n_rep, n_spa, grads, *rest):
    if tiled(n_rep, n_spa, grads.shape[2]):
        return windowed(n_rep, n_spa, grads, *rest)
    return shards(grads, *rest)


def shards(grads, master, velocity, layer_offsets, layer_sizes, lars_skip):
    n_rep = lax.axis_size("replica")
    n_spa = lax.axis_size("spatial")
    shard = master.shape[0]
    position = lax.axis_index(("replica", "spatial")) * shard + jnp.arange(shard, dtype=jnp.int32)
    inside = (position[None, :] >= layer_offsets[:, None]) & (
        position[None, :] < (layer_offsets + layer_sizes)[:, None]
    )
    onehot = inside.astype(jnp.float32)
    received = lax.all_to_all(
        grads[0, 0].reshape(n_rep, n_spa * shard),
        "replica",
        split_axis=0,
        concat_axis=0,
        tiled=True,
    )
    first = jnp.sum(received.astype(jnp.float32), axis=0)
    summed = lax.psum_scatter(
        first.reshape(n_spa, shard), "spatial", scatter_dimension=0, tiled=True
    )
    grad = summed.reshape(shard) / (n_rep * n_spa)
    gsq_local = jnp.dot(onehot, grad * grad, precision=lax.Precision.HIGHEST)
    wsq_local = jnp.dot(onehot, master * master, precision=lax.Precision.HIGHEST)
    wsq, gsq = lax.psum((wsq_local, gsq_local), ("replica", "spatial"))
    wnorm = jnp.sqrt(wsq)
    gnorm = jnp.sqrt(gsq)
    skipped = lars_skip.astype(jnp.float32)
    ratio = 0.02 * wnorm / (gnorm + 0.001 * wnorm + 1e-06)
    trust = skipped + (1.0 - skipped) * ratio
    decay = (1.0 - skipped) * 0.001
    trust_pos = jnp.dot(trust, onehot, precision=lax.Precision.HIGHEST)
    decay_pos = jnp.dot(decay, onehot, precision=lax.Precision.HIGHEST)
    new_velocity = 0.9 * velocity + 8.0 * trust_pos * (grad + decay_pos * master)
    new_master = master - new_velocity
    new_weights = lax.all_gather(
        new_master.astype(jnp.bfloat16), ("replica", "spatial"), axis=0, tiled=True
    )
    return (new_weights, new_master, new_velocity)


def solution(mesh):
    return jax.shard_map(
        functools.partial(step_fn, mesh.shape["replica"], mesh.shape["spatial"]),
        mesh=mesh,
        in_specs=(
            P("replica", "spatial", None),
            P(("replica", "spatial")),
            P(("replica", "spatial")),
            P(),
            P(),
            P(),
        ),
        out_specs=(P(), P(("replica", "spatial")), P(("replica", "spatial"))),
        check_vma=False,
    )
```

```python
import functools

import jax
import jax.numpy as jnp
from jax import lax
from jax.experimental import pallas as pl
from jax.experimental.pallas import tpu as pltpu
from jax.sharding import PartitionSpec as P

MESH = pl.DeviceIdType.MESH
TILE = 1024
ZTILES = 4
PIECES = 8
XOR = (2, 3, 1, 0)
RS = (
    "k1", "bar", "A1", "B1", "k2", "A2", "k3", "k4", "z1", "z2", "z3", "mv", "s1", "B2", "A3",
    "s2", "p1", "B3", "A4", "s3", "p2", "B4", "Z", "s4", "p3", "p4",
)
ZSEND = (1, 2, 3)
AG = (
    "c0", "c1", "g0", "x0", "y0", "c2", "e0", "c3", "x1", "y1", "d0", "x2", "y2", "d1", "h1",
    "h2", "h3", "x3", "y3", "d2", "d3",
)
DIRECT = (0, 3)


def flip(i, k):
    out, bit = 0, 1
    while bit <= k:
        b = (i // bit) % 2
        out = out + bit * (1 - 2 * b) * ((k // bit) % 2)
        bit *= 2
    return i + out


def kernel(
    plan,
    grads_ref,
    m_ref,
    v_ref,
    offsets_in,
    sizes_in,
    skip_in,
    ags,
    age,
    nmw,
    nvw,
    offsets_ref,
    sizes_ref,
    skip_ref,
    m_in,
    v_in,
    gin,
    packed,
    r1x,
    r1y,
    sx,
    sy,
    r2x,
    r2y,
    rz1,
    zs,
    rz2,
    re1,
    ze,
    re2,
    part,
    recv3,
    mv,
    halo,
    grad_buf,
    layer_of,
    nvw_pre,
    step_pre,
    wrow,
    stats,
    in_sem,
    mv_sem,
    table_sem,
    ready,
    send1x,
    got1x,
    send1y,
    got1y,
    send2x,
    got2x,
    send2y,
    got2y,
    sendz1,
    gotz1,
    sendz2,
    gotz2,
    send_e1,
    got_e1,
    send_e2,
    got_e2,
    send3,
    got3,
    halo_sem,
    send_s,
    got_s,
    send4,
    got4,
    send_g,
    got_in,
    got_gz,
    got_gc,
    send_e,
    got_e,
    back_sem,
):
    n_out, shard, step, span, layers, hx, hy, hz = plan
    plane = 8
    n = n_out * plane
    chunk = (plane - 1) * step + span
    rows = span * 8
    hxy = hx + hy
    last = n_out - 1
    half_a = (hxy + 1) // 2
    half_b = hxy - half_a
    r = lax.axis_index("replica")
    y = lax.axis_index("spatial")
    d = r * 2 + y
    z = d // plane
    p = d % plane
    x = p // 4
    c = (p // 2) % 2
    base = d * (step * TILE)
    off = d * (shard - step * TILE)

    def dev(flat):
        return (flat // 2, flat % 2)

    def at(zz, xx, cc, yy):
        return ((zz * 2 + xx) * 2 + cc, yy)

    barrier = pltpu.get_barrier_semaphore()

    def load(zt):
        start = pl.multiple_of(zt * (plane * step * TILE), TILE)
        return pltpu.make_async_copy(
            grads_ref.at[0, :, pl.ds(start, chunk * TILE)], gin.at[zt], in_sem.at[zt]
        )

    order = [(z + k) % n_out for k in range(1, n_out + 1)]
    if XOR:
        order = [flip(z, k) for k in XOR]
    for zt in order:
        load(zt).start()
    mv_loads = [
        pltpu.make_async_copy(ref, buf, mv_sem.at[j])
        for j, (ref, buf) in enumerate(((m_ref, m_in), (v_ref, v_in)))
    ]
    tables = [
        pltpu.make_async_copy(ref, buf, table_sem.at[j])
        for j, (ref, buf) in enumerate(
            ((offsets_in, offsets_ref), (sizes_in, sizes_ref), (skip_in, skip_ref))
        )
    ]
    for copy in mv_loads + tables:
        copy.start()

    def signal(sem, device):
        pl.semaphore_signal(sem, inc=1, device_id=device, device_id_type=MESH)

    def signal_z(sem, cores):
        @pl.when(z > 0)
        def _():
            for cc in cores:
                signal(sem, at(z - 1, x, cc, y))

        @pl.when(z < n_out - 1)
        def _():
            for cc in cores:
                signal(sem, at(z + 1, x, cc, y))

    n_z = jnp.where(z > 0, 1, 0) + jnp.where(z < n_out - 1, 1, 0)
    for device in (
        at(z, x, 1 - c, y),
        at(z, 1 - x, c, y),
        at(z, x, c, 1 - y),
        at(z, 1 - x, 1 - c, y),
        at(z, x, 1 - c, 1 - y),
    ):
        signal(barrier, device)
    signal_z(barrier, (c, 1 - c))

    group = max(g for g in range(1, 33) if chunk % g == 0)

    def pack(k):
        zt = order[k - 1]
        load(zt).wait()
        @pl.loop(0, chunk // group)
        def _(i):
            first = pl.multiple_of(i * (group * TILE), group * TILE)
            v = gin[zt, :, pl.ds(first, group * TILE)].astype(jnp.float32)
            packed[zt, pl.ds(i * group, group)] = v.reshape(group, 8, 128).astype(jnp.bfloat16)

    def remote(src, dst, send, recv, device):
        return pltpu.make_async_remote_copy(
            src_ref=src,
            dst_ref=dst,
            send_sem=send,
            recv_sem=recv,
            device_id=device,
            device_id_type=MESH,
        )

    def landed(ref, sem):
        pltpu.make_async_copy(ref, ref, sem).wait()

    def first(xx, cc, yy):
        return (xx * 4 + cc * 2 + yy) * step

    def send_raw(zt, h):
        yb, xb = (y, x) if h else (1 - y, 1 - x)
        for m in (3, 2, 1):
            xx, cc = (1 - x if m >= 2 else x), (1 - c if m % 2 else c)
            remote(
                packed.at[zt, pl.ds(first(xx, cc, yb), hx)],
                r1x.at[h, zt, m - 1],
                send1x,
                got1x.at[h, zt],
                at(z, xx, cc, y),
            ).start()
            yy = 1 - y if m >= 2 else y
            remote(
                packed.at[zt, pl.ds(first(xb, cc, yy) + hx, hy)],
                r1y.at[h, zt, m - 1],
                send1y,
                got1y.at[h, zt],
                at(z, x, cc, yy),
            ).start()

    def raws(zt, h, t, r1, own):
        v = packed[zt, own + t].astype(jnp.float32) + r1[h, zt, 0, t].astype(jnp.float32)
        return v + (r1[h, zt, 1, t].astype(jnp.float32) + r1[h, zt, 2, t].astype(jnp.float32))

    def sum_raw(zt):
        landed(r1x.at[0, zt], got1x.at[0, zt])
        own = first(x, c, 1 - y)

        @pl.loop(0, hx, unroll=2)
        def _(t):
            sx[zt, t] = raws(zt, 0, t, r1x, own)

        remote(sx.at[zt], r2x.at[zt], send2x, got2x.at[zt], at(z, x, c, 1 - y)).start()
        landed(r1y.at[0, zt], got1y.at[0, zt])
        own2 = first(1 - x, c, y) + hx

        @pl.loop(0, hy, unroll=2)
        def _(t):
            sy[zt, t] = raws(zt, 0, t, r1y, own2)

        remote(sy.at[zt], r2y.at[zt], send2y, got2y.at[zt], at(z, 1 - x, c, y)).start()

    def copy3(zt, src):
        return remote(part.at[zt], recv3.at[src], send3, got3, at(zt, x, c, y))

    def sum_plane(zt):
        own = first(x, c, y)
        landed(r1x.at[1, zt], got1x.at[1, zt])
        landed(r2x.at[zt], got2x.at[zt])

        @pl.loop(0, hx, unroll=2)
        def _(t):
            part[zt, t] = raws(zt, 1, t, r1x, own) + r2x[zt, t]

        landed(r1y.at[1, zt], got1y.at[1, zt])
        landed(r2y.at[zt], got2y.at[zt])

        @pl.loop(0, hy, unroll=2)
        def _(t):
            part[zt, hx + t] = raws(zt, 1, t, r1y, own + hx) + r2y[zt, t]

    def send_far(zt, other):
        cc = 1 - c if other else c
        for j in range(4):
            remote(
                packed.at[zt, pl.ds(first(j // 2, cc, j % 2) + hxy, hz)],
                rz1.at[other * n_out + z, j],
                sendz1,
                gotz1,
                at(zt, x, cc, y),
            ).start()

        @pl.when((zt == last) & (cc == 1))
        def _():
            remote(
                packed.at[last, pl.ds(chunk - 1, 1)],
                re1.at[pl.ds(z * 2 + c, 1)],
                send_e1,
                got_e1,
                at(zt, x, cc, y),
            ).start()

    def send_distance(j):
        @pl.when(z >= j)
        def _():
            for other in (0, 1):
                send_far(z - j, other)

        @pl.when(z < n_out - j)
        def _():
            for other in (0, 1):
                send_far(z + j, other)

    def sum_far():
        landed(rz1.at[pl.ds(0, 2 * n_out - 1)], gotz1)

        @pl.loop(0, 4)
        def _(j):
            own = first(j // 2, c, j % 2) + hxy
            for t in range(hz):
                acc = packed[z, own + t].astype(jnp.float32)
                acc = acc + rz1[n_out + z, j, t].astype(jnp.float32)
                for k in range(1, n_out):
                    zz = (z + k) % n_out
                    two = rz1[zz, j, t].astype(jnp.float32)
                    acc = acc + (two + rz1[n_out + zz, j, t].astype(jnp.float32))
                zs[j, t] = acc

        for m in (3, 2, 1):
            xx, yy = (1 - x if m >= 2 else x), (1 - y if m % 2 else y)
            remote(zs.at[xx * 2 + yy], rz2.at[m - 1], sendz2, gotz2, at(z, xx, c, yy)).start()

        @pl.when((z == last) & (c == 1))
        def _():
            landed(re1.at[pl.ds(0, 2 * n_out - 1)], got_e1)
            acc = packed[last, chunk - 1].astype(jnp.float32)
            for j in range(2 * n_out - 1):
                acc = acc + re1[j].astype(jnp.float32)
            ze[0] = acc

            @pl.when(x * 2 + y < 3)
            def _():
                remote(
                    ze, re2.at[pl.ds(x * 2 + y, 1)], send_e2, got_e2, at(z, 1, 1, 1)
                ).start()

    lane = lax.broadcasted_iota(jnp.int32, (rows, 128), 1)
    shift_l = off % 128
    shift_r = off // 128
    whole = step * TILE

    def window(j, ref):
        mv_loads[j].wait()
        edge = jnp.pad(ref[pl.ds(whole, shard - whole)], (0, 128 - (shard - whole)))
        edge = jnp.broadcast_to(edge.reshape(1, 128), (8, 128))
        w = jnp.concatenate([ref[pl.ds(0, whole)].reshape(step * 8, 128), edge], 0)
        w = pltpu.roll(w, shift_l, 1)
        w = jnp.where(lane < shift_l, pltpu.roll(w, 1, 0), w)
        w = pltpu.roll(w, shift_r, 0)
        mv[:, j] = w.reshape(span, 8, 128)

    place = lax.broadcasted_iota(jnp.int32, (8, 128), 0) * 128 + lax.broadcasted_iota(
        jnp.int32, (8, 128), 1
    )
    low, high, own_low, own_high = [], [], [], []

    def bounds():
        for copy in tables:
            copy.wait()
        for l in range(layers):
            low.append(offsets_ref[l] - base)
            high.append(offsets_ref[l] + sizes_ref[l] - base)
            own_low.append(jnp.maximum(low[l], off))
            own_high.append(jnp.minimum(high[l], off + shard))

    lane1 = lax.broadcasted_iota(jnp.int32, (1, 128), 1)

    def squares(value, start, stop, lows, highs, sums=None):
        def add(t, accs):
            pos = place + t * TILE
            v = value(t)
            v = v * v
            return tuple(
                acc + jnp.where((pos >= lo) & (pos < hi), v, 0.0)
                for acc, lo, hi in zip(accs, lows, highs)
            )

        if sums is None:
            sums = tuple(jnp.zeros((8, 128), jnp.float32) for _ in range(layers))
        return lax.fori_loop(start, stop, add, sums)

    def as_row(sums, first):
        row = jnp.zeros((1, 128), jnp.float32)
        for l, acc in enumerate(sums):
            row = jnp.where(lane1 == first + l, jnp.sum(acc, axis=(0, 1), keepdims=True), row)
        return row

    def step_z(j):
        if j == 1:
            send_distance(1)
            send_far(z, 1)
            return
        pl.semaphore_wait(ready.at[j - 2], n_z)
        if j < n_out - 1:
            signal_z(ready.at[j - 1], (c,))
        send_distance(j)

    for op in RS:
        i = int(op[1:] or 0) if op != "bar" and op != "mv" else 0
        zt = order[i - 1]
        if op == "bar":
            pl.semaphore_wait(barrier, 5 + 2 * n_z)
            signal_z(ready.at[0], (c,))
        elif op == "mv":
            bounds()
            for j, ref in enumerate((m_in, v_in)):
                window(j, ref)
            wrow[...] = as_row(squares(lambda t: mv[t, 0], 0, span, own_low, own_high), 0)
        elif op[0] == "k":
            pack(i)
        elif op[0] == "A":
            send_raw(zt, 0)
        elif op[0] == "B":
            send_raw(zt, 1)
        elif op[0] == "z":
            step_z(i)
        elif op[0] == "Z":
            sum_far()
        elif op[0] == "s":
            sum_raw(zt)
        elif op[0] == "p":
            sum_plane(zt)
            if i < n_out:
                copy3(zt, z).start()

    landed(recv3.at[pl.ds(0, n_out - 1)], got3)
    halo_copy = remote(mv.at[span - 1], halo, halo_sem.at[0], halo_sem.at[1], dev((d + 1) % n))
    halo_copy.start()
    landed(rz2, gotz2)
    for t in range(hz):
        acc = zs[x * 2 + y, t] + rz2[0, t]
        grad_buf[hxy + t] = (acc + (rz2[1, t] + rz2[2, t])) / n
    grad_buf[step] = jnp.zeros((8, 128), jnp.float32)

    @pl.when(d == n - 1)
    def _():
        landed(re2, got_e2)
        grad_buf[step] = (ze[0] + re2[0] + (re2[1] + re2[2])) / n

    def total_grad(t):
        acc = part[z, t]
        for k in range(1, n_out):
            acc = acc + recv3[(z + k) % n_out, t]
        acc = acc / n
        grad_buf[t] = acc
        return acc

    sums = squares(total_grad, 0, hxy, low, high)
    sums = squares(lambda t: grad_buf[t], hxy, span, low, high, sums)
    stats[d] = as_row(sums, layers) + wrow[...]

    for k in range(n_out - 1, -1, -1):
        for q in range(plane - 1, -1, -1):
            if k + q > 0:
                peer = flip(z, k) * plane + flip(p, q)
                remote(stats.at[d], stats.at[d], send_s, got_s, dev(peer)).start()

    skip_row = jnp.zeros((1, 128), jnp.float32)
    for l in range(layers):
        skip_row = jnp.where(lane1 == l, skip_ref[l].astype(jnp.float32), skip_row)

    def prepare(t):
        pos = place + t * TILE
        which = jnp.zeros((8, 128), jnp.int32)
        decay = jnp.zeros((8, 128), jnp.float32)
        for l in range(layers):
            inside = (pos >= low[l]) & (pos < high[l])
            which = jnp.where(inside, l, which)
            decay = jnp.where(inside, (1.0 - skip_ref[l].astype(jnp.float32)) * 0.001, decay)
        layer_of[t] = which
        nvw_pre[t] = 0.9 * mv[t, 1]
        step_pre[t] = 8.0 * (grad_buf[t] + decay * mv[t, 0])

    @pl.loop(1, span)
    def _(t):
        prepare(t)

    halo_copy.wait()
    for j in range(2):
        mv[0, j] = jnp.where(place < off, halo[j], mv[0, j])
    prepare(0)

    landed(stats.at[pl.ds(0, n - 1)], got_s)
    norms = jnp.sqrt(jnp.sum(stats[...], axis=0))
    wnorm = jnp.broadcast_to(norms, (8, 128))
    gnorm = pltpu.roll(wnorm, 128 - layers, 1)
    ratio = 0.02 * wnorm / (gnorm + 0.001 * wnorm + 1e-06)
    trust_row = skip_row + (1.0 - skip_row) * ratio
    trust = [
        jnp.sum(jnp.where(lane1 == l, trust_row, 0.0), axis=1, keepdims=True)
        for l in range(layers)
    ]

    def update(t):
        which = layer_of[t]
        trust_pos = jnp.broadcast_to(trust[0], (8, 128))
        for l in range(1, layers):
            trust_pos = jnp.where(which == l, trust[l], trust_pos)
        nv = nvw_pre[t] + trust_pos * step_pre[t]
        nm = mv[t, 0] - nv
        nvw[t] = nv
        nmw[t] = nm
        return nm.astype(jnp.bfloat16)

    x_side = at(z, 1 - x, c, y)
    y_side = at(z, x, c, 1 - y)
    across = at(z, 1 - x, c, 1 - y)
    partner = at(z, x, 1 - c, y)

    def share(b):
        return ags.at[b, pl.ds(hxy, hz)]

    for t in range(hz):
        ags[d, hxy + t] = update(hxy + t)
    for device in (across, x_side, y_side):
        remote(share(d), share(d), send_g, got_in, device).start()

    @pl.loop(0, hxy)
    def _(t):
        ags[d, t] = update(t)

    def send_edge():
        for i, ref in enumerate((nmw, nvw)):
            remote(ref.at[0], ref.at[step], back_sem.at[i], back_sem.at[2 + i], dev(d - 1)).start()

    def block(zz, xx, cc, yy):
        return zz * plane + xx * 4 + cc * 2 + yy

    def forward(b, device, lo=0, size=hxy):
        piece = ags.at[b, pl.ds(lo, size)]
        remote(piece, piece, send4, got4.at[b], device).start()

    def arrived(b):
        landed(ags.at[b, pl.ds(0, hxy)], got4.at[b])

    def tiles(count):
        return ags.at[pl.ds(0, count), pl.ds(0, hz)]

    def z_share():
        landed(tiles(3), got_in)
        for j in range(4):
            b = block(z, j // 2, c, j % 2)
            for k in ZSEND:
                peer = at(flip(z, k), x, c, y)
                remote(share(b), share(b), send_g, got_gz.at[z], peer).start()
            remote(share(b), share(b), send_g, got_gc, partner).start()

    def z_arrived(k):
        landed(tiles(4), got_gz.at[flip(z, k)])
        for j in range(4):
            b = block(flip(z, k), j // 2, c, j % 2)
            remote(share(b), share(b), send_g, got_gc, partner).start()

    for k in ZSEND:
        forward(d, at(flip(z, k), x, c, y))

    def column(k):
        b = block(flip(z, k), x, c, y)
        if k > 0:
            arrived(b)
        forward(b, x_side)
        forward(b, y_side)
        if k in DIRECT:
            forward(b, across)
        forward(b, partner)

    def from_y(k):
        b = block(flip(z, k), x, c, 1 - y)
        arrived(b)
        if k not in DIRECT:
            forward(b, x_side, 0, half_a)
        forward(b, partner)

    def from_x(k):
        b = block(flip(z, k), 1 - x, c, y)
        arrived(b)
        if k not in DIRECT:
            forward(b, y_side, half_a, half_b)
        forward(b, partner)

    def corner(k):
        b = block(flip(z, k), 1 - x, c, 1 - y)
        arrived(b)
        forward(b, partner)

    def edges():
        @pl.when(d > 0)
        def _():
            send_edge()

        @pl.when(d == n - 1)
        def _():
            age[0] = update(step)
            for q in range(1, n):
                remote(age, age, send_e, got_e, dev(d - q)).start()

    for op in AG:
        i = int(op[1:])
        if op[0] == "c":
            column(i)
        elif op[0] == "x":
            from_x(i)
        elif op[0] == "y":
            from_y(i)
        elif op[0] == "d":
            corner(i)
        elif op[0] == "g":
            z_share()
        elif op[0] == "h":
            z_arrived(i)
        elif op[0] == "e":
            edges()

    @pl.loop(0, n_out)
    def _(k):
        for xx in range(2):
            for yy in range(2):
                arrived(block(k, xx, 1 - c, yy))

    landed(tiles(4 * n_out), got_gc)

    @pl.when(d < n - 1)
    def _():
        landed(age, got_e)
        for i, ref in enumerate((nmw, nvw)):
            landed(ref.at[step], back_sem.at[2 + i])

    @pl.when(d == n - 1)
    def _():
        landed(ags.at[pl.ds(0, n - 1), 0], send_e)

    @pl.when(d > 0)
    def _():
        for i, ref in enumerate((nmw, nvw)):
            landed(ref.at[step], back_sem.at[i])

    @pl.when((z != last) | (c != 1))
    def _():
        landed(re1.at[pl.ds(0, 1)], send_e1)

    @pl.when((z == last) & (c == 1) & (x * 2 + y < 3))
    def _():
        landed(ze, send_e2)

    for ref, sem in (
        (r1x, send1x),
        (r1y, send1y),
        (r2x, send2x),
        (r2y, send2y),
        (rz1.at[pl.ds(0, 2 * n_out - 1)], sendz1),
        (rz2, sendz2),
        (recv3.at[pl.ds(0, n_out - 1)], send3),
        (stats.at[pl.ds(0, n - 1)], send_s),
        (ags.at[pl.ds(0, n - 1), pl.ds(0, hxy)], send4),
        (tiles(n - 1), send_g),
    ):
        landed(ref, sem)


def finish(
    plan,
    ags,
    age,
    nmw,
    nvw,
    out_ref,
    nm_ref,
    nv_ref,
    nm_out,
    nv_out,
    out_sem,
    own_sem,
):
    n, n_spa, shard, step, span = plan
    rows = span * 8
    whole = step * TILE
    part = n * step // PIECES
    copies = [
        pltpu.make_async_copy(
            ags.at[pl.ds(i * part, part)], out_ref.at[pl.ds(i * part, part)], out_sem.at[i]
        )
        for i in range(PIECES)
    ]
    copies.append(
        pltpu.make_async_copy(age, out_ref.at[pl.ds(n * step, 1)], out_sem.at[PIECES])
    )
    for copy in copies:
        copy.start()
    d = lax.axis_index("replica") * n_spa + lax.axis_index("spatial")
    off = d * (shard - whole)
    shift_l = off % 128
    shift_r = off // 128
    back_l = 128 - shift_l
    lane = lax.broadcasted_iota(jnp.int32, (rows, 128), 1)
    for j, (src, buf, ref) in enumerate(((nmw, nm_out, nm_ref), (nvw, nv_out, nv_ref))):
        x = src[...].reshape(rows, 128)
        x = pltpu.roll(x, (rows - shift_r) % rows, 0)
        x = pltpu.roll(x, back_l % 128, 1)
        x = jnp.where(lane < back_l, x, pltpu.roll(x, rows - 1, 0))
        buf[pl.ds(0, whole)] = x[: step * 8].reshape(whole)
        buf[pl.ds(whole, shard - whole)] = x[step * 8, : shard - whole].reshape(shard - whole)
        copy = pltpu.make_async_copy(buf, ref, own_sem.at[j])
        copy.start()
        copies.append(copy)
    for copy in copies:
        copy.wait()


def windowed(n_rep, n_spa, grads, master, velocity, layer_offsets, layer_sizes, lars_skip):
    shard = master.shape[0]
    params = grads.shape[2]
    layers = layer_offsets.shape[0]
    plane = 8
    n = n_rep * n_spa
    n_out = n // plane
    step = shard // TILE
    span = params // TILE - (n - 1) * step
    chunk = (plane - 1) * step + span
    tiles = params // TILE
    hz = ZTILES
    hx = (step - hz + 1) // 2
    hy = step - hz - hx
    plan = (n_out, shard, step, span, layers, hx, hy, hz)
    vmem = pl.BlockSpec(memory_space=pltpu.VMEM)
    anywhere = pl.BlockSpec(memory_space=pltpu.HBM)
    f32, bf16 = jnp.float32, jnp.bfloat16
    dma = pltpu.SemaphoreType.DMA
    ags, age, nmw, nvw = pl.pallas_call(
        functools.partial(kernel, plan),
        out_shape=(
            pltpu.VMEM((n, step, 8, 128), bf16),
            pltpu.VMEM((1, 8, 128), bf16),
            pltpu.VMEM((span, 8, 128), f32),
            pltpu.VMEM((span, 8, 128), f32),
        ),
        in_specs=[anywhere] * 6,
        out_specs=(vmem,) * 4,
        scratch_shapes=[
            pltpu.SMEM((layers,), jnp.int32),
            pltpu.SMEM((layers,), jnp.int32),
            pltpu.SMEM((layers,), jnp.int32),
            pltpu.VMEM((shard,), f32),
            pltpu.VMEM((shard,), f32),
            pltpu.VMEM((n_out, 1, chunk * TILE), bf16),
            pltpu.VMEM((n_out, chunk, 8, 128), bf16),
            pltpu.VMEM((2, n_out, 3, hx, 8, 128), bf16),
            pltpu.VMEM((2, n_out, 3, hy, 8, 128), bf16),
            pltpu.VMEM((n_out, hx, 8, 128), f32),
            pltpu.VMEM((n_out, hy, 8, 128), f32),
            pltpu.VMEM((n_out, hx, 8, 128), f32),
            pltpu.VMEM((n_out, hy, 8, 128), f32),
            pltpu.VMEM((2 * n_out, 4, hz, 8, 128), bf16),
            pltpu.VMEM((4, hz, 8, 128), f32),
            pltpu.VMEM((3, hz, 8, 128), f32),
            pltpu.VMEM((2 * n_out, 8, 128), bf16),
            pltpu.VMEM((1, 8, 128), f32),
            pltpu.VMEM((3, 8, 128), f32),
            pltpu.VMEM((n_out, hx + hy, 8, 128), f32),
            pltpu.VMEM((n_out, hx + hy, 8, 128), f32),
            pltpu.VMEM((span, 2, 8, 128), f32),
            pltpu.VMEM((2, 8, 128), f32),
            pltpu.VMEM((span, 8, 128), f32),
            pltpu.VMEM((span, 8, 128), jnp.int32),
            pltpu.VMEM((span, 8, 128), f32),
            pltpu.VMEM((span, 8, 128), f32),
            pltpu.VMEM((1, 128), f32),
            pltpu.VMEM((n, 1, 128), f32),
            dma((n_out,)),
            dma((2,)),
            dma((3,)),
            pltpu.SemaphoreType.REGULAR((n_out,)),
            dma(()),
            dma((2, n_out)),
            dma(()),
            dma((2, n_out)),
            dma(()),
            dma((n_out,)),
            dma(()),
            dma((n_out,)),
            dma(()),
            dma(()),
            dma(()),
            dma(()),
            dma(()),
            dma(()),
            dma(()),
            dma(()),
            dma(()),
            dma(()),
            dma((2,)),
            dma(()),
            dma(()),
            dma(()),
            dma((n,)),
            dma(()),
            dma(()),
            dma((n_out,)),
            dma(()),
            dma(()),
            dma(()),
            dma((4,)),
        ],
        compiler_params=pltpu.CompilerParams(
            collective_id=0, has_side_effects=True, vmem_limit_bytes=61 * 2**20
        ),
    )(grads, master, velocity, layer_offsets, layer_sizes, lars_skip)
    weights, nm, nv = pl.pallas_call(
        functools.partial(finish, (n, n_spa, shard, step, span)),
        out_shape=(
            jax.ShapeDtypeStruct((tiles, 8, 128), bf16),
            jax.ShapeDtypeStruct((shard,), f32),
            jax.ShapeDtypeStruct((shard,), f32),
        ),
        in_specs=[vmem] * 4,
        out_specs=(anywhere, anywhere, anywhere),
        scratch_shapes=[
            pltpu.VMEM((shard,), f32),
            pltpu.VMEM((shard,), f32),
            dma((PIECES + 1,)),
            dma((2,)),
        ],
        compiler_params=pltpu.CompilerParams(vmem_limit_bytes=16 * 2**20),
    )(ags.reshape(n * step, 8, 128), age, nmw, nvw)
    return weights.reshape(params), nm, nv


def tiled(n_rep, n_spa, params):
    n = n_rep * n_spa
    shard = params // n
    rest = shard % TILE
    n_out = n_rep // 4
    return (
        n_spa == 2
        and n_rep % 4 == 0
        and n_out >= 2
        and n_out & (n_out - 1) == 0
        and params % TILE == 0
        and shard >= TILE
        and 0 < n * rest <= TILE
        and rest <= 128
    )


def step_fn(n_rep, n_spa, grads, *rest):
    if tiled(n_rep, n_spa, grads.shape[2]):
        return windowed(n_rep, n_spa, grads, *rest)
    return shards(grads, *rest)


def shards(grads, master, velocity, layer_offsets, layer_sizes, lars_skip):
    n_rep = lax.axis_size("replica")
    n_spa = lax.axis_size("spatial")
    shard = master.shape[0]
    position = lax.axis_index(("replica", "spatial")) * shard + jnp.arange(shard, dtype=jnp.int32)
    inside = (position[None, :] >= layer_offsets[:, None]) & (
        position[None, :] < (layer_offsets + layer_sizes)[:, None]
    )
    onehot = inside.astype(jnp.float32)
    received = lax.all_to_all(
        grads[0, 0].reshape(n_rep, n_spa * shard),
        "replica",
        split_axis=0,
        concat_axis=0,
        tiled=True,
    )
    first = jnp.sum(received.astype(jnp.float32), axis=0)
    summed = lax.psum_scatter(
        first.reshape(n_spa, shard), "spatial", scatter_dimension=0, tiled=True
    )
    grad = summed.reshape(shard) / (n_rep * n_spa)
    gsq_local = jnp.dot(onehot, grad * grad, precision=lax.Precision.HIGHEST)
    wsq_local = jnp.dot(onehot, master * master, precision=lax.Precision.HIGHEST)
    wsq, gsq = lax.psum((wsq_local, gsq_local), ("replica", "spatial"))
    wnorm = jnp.sqrt(wsq)
    gnorm = jnp.sqrt(gsq)
    skipped = lars_skip.astype(jnp.float32)
    ratio = 0.02 * wnorm / (gnorm + 0.001 * wnorm + 1e-06)
    trust = skipped + (1.0 - skipped) * ratio
    decay = (1.0 - skipped) * 0.001
    trust_pos = jnp.dot(trust, onehot, precision=lax.Precision.HIGHEST)
    decay_pos = jnp.dot(decay, onehot, precision=lax.Precision.HIGHEST)
    new_velocity = 0.9 * velocity + 8.0 * trust_pos * (grad + decay_pos * master)
    new_master = master - new_velocity
    new_weights = lax.all_gather(
        new_master.astype(jnp.bfloat16), ("replica", "spatial"), axis=0, tiled=True
    )
    return (new_weights, new_master, new_velocity)


def solution(mesh):
    return jax.shard_map(
        functools.partial(step_fn, mesh.shape["replica"], mesh.shape["spatial"]),
        mesh=mesh,
        in_specs=(
            P("replica", "spatial", None),
            P(("replica", "spatial")),
            P(("replica", "spatial")),
            P(),
            P(),
            P(),
        ),
        out_specs=(P(), P(("replica", "spatial")), P(("replica", "spatial"))),
        check_vma=False,
    )
```

```python
import functools

import jax
import jax.numpy as jnp
from jax import lax
from jax.experimental import pallas as pl
from jax.experimental.pallas import tpu as pltpu
from jax.sharding import PartitionSpec as P

MESH = pl.DeviceIdType.MESH
TILE = 1024
ZTILES = 4
SHARE = 6
PIECES = 8
RS = (
    "k1", "bar", "A1", "B1", "k2", "A2", "k3", "k4", "z1", "z2", "z3", "mv", "s1", "B2", "A3",
    "s2", "p1", "B3", "A4", "s3", "p2", "B4", "s4", "Z", "p3", "p4",
)
ZSEND = (1, 2, 3)
AG = (
    "c0", "c1", "g0", "x0", "y0", "c2", "e0", "c3", "x1", "y1", "d0", "x2", "y2", "d1", "h1",
    "h2", "h3", "x3", "y3", "d2", "d3",
)
DIRECT = (0, 1, 2, 3)


def flip(i, k):
    out, bit = 0, 1
    while bit <= k:
        b = (i // bit) % 2
        out = out + bit * (1 - 2 * b) * ((k // bit) % 2)
        bit *= 2
    return i + out


def kernel(
    plan,
    grads_ref,
    m_ref,
    v_ref,
    offsets_in,
    sizes_in,
    skip_in,
    ags,
    age,
    nmw,
    nvw,
    offsets_ref,
    sizes_ref,
    skip_ref,
    m_in,
    v_in,
    gin,
    packed,
    r1x,
    r1y,
    sx,
    sy,
    r2x,
    r2y,
    rz1,
    zs,
    rz2,
    re1,
    ze,
    re2,
    part,
    recv3,
    mv,
    halo,
    grad_buf,
    layer_of,
    nvw_pre,
    step_pre,
    wrow,
    stats,
    in_sem,
    mv_sem,
    table_sem,
    ready,
    send1x,
    got1x,
    send1y,
    got1y,
    send2x,
    got2x,
    send2y,
    got2y,
    sendz1,
    gotz1,
    sendz2,
    gotz2,
    send_e1,
    got_e1,
    send_e2,
    got_e2,
    send3,
    got3,
    halo_sem,
    send_s,
    got_s,
    send4,
    got4,
    send_g,
    got_in,
    got_gz,
    got_gc,
    send_e,
    got_e,
    back_sem,
):
    n_out, shard, step, span, layers, hx, hy, hz = plan
    plane = 8
    n = n_out * plane
    chunk = (plane - 1) * step + span
    rows = span * 8
    hxy = hx + hy
    last = n_out - 1
    main = step - SHARE
    half_a = (main + 1) // 2
    half_b = main - half_a
    r = lax.axis_index("replica")
    y = lax.axis_index("spatial")
    d = r * 2 + y
    z = d // plane
    p = d % plane
    x = p // 4
    c = (p // 2) % 2
    base = d * (step * TILE)
    off = d * (shard - step * TILE)

    def dev(flat):
        return (flat // 2, flat % 2)

    def at(zz, xx, cc, yy):
        return ((zz * 2 + xx) * 2 + cc, yy)

    barrier = pltpu.get_barrier_semaphore()

    def load(zt):
        start = pl.multiple_of(zt * (plane * step * TILE), TILE)
        return pltpu.make_async_copy(
            grads_ref.at[0, :, pl.ds(start, chunk * TILE)], gin.at[zt], in_sem.at[zt]
        )

    h = z // 2
    order = [3 - 3 * h, 2 - h, flip(z, 1), z]
    for zt in order:
        load(zt).start()
    mv_loads = [
        pltpu.make_async_copy(ref, buf, mv_sem.at[j])
        for j, (ref, buf) in enumerate(((m_ref, m_in), (v_ref, v_in)))
    ]
    tables = [
        pltpu.make_async_copy(ref, buf, table_sem.at[j])
        for j, (ref, buf) in enumerate(
            ((offsets_in, offsets_ref), (sizes_in, sizes_ref), (skip_in, skip_ref))
        )
    ]
    for copy in mv_loads + tables:
        copy.start()

    def signal(sem, device):
        pl.semaphore_signal(sem, inc=1, device_id=device, device_id_type=MESH)

    def signal_z(sem, cores):
        @pl.when(z > 0)
        def _():
            for cc in cores:
                signal(sem, at(z - 1, x, cc, y))

        @pl.when(z < n_out - 1)
        def _():
            for cc in cores:
                signal(sem, at(z + 1, x, cc, y))

    n_z = jnp.where(z > 0, 1, 0) + jnp.where(z < n_out - 1, 1, 0)
    for device in (
        at(z, x, 1 - c, y),
        at(z, 1 - x, c, y),
        at(z, x, c, 1 - y),
        at(z, 1 - x, 1 - c, y),
        at(z, x, 1 - c, 1 - y),
    ):
        signal(barrier, device)
    signal_z(barrier, (c, 1 - c))

    group = max(g for g in range(1, 33) if chunk % g == 0)

    def pack(k):
        zt = order[k - 1]
        load(zt).wait()
        @pl.loop(0, chunk // group)
        def _(i):
            first = pl.multiple_of(i * (group * TILE), group * TILE)
            v = gin[zt, :, pl.ds(first, group * TILE)].astype(jnp.float32)
            packed[zt, pl.ds(i * group, group)] = v.reshape(group, 8, 128).astype(jnp.bfloat16)

    def remote(src, dst, send, recv, device):
        return pltpu.make_async_remote_copy(
            src_ref=src,
            dst_ref=dst,
            send_sem=send,
            recv_sem=recv,
            device_id=device,
            device_id_type=MESH,
        )

    def landed(ref, sem):
        pltpu.make_async_copy(ref, ref, sem).wait()

    def first(xx, cc, yy):
        return (xx * 4 + cc * 2 + yy) * step

    def send_raw(zt, h):
        yb, xb = (y, x) if h else (1 - y, 1 - x)
        for m in (3, 2, 1):
            xx, cc = (1 - x if m >= 2 else x), (1 - c if m % 2 else c)
            remote(
                packed.at[zt, pl.ds(first(xx, cc, yb), hx)],
                r1x.at[h, zt, m - 1],
                send1x,
                got1x.at[h, zt],
                at(z, xx, cc, y),
            ).start()
            yy = 1 - y if m >= 2 else y
            remote(
                packed.at[zt, pl.ds(first(xb, cc, yy) + hx, hy)],
                r1y.at[h, zt, m - 1],
                send1y,
                got1y.at[h, zt],
                at(z, x, cc, yy),
            ).start()

    def raws(zt, h, t, r1, own):
        v = packed[zt, own + t].astype(jnp.float32) + r1[h, zt, 0, t].astype(jnp.float32)
        return v + (r1[h, zt, 1, t].astype(jnp.float32) + r1[h, zt, 2, t].astype(jnp.float32))

    def sum_raw(zt):
        landed(r1x.at[0, zt], got1x.at[0, zt])
        own = first(x, c, 1 - y)

        @pl.loop(0, hx, unroll=2)
        def _(t):
            sx[zt, t] = raws(zt, 0, t, r1x, own)

        remote(sx.at[zt], r2x.at[zt], send2x, got2x.at[zt], at(z, x, c, 1 - y)).start()
        landed(r1y.at[0, zt], got1y.at[0, zt])
        own2 = first(1 - x, c, y) + hx

        @pl.loop(0, hy, unroll=2)
        def _(t):
            sy[zt, t] = raws(zt, 0, t, r1y, own2)

        remote(sy.at[zt], r2y.at[zt], send2y, got2y.at[zt], at(z, 1 - x, c, y)).start()

    def pass_on(zt, lo, size):
        rows = pl.ds(lo, size)
        to = at(zt, x, c, y)
        remote(part.at[zt, rows], recv3.at[z, rows], send3, got3, to).start()

    def sum_plane(zt, send):
        own = first(x, c, y)
        landed(r1x.at[1, zt], got1x.at[1, zt])
        landed(r2x.at[zt], got2x.at[zt])

        @pl.loop(0, hx, unroll=2)
        def _(t):
            part[zt, t] = raws(zt, 1, t, r1x, own) + r2x[zt, t]

        if send:
            pass_on(zt, 0, hx)
        landed(r1y.at[1, zt], got1y.at[1, zt])
        landed(r2y.at[zt], got2y.at[zt])

        @pl.loop(0, hy, unroll=2)
        def _(t):
            part[zt, hx + t] = raws(zt, 1, t, r1y, own + hx) + r2y[zt, t]

        if send:
            pass_on(zt, hx, hy)

    def send_far(zt, other):
        cc = 1 - c if other else c
        for j in range(4):
            remote(
                packed.at[zt, pl.ds(first(j // 2, cc, j % 2) + hxy, hz)],
                rz1.at[other * n_out + z, j],
                sendz1,
                gotz1,
                at(zt, x, cc, y),
            ).start()

        @pl.when((zt == last) & (cc == 1))
        def _():
            remote(
                packed.at[last, pl.ds(chunk - 1, 1)],
                re1.at[pl.ds(z * 2 + c, 1)],
                send_e1,
                got_e1,
                at(zt, x, cc, y),
            ).start()

    def send_distance(j):
        @pl.when(z >= j)
        def _():
            for other in (0, 1):
                send_far(z - j, other)

        @pl.when(z < n_out - j)
        def _():
            for other in (0, 1):
                send_far(z + j, other)

    def sum_far():
        landed(rz1.at[pl.ds(0, 2 * n_out - 1)], gotz1)

        @pl.loop(0, 4)
        def _(j):
            own = first(j // 2, c, j % 2) + hxy
            for t in range(hz):
                acc = packed[z, own + t].astype(jnp.float32)
                acc = acc + rz1[n_out + z, j, t].astype(jnp.float32)
                for k in range(1, n_out):
                    zz = (z + k) % n_out
                    two = rz1[zz, j, t].astype(jnp.float32)
                    acc = acc + (two + rz1[n_out + zz, j, t].astype(jnp.float32))
                zs[j, t] = acc

        for m in (3, 2, 1):
            xx, yy = (1 - x if m >= 2 else x), (1 - y if m % 2 else y)
            remote(zs.at[xx * 2 + yy], rz2.at[m - 1], sendz2, gotz2, at(z, xx, c, yy)).start()

        @pl.when((z == last) & (c == 1))
        def _():
            landed(re1.at[pl.ds(0, 2 * n_out - 1)], got_e1)
            acc = packed[last, chunk - 1].astype(jnp.float32)
            for j in range(2 * n_out - 1):
                acc = acc + re1[j].astype(jnp.float32)
            ze[0] = acc

            @pl.when(x * 2 + y < 3)
            def _():
                remote(
                    ze, re2.at[pl.ds(x * 2 + y, 1)], send_e2, got_e2, at(z, 1, 1, 1)
                ).start()

    lane = lax.broadcasted_iota(jnp.int32, (rows, 128), 1)
    shift_l = off % 128
    shift_r = off // 128
    whole = step * TILE

    def window(j, ref):
        mv_loads[j].wait()
        edge = jnp.pad(ref[pl.ds(whole, shard - whole)], (0, 128 - (shard - whole)))
        edge = jnp.broadcast_to(edge.reshape(1, 128), (8, 128))
        w = jnp.concatenate([ref[pl.ds(0, whole)].reshape(step * 8, 128), edge], 0)
        w = pltpu.roll(w, shift_l, 1)
        w = jnp.where(lane < shift_l, pltpu.roll(w, 1, 0), w)
        w = pltpu.roll(w, shift_r, 0)
        mv[:, j] = w.reshape(span, 8, 128)

    place = lax.broadcasted_iota(jnp.int32, (8, 128), 0) * 128 + lax.broadcasted_iota(
        jnp.int32, (8, 128), 1
    )
    low, high, own_low, own_high = [], [], [], []

    def bounds():
        for copy in tables:
            copy.wait()
        for l in range(layers):
            low.append(offsets_ref[l] - base)
            high.append(offsets_ref[l] + sizes_ref[l] - base)
            own_low.append(jnp.maximum(low[l], off))
            own_high.append(jnp.minimum(high[l], off + shard))

    lane1 = lax.broadcasted_iota(jnp.int32, (1, 128), 1)

    def squares(value, start, stop, lows, highs, sums=None):
        def add(t, accs):
            pos = place + t * TILE
            v = value(t)
            v = v * v
            return tuple(
                acc + jnp.where((pos >= lo) & (pos < hi), v, 0.0)
                for acc, lo, hi in zip(accs, lows, highs)
            )

        if sums is None:
            sums = tuple(jnp.zeros((8, 128), jnp.float32) for _ in range(layers))
        return lax.fori_loop(start, stop, add, sums)

    def as_row(sums, first):
        row = jnp.zeros((1, 128), jnp.float32)
        for l, acc in enumerate(sums):
            row = jnp.where(lane1 == first + l, jnp.sum(acc, axis=(0, 1), keepdims=True), row)
        return row

    def step_z(j):
        if j == 1:
            send_distance(1)
            send_far(z, 1)
            return
        pl.semaphore_wait(ready.at[j - 2], n_z)
        if j < n_out - 1:
            signal_z(ready.at[j - 1], (c,))
        send_distance(j)

    for op in RS:
        i = int(op[1:] or 0) if op != "bar" and op != "mv" else 0
        zt = order[i - 1]
        if op == "bar":
            pl.semaphore_wait(barrier, 5 + 2 * n_z)
            signal_z(ready.at[0], (c,))
        elif op == "mv":
            bounds()
            for j, ref in enumerate((m_in, v_in)):
                window(j, ref)
            wrow[...] = as_row(squares(lambda t: mv[t, 0], 0, span, own_low, own_high), 0)
        elif op[0] == "k":
            pack(i)
        elif op[0] == "A":
            send_raw(zt, 0)
        elif op[0] == "B":
            send_raw(zt, 1)
        elif op[0] == "z":
            step_z(i)
        elif op[0] == "Z":
            sum_far()
        elif op[0] == "s":
            sum_raw(zt)
        elif op[0] == "p":
            sum_plane(zt, i < n_out)

    landed(recv3.at[pl.ds(0, n_out - 1)], got3)
    halo_copy = remote(mv.at[span - 1], halo, halo_sem.at[0], halo_sem.at[1], dev((d + 1) % n))
    halo_copy.start()
    landed(rz2, gotz2)
    for t in range(hz):
        acc = zs[x * 2 + y, t] + rz2[0, t]
        grad_buf[hxy + t] = (acc + (rz2[1, t] + rz2[2, t])) / n
    grad_buf[step] = jnp.zeros((8, 128), jnp.float32)

    @pl.when(d == n - 1)
    def _():
        landed(re2, got_e2)
        grad_buf[step] = (ze[0] + re2[0] + (re2[1] + re2[2])) / n

    def total_grad(t):
        acc = part[z, t]
        for k in range(1, n_out):
            acc = acc + recv3[(z + k) % n_out, t]
        acc = acc / n
        grad_buf[t] = acc
        return acc

    sums = squares(total_grad, 0, hxy, low, high)
    sums = squares(lambda t: grad_buf[t], hxy, span, low, high, sums)
    stats[d] = as_row(sums, layers) + wrow[...]

    for k in range(n_out - 1, -1, -1):
        for q in range(plane - 1, -1, -1):
            if k + q > 0:
                peer = flip(z, k) * plane + flip(p, q)
                remote(stats.at[d], stats.at[d], send_s, got_s, dev(peer)).start()

    skip_row = jnp.zeros((1, 128), jnp.float32)
    for l in range(layers):
        skip_row = jnp.where(lane1 == l, skip_ref[l].astype(jnp.float32), skip_row)

    def prepare(t):
        pos = place + t * TILE
        which = jnp.zeros((8, 128), jnp.int32)
        decay = jnp.zeros((8, 128), jnp.float32)
        for l in range(layers):
            inside = (pos >= low[l]) & (pos < high[l])
            which = jnp.where(inside, l, which)
            decay = jnp.where(inside, (1.0 - skip_ref[l].astype(jnp.float32)) * 0.001, decay)
        layer_of[t] = which
        nvw_pre[t] = 0.9 * mv[t, 1]
        step_pre[t] = 8.0 * (grad_buf[t] + decay * mv[t, 0])

    @pl.loop(1, span)
    def _(t):
        prepare(t)

    halo_copy.wait()
    for j in range(2):
        mv[0, j] = jnp.where(place < off, halo[j], mv[0, j])
    prepare(0)

    landed(stats.at[pl.ds(0, n - 1)], got_s)
    norms = jnp.sqrt(jnp.sum(stats[...], axis=0))
    wnorm = jnp.broadcast_to(norms, (8, 128))
    gnorm = pltpu.roll(wnorm, 128 - layers, 1)
    ratio = 0.02 * wnorm / (gnorm + 0.001 * wnorm + 1e-06)
    trust_row = skip_row + (1.0 - skip_row) * ratio
    trust = [
        jnp.sum(jnp.where(lane1 == l, trust_row, 0.0), axis=1, keepdims=True)
        for l in range(layers)
    ]

    def update(t):
        which = layer_of[t]
        trust_pos = jnp.broadcast_to(trust[0], (8, 128))
        for l in range(1, layers):
            trust_pos = jnp.where(which == l, trust[l], trust_pos)
        nv = nvw_pre[t] + trust_pos * step_pre[t]
        nm = mv[t, 0] - nv
        nvw[t] = nv
        nmw[t] = nm
        return nm.astype(jnp.bfloat16)

    x_side = at(z, 1 - x, c, y)
    y_side = at(z, x, c, 1 - y)
    across = at(z, 1 - x, c, 1 - y)
    partner = at(z, x, 1 - c, y)

    def share(b):
        return ags.at[b, pl.ds(main, SHARE)]

    for t in range(main, step):
        ags[d, t] = update(t)
    for device in (across, x_side, y_side):
        remote(share(d), share(d), send_g, got_in, device).start()

    @pl.loop(0, main)
    def _(t):
        ags[d, t] = update(t)

    def send_edge():
        for i, ref in enumerate((nmw, nvw)):
            remote(ref.at[0], ref.at[step], back_sem.at[i], back_sem.at[2 + i], dev(d - 1)).start()

    def block(zz, xx, cc, yy):
        return zz * plane + xx * 4 + cc * 2 + yy

    def forward(b, device, lo=0, size=main):
        piece = ags.at[b, pl.ds(lo, size)]
        remote(piece, piece, send4, got4.at[b], device).start()

    def arrived(b):
        landed(ags.at[b, pl.ds(0, main)], got4.at[b])

    def tiles(count):
        return ags.at[pl.ds(0, count), pl.ds(0, SHARE)]

    def z_share():
        landed(tiles(3), got_in)
        for j in range(4):
            b = block(z, j // 2, c, j % 2)
            for k in ZSEND:
                peer = at(flip(z, k), x, c, y)
                remote(share(b), share(b), send_g, got_gz.at[z], peer).start()
            remote(share(b), share(b), send_g, got_gc, partner).start()

    def z_arrived(k):
        landed(tiles(4), got_gz.at[flip(z, k)])
        for j in range(4):
            b = block(flip(z, k), j // 2, c, j % 2)
            remote(share(b), share(b), send_g, got_gc, partner).start()

    for k in ZSEND:
        forward(d, at(flip(z, k), x, c, y))

    def column(k):
        b = block(flip(z, k), x, c, y)
        if k > 0:
            arrived(b)
        forward(b, x_side)
        forward(b, y_side)
        if k in DIRECT:
            forward(b, across)
        forward(b, partner)

    def from_y(k):
        b = block(flip(z, k), x, c, 1 - y)
        arrived(b)
        if k not in DIRECT:
            forward(b, x_side, 0, half_a)
        forward(b, partner)

    def from_x(k):
        b = block(flip(z, k), 1 - x, c, y)
        arrived(b)
        if k not in DIRECT:
            forward(b, y_side, half_a, half_b)
        forward(b, partner)

    def corner(k):
        b = block(flip(z, k), 1 - x, c, 1 - y)
        arrived(b)
        forward(b, partner)

    def edges():
        @pl.when(d > 0)
        def _():
            send_edge()

        @pl.when(d == n - 1)
        def _():
            age[0] = update(step)
            for q in range(1, n):
                remote(age, age, send_e, got_e, dev(d - q)).start()

    for op in AG:
        i = int(op[1:])
        if op[0] == "c":
            column(i)
        elif op[0] == "x":
            from_x(i)
        elif op[0] == "y":
            from_y(i)
        elif op[0] == "d":
            corner(i)
        elif op[0] == "g":
            z_share()
        elif op[0] == "h":
            z_arrived(i)
        elif op[0] == "e":
            edges()

    @pl.loop(0, n_out)
    def _(k):
        for xx in range(2):
            for yy in range(2):
                arrived(block(k, xx, 1 - c, yy))

    landed(tiles(4 * n_out), got_gc)

    @pl.when(d < n - 1)
    def _():
        landed(age, got_e)
        for i, ref in enumerate((nmw, nvw)):
            landed(ref.at[step], back_sem.at[2 + i])

    @pl.when(d == n - 1)
    def _():
        landed(ags.at[pl.ds(0, n - 1), 0], send_e)

    @pl.when(d > 0)
    def _():
        for i, ref in enumerate((nmw, nvw)):
            landed(ref.at[step], back_sem.at[i])

    @pl.when((z != last) | (c != 1))
    def _():
        landed(re1.at[pl.ds(0, 1)], send_e1)

    @pl.when((z == last) & (c == 1) & (x * 2 + y < 3))
    def _():
        landed(ze, send_e2)

    for ref, sem in (
        (r1x, send1x),
        (r1y, send1y),
        (r2x, send2x),
        (r2y, send2y),
        (rz1.at[pl.ds(0, 2 * n_out - 1)], sendz1),
        (rz2, sendz2),
        (recv3.at[pl.ds(0, n_out - 1)], send3),
        (stats.at[pl.ds(0, n - 1)], send_s),
        (ags.at[pl.ds(0, n - 1), pl.ds(0, main)], send4),
        (tiles(n - 1), send_g),
    ):
        landed(ref, sem)


def finish(
    plan,
    ags,
    age,
    nmw,
    nvw,
    out_ref,
    nm_ref,
    nv_ref,
    nm_out,
    nv_out,
    out_sem,
    own_sem,
):
    n, n_spa, shard, step, span = plan
    rows = span * 8
    whole = step * TILE
    part = n * step // PIECES
    copies = [
        pltpu.make_async_copy(
            ags.at[pl.ds(i * part, part)], out_ref.at[pl.ds(i * part, part)], out_sem.at[i]
        )
        for i in range(PIECES)
    ]
    copies.append(
        pltpu.make_async_copy(age, out_ref.at[pl.ds(n * step, 1)], out_sem.at[PIECES])
    )
    for copy in copies:
        copy.start()
    d = lax.axis_index("replica") * n_spa + lax.axis_index("spatial")
    off = d * (shard - whole)
    shift_l = off % 128
    shift_r = off // 128
    back_l = 128 - shift_l
    lane = lax.broadcasted_iota(jnp.int32, (rows, 128), 1)
    for j, (src, buf, ref) in enumerate(((nmw, nm_out, nm_ref), (nvw, nv_out, nv_ref))):
        x = src[...].reshape(rows, 128)
        x = pltpu.roll(x, (rows - shift_r) % rows, 0)
        x = pltpu.roll(x, back_l % 128, 1)
        x = jnp.where(lane < back_l, x, pltpu.roll(x, rows - 1, 0))
        buf[pl.ds(0, whole)] = x[: step * 8].reshape(whole)
        buf[pl.ds(whole, shard - whole)] = x[step * 8, : shard - whole].reshape(shard - whole)
        copy = pltpu.make_async_copy(buf, ref, own_sem.at[j])
        copy.start()
        copies.append(copy)
    for copy in copies:
        copy.wait()


def windowed(n_rep, n_spa, grads, master, velocity, layer_offsets, layer_sizes, lars_skip):
    shard = master.shape[0]
    params = grads.shape[2]
    layers = layer_offsets.shape[0]
    plane = 8
    n = n_rep * n_spa
    n_out = n // plane
    step = shard // TILE
    span = params // TILE - (n - 1) * step
    chunk = (plane - 1) * step + span
    tiles = params // TILE
    hz = ZTILES
    hx = (step - hz + 1) // 2
    hy = step - hz - hx
    plan = (n_out, shard, step, span, layers, hx, hy, hz)
    vmem = pl.BlockSpec(memory_space=pltpu.VMEM)
    anywhere = pl.BlockSpec(memory_space=pltpu.HBM)
    f32, bf16 = jnp.float32, jnp.bfloat16
    dma = pltpu.SemaphoreType.DMA
    ags, age, nmw, nvw = pl.pallas_call(
        functools.partial(kernel, plan),
        out_shape=(
            pltpu.VMEM((n, step, 8, 128), bf16),
            pltpu.VMEM((1, 8, 128), bf16),
            pltpu.VMEM((span, 8, 128), f32),
            pltpu.VMEM((span, 8, 128), f32),
        ),
        in_specs=[anywhere] * 6,
        out_specs=(vmem,) * 4,
        scratch_shapes=[
            pltpu.SMEM((layers,), jnp.int32),
            pltpu.SMEM((layers,), jnp.int32),
            pltpu.SMEM((layers,), jnp.int32),
            pltpu.VMEM((shard,), f32),
            pltpu.VMEM((shard,), f32),
            pltpu.VMEM((n_out, 1, chunk * TILE), bf16),
            pltpu.VMEM((n_out, chunk, 8, 128), bf16),
            pltpu.VMEM((2, n_out, 3, hx, 8, 128), bf16),
            pltpu.VMEM((2, n_out, 3, hy, 8, 128), bf16),
            pltpu.VMEM((n_out, hx, 8, 128), f32),
            pltpu.VMEM((n_out, hy, 8, 128), f32),
            pltpu.VMEM((n_out, hx, 8, 128), f32),
            pltpu.VMEM((n_out, hy, 8, 128), f32),
            pltpu.VMEM((2 * n_out, 4, hz, 8, 128), bf16),
            pltpu.VMEM((4, hz, 8, 128), f32),
            pltpu.VMEM((3, hz, 8, 128), f32),
            pltpu.VMEM((2 * n_out, 8, 128), bf16),
            pltpu.VMEM((1, 8, 128), f32),
            pltpu.VMEM((3, 8, 128), f32),
            pltpu.VMEM((n_out, hx + hy, 8, 128), f32),
            pltpu.VMEM((n_out, hx + hy, 8, 128), f32),
            pltpu.VMEM((span, 2, 8, 128), f32),
            pltpu.VMEM((2, 8, 128), f32),
            pltpu.VMEM((span, 8, 128), f32),
            pltpu.VMEM((span, 8, 128), jnp.int32),
            pltpu.VMEM((span, 8, 128), f32),
            pltpu.VMEM((span, 8, 128), f32),
            pltpu.VMEM((1, 128), f32),
            pltpu.VMEM((n, 1, 128), f32),
            dma((n_out,)),
            dma((2,)),
            dma((3,)),
            pltpu.SemaphoreType.REGULAR((n_out,)),
            dma(()),
            dma((2, n_out)),
            dma(()),
            dma((2, n_out)),
            dma(()),
            dma((n_out,)),
            dma(()),
            dma((n_out,)),
            dma(()),
            dma(()),
            dma(()),
            dma(()),
            dma(()),
            dma(()),
            dma(()),
            dma(()),
            dma(()),
            dma(()),
            dma((2,)),
            dma(()),
            dma(()),
            dma(()),
            dma((n,)),
            dma(()),
            dma(()),
            dma((n_out,)),
            dma(()),
            dma(()),
            dma(()),
            dma((4,)),
        ],
        compiler_params=pltpu.CompilerParams(
            collective_id=0, has_side_effects=True, vmem_limit_bytes=61 * 2**20
        ),
    )(grads, master, velocity, layer_offsets, layer_sizes, lars_skip)
    weights, nm, nv = pl.pallas_call(
        functools.partial(finish, (n, n_spa, shard, step, span)),
        out_shape=(
            jax.ShapeDtypeStruct((tiles, 8, 128), bf16),
            jax.ShapeDtypeStruct((shard,), f32),
            jax.ShapeDtypeStruct((shard,), f32),
        ),
        in_specs=[vmem] * 4,
        out_specs=(anywhere, anywhere, anywhere),
        scratch_shapes=[
            pltpu.VMEM((shard,), f32),
            pltpu.VMEM((shard,), f32),
            dma((PIECES + 1,)),
            dma((2,)),
        ],
        compiler_params=pltpu.CompilerParams(vmem_limit_bytes=16 * 2**20),
    )(ags.reshape(n * step, 8, 128), age, nmw, nvw)
    return weights.reshape(params), nm, nv


def tiled(n_rep, n_spa, params):
    n = n_rep * n_spa
    shard = params // n
    rest = shard % TILE
    n_out = n_rep // 4
    return (
        n_spa == 2
        and n_rep % 4 == 0
        and n_out == 4
        and params % TILE == 0
        and shard >= TILE
        and 0 < n * rest <= TILE
        and rest <= 128
    )


def step_fn(n_rep, n_spa, grads, *rest):
    if tiled(n_rep, n_spa, grads.shape[2]):
        return windowed(n_rep, n_spa, grads, *rest)
    return shards(grads, *rest)


def shards(grads, master, velocity, layer_offsets, layer_sizes, lars_skip):
    n_rep = lax.axis_size("replica")
    n_spa = lax.axis_size("spatial")
    shard = master.shape[0]
    position = lax.axis_index(("replica", "spatial")) * shard + jnp.arange(shard, dtype=jnp.int32)
    inside = (position[None, :] >= layer_offsets[:, None]) & (
        position[None, :] < (layer_offsets + layer_sizes)[:, None]
    )
    onehot = inside.astype(jnp.float32)
    received = lax.all_to_all(
        grads[0, 0].reshape(n_rep, n_spa * shard),
        "replica",
        split_axis=0,
        concat_axis=0,
        tiled=True,
    )
    first = jnp.sum(received.astype(jnp.float32), axis=0)
    summed = lax.psum_scatter(
        first.reshape(n_spa, shard), "spatial", scatter_dimension=0, tiled=True
    )
    grad = summed.reshape(shard) / (n_rep * n_spa)
    gsq_local = jnp.dot(onehot, grad * grad, precision=lax.Precision.HIGHEST)
    wsq_local = jnp.dot(onehot, master * master, precision=lax.Precision.HIGHEST)
    wsq, gsq = lax.psum((wsq_local, gsq_local), ("replica", "spatial"))
    wnorm = jnp.sqrt(wsq)
    gnorm = jnp.sqrt(gsq)
    skipped = lars_skip.astype(jnp.float32)
    ratio = 0.02 * wnorm / (gnorm + 0.001 * wnorm + 1e-06)
    trust = skipped + (1.0 - skipped) * ratio
    decay = (1.0 - skipped) * 0.001
    trust_pos = jnp.dot(trust, onehot, precision=lax.Precision.HIGHEST)
    decay_pos = jnp.dot(decay, onehot, precision=lax.Precision.HIGHEST)
    new_velocity = 0.9 * velocity + 8.0 * trust_pos * (grad + decay_pos * master)
    new_master = master - new_velocity
    new_weights = lax.all_gather(
        new_master.astype(jnp.bfloat16), ("replica", "spatial"), axis=0, tiled=True
    )
    return (new_weights, new_master, new_velocity)


def solution(mesh):
    return jax.shard_map(
        functools.partial(step_fn, mesh.shape["replica"], mesh.shape["spatial"]),
        mesh=mesh,
        in_specs=(
            P("replica", "spatial", None),
            P(("replica", "spatial")),
            P(("replica", "spatial")),
            P(),
            P(),
            P(),
        ),
        out_specs=(P(), P(("replica", "spatial")), P(("replica", "spatial"))),
        check_vma=False,
    )
```

```python
import functools

import jax
import jax.numpy as jnp
from jax import lax
from jax.experimental import pallas as pl
from jax.experimental.pallas import tpu as pltpu
from jax.sharding import PartitionSpec as P

MESH = pl.DeviceIdType.MESH
TILE = 1024
ZTILES = 4
SHARE = 6
PIECES = 8
RS = (
    "k1", "bar", "A1", "B1", "k2", "A2", "k3", "k4", "z1", "z2", "z3", "mv", "s1", "B2", "A3",
    "s2", "p1", "B3", "A4", "s3", "p2", "B4", "s4", "Z", "p3", "p4",
)
ZSEND = "mfn"
VISIT = "mnf"
COLUMN = "axyp"
AG = (
    "c0", "c1", "g0", "c2", "x0", "y0", "c3", "e0", "x1", "y1", "d0", "x2", "y2", "d1", "x3",
    "y3", "d2", "h1", "h2", "h3", "d3",
)
DIRECT = (0, 1, 2, 3)


def flip(i, k):
    out, bit = 0, 1
    while bit <= k:
        b = (i // bit) % 2
        out = out + bit * (1 - 2 * b) * ((k // bit) % 2)
        bit *= 2
    return i + out


def kernel(
    plan,
    grads_ref,
    m_ref,
    v_ref,
    offsets_in,
    sizes_in,
    skip_in,
    ags,
    age,
    nmw,
    nvw,
    offsets_ref,
    sizes_ref,
    skip_ref,
    m_in,
    v_in,
    gin,
    packed,
    r1x,
    r1y,
    sx,
    sy,
    r2x,
    r2y,
    rz1,
    zs,
    rz2,
    re1,
    ze,
    re2,
    part,
    recv3,
    mv,
    halo,
    grad_buf,
    layer_of,
    nvw_pre,
    step_pre,
    wrow,
    stats,
    in_sem,
    mv_sem,
    table_sem,
    ready,
    send1x,
    got1x,
    send1y,
    got1y,
    send2x,
    got2x,
    send2y,
    got2y,
    sendz1,
    gotz1,
    sendz2,
    gotz2,
    send_e1,
    got_e1,
    send_e2,
    got_e2,
    send3,
    got3,
    halo_sem,
    send_s,
    got_s,
    send4,
    got4,
    send_g,
    got_in,
    got_gz,
    got_gc,
    send_e,
    got_e,
    back_sem,
):
    n_out, shard, step, span, layers, hx, hy, hz = plan
    plane = 8
    n = n_out * plane
    chunk = (plane - 1) * step + span
    rows = span * 8
    hxy = hx + hy
    last = n_out - 1
    main = step - SHARE
    half_a = (main + 1) // 2
    half_b = main - half_a
    r = lax.axis_index("replica")
    y = lax.axis_index("spatial")
    d = r * 2 + y
    z = d // plane
    p = d % plane
    x = p // 4
    c = (p // 2) % 2
    base = d * (step * TILE)
    off = d * (shard - step * TILE)

    def dev(flat):
        return (flat // 2, flat % 2)

    def at(zz, xx, cc, yy):
        return ((zz * 2 + xx) * 2 + cc, yy)

    barrier = pltpu.get_barrier_semaphore()

    def load(zt):
        start = pl.multiple_of(zt * (plane * step * TILE), TILE)
        return pltpu.make_async_copy(
            grads_ref.at[0, :, pl.ds(start, chunk * TILE)], gin.at[zt], in_sem.at[zt]
        )

    h = z // 2
    order = [3 - 3 * h, 2 - h, flip(z, 1), z]
    for zt in order:
        load(zt).start()
    mv_loads = [
        pltpu.make_async_copy(ref, buf, mv_sem.at[j])
        for j, (ref, buf) in enumerate(((m_ref, m_in), (v_ref, v_in)))
    ]
    tables = [
        pltpu.make_async_copy(ref, buf, table_sem.at[j])
        for j, (ref, buf) in enumerate(
            ((offsets_in, offsets_ref), (sizes_in, sizes_ref), (skip_in, skip_ref))
        )
    ]
    for copy in mv_loads + tables:
        copy.start()

    def signal(sem, device):
        pl.semaphore_signal(sem, inc=1, device_id=device, device_id_type=MESH)

    def signal_z(sem, cores):
        @pl.when(z > 0)
        def _():
            for cc in cores:
                signal(sem, at(z - 1, x, cc, y))

        @pl.when(z < n_out - 1)
        def _():
            for cc in cores:
                signal(sem, at(z + 1, x, cc, y))

    n_z = jnp.where(z > 0, 1, 0) + jnp.where(z < n_out - 1, 1, 0)
    for device in (
        at(z, x, 1 - c, y),
        at(z, 1 - x, c, y),
        at(z, x, c, 1 - y),
        at(z, 1 - x, 1 - c, y),
        at(z, x, 1 - c, 1 - y),
    ):
        signal(barrier, device)
    signal_z(barrier, (c, 1 - c))

    group = max(g for g in range(1, 33) if chunk % g == 0)

    def pack(k):
        zt = order[k - 1]
        load(zt).wait()
        @pl.loop(0, chunk // group)
        def _(i):
            first = pl.multiple_of(i * (group * TILE), group * TILE)
            v = gin[zt, :, pl.ds(first, group * TILE)].astype(jnp.float32)
            packed[zt, pl.ds(i * group, group)] = v.reshape(group, 8, 128).astype(jnp.bfloat16)

    def remote(src, dst, send, recv, device):
        return pltpu.make_async_remote_copy(
            src_ref=src,
            dst_ref=dst,
            send_sem=send,
            recv_sem=recv,
            device_id=device,
            device_id_type=MESH,
        )

    def landed(ref, sem):
        pltpu.make_async_copy(ref, ref, sem).wait()

    def first(xx, cc, yy):
        return (xx * 4 + cc * 2 + yy) * step

    def send_raw(zt, h):
        yb, xb = (y, x) if h else (1 - y, 1 - x)
        for m in (3, 2, 1):
            xx, cc = (1 - x if m >= 2 else x), (1 - c if m % 2 else c)
            remote(
                packed.at[zt, pl.ds(first(xx, cc, yb), hx)],
                r1x.at[h, zt, m - 1],
                send1x,
                got1x.at[h, zt],
                at(z, xx, cc, y),
            ).start()
            yy = 1 - y if m >= 2 else y
            remote(
                packed.at[zt, pl.ds(first(xb, cc, yy) + hx, hy)],
                r1y.at[h, zt, m - 1],
                send1y,
                got1y.at[h, zt],
                at(z, x, cc, yy),
            ).start()

    def raws(zt, h, t, r1, own):
        v = packed[zt, own + t].astype(jnp.float32) + r1[h, zt, 0, t].astype(jnp.float32)
        return v + (r1[h, zt, 1, t].astype(jnp.float32) + r1[h, zt, 2, t].astype(jnp.float32))

    def sum_raw(zt):
        landed(r1x.at[0, zt], got1x.at[0, zt])
        own = first(x, c, 1 - y)

        @pl.loop(0, hx, unroll=2)
        def _(t):
            sx[zt, t] = raws(zt, 0, t, r1x, own)

        remote(sx.at[zt], r2x.at[zt], send2x, got2x.at[zt], at(z, x, c, 1 - y)).start()
        landed(r1y.at[0, zt], got1y.at[0, zt])
        own2 = first(1 - x, c, y) + hx

        @pl.loop(0, hy, unroll=2)
        def _(t):
            sy[zt, t] = raws(zt, 0, t, r1y, own2)

        remote(sy.at[zt], r2y.at[zt], send2y, got2y.at[zt], at(z, 1 - x, c, y)).start()

    def pass_on(zt, lo, size):
        rows = pl.ds(lo, size)
        to = at(zt, x, c, y)
        remote(part.at[zt, rows], recv3.at[z, rows], send3, got3, to).start()

    def sum_plane(zt, send):
        own = first(x, c, y)
        landed(r1x.at[1, zt], got1x.at[1, zt])
        landed(r2x.at[zt], got2x.at[zt])

        @pl.loop(0, hx, unroll=2)
        def _(t):
            part[zt, t] = raws(zt, 1, t, r1x, own) + r2x[zt, t]

        if send:
            pass_on(zt, 0, hx)
        landed(r1y.at[1, zt], got1y.at[1, zt])
        landed(r2y.at[zt], got2y.at[zt])

        @pl.loop(0, hy, unroll=2)
        def _(t):
            part[zt, hx + t] = raws(zt, 1, t, r1y, own + hx) + r2y[zt, t]

        if send:
            pass_on(zt, hx, hy)

    def send_far(zt, other):
        cc = 1 - c if other else c
        for j in range(4):
            remote(
                packed.at[zt, pl.ds(first(j // 2, cc, j % 2) + hxy, hz)],
                rz1.at[other * n_out + z, j],
                sendz1,
                gotz1,
                at(zt, x, cc, y),
            ).start()

        @pl.when((zt == last) & (cc == 1))
        def _():
            remote(
                packed.at[last, pl.ds(chunk - 1, 1)],
                re1.at[pl.ds(z * 2 + c, 1)],
                send_e1,
                got_e1,
                at(zt, x, cc, y),
            ).start()

    def send_distance(j):
        @pl.when(z >= j)
        def _():
            for other in (0, 1):
                send_far(z - j, other)

        @pl.when(z < n_out - j)
        def _():
            for other in (0, 1):
                send_far(z + j, other)

    def sum_far():
        landed(rz1.at[pl.ds(0, 2 * n_out - 1)], gotz1)

        @pl.loop(0, 4)
        def _(j):
            own = first(j // 2, c, j % 2) + hxy
            for t in range(hz):
                acc = packed[z, own + t].astype(jnp.float32)
                acc = acc + rz1[n_out + z, j, t].astype(jnp.float32)
                for k in range(1, n_out):
                    zz = (z + k) % n_out
                    two = rz1[zz, j, t].astype(jnp.float32)
                    acc = acc + (two + rz1[n_out + zz, j, t].astype(jnp.float32))
                zs[j, t] = acc

        for m in (3, 2, 1):
            xx, yy = (1 - x if m >= 2 else x), (1 - y if m % 2 else y)
            remote(zs.at[xx * 2 + yy], rz2.at[m - 1], sendz2, gotz2, at(z, xx, c, yy)).start()

        @pl.when((z == last) & (c == 1))
        def _():
            landed(re1.at[pl.ds(0, 2 * n_out - 1)], got_e1)
            acc = packed[last, chunk - 1].astype(jnp.float32)
            for j in range(2 * n_out - 1):
                acc = acc + re1[j].astype(jnp.float32)
            ze[0] = acc

            @pl.when(x * 2 + y < 3)
            def _():
                remote(
                    ze, re2.at[pl.ds(x * 2 + y, 1)], send_e2, got_e2, at(z, 1, 1, 1)
                ).start()

    lane = lax.broadcasted_iota(jnp.int32, (rows, 128), 1)
    shift_l = off % 128
    shift_r = off // 128
    whole = step * TILE

    def window(j, ref):
        mv_loads[j].wait()
        edge = jnp.pad(ref[pl.ds(whole, shard - whole)], (0, 128 - (shard - whole)))
        edge = jnp.broadcast_to(edge.reshape(1, 128), (8, 128))
        w = jnp.concatenate([ref[pl.ds(0, whole)].reshape(step * 8, 128), edge], 0)
        w = pltpu.roll(w, shift_l, 1)
        w = jnp.where(lane < shift_l, pltpu.roll(w, 1, 0), w)
        w = pltpu.roll(w, shift_r, 0)
        mv[:, j] = w.reshape(span, 8, 128)

    place = lax.broadcasted_iota(jnp.int32, (8, 128), 0) * 128 + lax.broadcasted_iota(
        jnp.int32, (8, 128), 1
    )
    low, high, own_low, own_high = [], [], [], []

    def bounds():
        for copy in tables:
            copy.wait()
        for l in range(layers):
            low.append(offsets_ref[l] - base)
            high.append(offsets_ref[l] + sizes_ref[l] - base)
            own_low.append(jnp.maximum(low[l], off))
            own_high.append(jnp.minimum(high[l], off + shard))

    lane1 = lax.broadcasted_iota(jnp.int32, (1, 128), 1)

    def squares(value, start, stop, lows, highs, sums=None):
        def add(t, accs):
            pos = place + t * TILE
            v = value(t)
            v = v * v
            return tuple(
                acc + jnp.where((pos >= lo) & (pos < hi), v, 0.0)
                for acc, lo, hi in zip(accs, lows, highs)
            )

        if sums is None:
            sums = tuple(jnp.zeros((8, 128), jnp.float32) for _ in range(layers))
        return lax.fori_loop(start, stop, add, sums)

    def as_row(sums, first):
        row = jnp.zeros((1, 128), jnp.float32)
        for l, acc in enumerate(sums):
            row = jnp.where(lane1 == first + l, jnp.sum(acc, axis=(0, 1), keepdims=True), row)
        return row

    def step_z(j):
        if j == 1:
            send_distance(1)
            send_far(z, 1)
            return
        pl.semaphore_wait(ready.at[j - 2], n_z)
        if j < n_out - 1:
            signal_z(ready.at[j - 1], (c,))
        send_distance(j)

    for op in RS:
        i = int(op[1:] or 0) if op != "bar" and op != "mv" else 0
        zt = order[i - 1]
        if op == "bar":
            pl.semaphore_wait(barrier, 5 + 2 * n_z)
            signal_z(ready.at[0], (c,))
        elif op == "mv":
            bounds()
            for j, ref in enumerate((m_in, v_in)):
                window(j, ref)
            wrow[...] = as_row(squares(lambda t: mv[t, 0], 0, span, own_low, own_high), 0)
        elif op[0] == "k":
            pack(i)
        elif op[0] == "A":
            send_raw(zt, 0)
        elif op[0] == "B":
            send_raw(zt, 1)
        elif op[0] == "z":
            step_z(i)
        elif op[0] == "Z":
            sum_far()
        elif op[0] == "s":
            sum_raw(zt)
        elif op[0] == "p":
            sum_plane(zt, i < n_out)

    landed(recv3.at[pl.ds(0, n_out - 1)], got3)
    halo_copy = remote(mv.at[span - 1], halo, halo_sem.at[0], halo_sem.at[1], dev((d + 1) % n))
    halo_copy.start()
    landed(rz2, gotz2)
    for t in range(hz):
        acc = zs[x * 2 + y, t] + rz2[0, t]
        grad_buf[hxy + t] = (acc + (rz2[1, t] + rz2[2, t])) / n
    grad_buf[step] = jnp.zeros((8, 128), jnp.float32)

    @pl.when(d == n - 1)
    def _():
        landed(re2, got_e2)
        grad_buf[step] = (ze[0] + re2[0] + (re2[1] + re2[2])) / n

    def total_grad(t):
        acc = part[z, t]
        for k in range(1, n_out):
            acc = acc + recv3[(z + k) % n_out, t]
        acc = acc / n
        grad_buf[t] = acc
        return acc

    sums = squares(total_grad, 0, hxy, low, high)
    sums = squares(lambda t: grad_buf[t], hxy, span, low, high, sums)
    stats[d] = as_row(sums, layers) + wrow[...]

    for k in range(n_out - 1, -1, -1):
        for q in range(plane - 1, -1, -1):
            if k + q > 0:
                peer = flip(z, k) * plane + flip(p, q)
                remote(stats.at[d], stats.at[d], send_s, got_s, dev(peer)).start()

    skip_row = jnp.zeros((1, 128), jnp.float32)
    for l in range(layers):
        skip_row = jnp.where(lane1 == l, skip_ref[l].astype(jnp.float32), skip_row)

    def prepare(t):
        pos = place + t * TILE
        which = jnp.zeros((8, 128), jnp.int32)
        decay = jnp.zeros((8, 128), jnp.float32)
        for l in range(layers):
            inside = (pos >= low[l]) & (pos < high[l])
            which = jnp.where(inside, l, which)
            decay = jnp.where(inside, (1.0 - skip_ref[l].astype(jnp.float32)) * 0.001, decay)
        layer_of[t] = which
        nvw_pre[t] = 0.9 * mv[t, 1]
        step_pre[t] = 8.0 * (grad_buf[t] + decay * mv[t, 0])

    @pl.loop(1, span)
    def _(t):
        prepare(t)

    halo_copy.wait()
    for j in range(2):
        mv[0, j] = jnp.where(place < off, halo[j], mv[0, j])
    prepare(0)

    landed(stats.at[pl.ds(0, n - 1)], got_s)
    norms = jnp.sqrt(jnp.sum(stats[...], axis=0))
    wnorm = jnp.broadcast_to(norms, (8, 128))
    gnorm = pltpu.roll(wnorm, 128 - layers, 1)
    ratio = 0.02 * wnorm / (gnorm + 0.001 * wnorm + 1e-06)
    trust_row = skip_row + (1.0 - skip_row) * ratio
    trust = [
        jnp.sum(jnp.where(lane1 == l, trust_row, 0.0), axis=1, keepdims=True)
        for l in range(layers)
    ]

    def update(t):
        which = layer_of[t]
        trust_pos = jnp.broadcast_to(trust[0], (8, 128))
        for l in range(1, layers):
            trust_pos = jnp.where(which == l, trust[l], trust_pos)
        nv = nvw_pre[t] + trust_pos * step_pre[t]
        nm = mv[t, 0] - nv
        nvw[t] = nv
        nmw[t] = nm
        return nm.astype(jnp.bfloat16)

    x_side = at(z, 1 - x, c, y)
    y_side = at(z, x, c, 1 - y)
    across = at(z, 1 - x, c, 1 - y)
    partner = at(z, x, 1 - c, y)

    def share(b):
        return ags.at[b, pl.ds(main, SHARE)]

    for t in range(main, step):
        ags[d, t] = update(t)
    for device in (across, x_side, y_side):
        remote(share(d), share(d), send_g, got_in, device).start()

    @pl.loop(0, main)
    def _(t):
        ags[d, t] = update(t)

    def send_edge():
        for i, ref in enumerate((nmw, nvw)):
            remote(ref.at[0], ref.at[step], back_sem.at[i], back_sem.at[2 + i], dev(d - 1)).start()

    def block(zz, xx, cc, yy):
        return zz * plane + xx * 4 + cc * 2 + yy

    def forward(b, device, lo=0, size=main):
        piece = ags.at[b, pl.ds(lo, size)]
        remote(piece, piece, send4, got4.at[b], device).start()

    def arrived(b):
        landed(ags.at[b, pl.ds(0, main)], got4.at[b])

    zone = {"m": flip(z, 1), "n": 2 - h, "f": 3 - 3 * h}
    visits = [z] + [zone[k] for k in VISIT]
    sends = [zone[k] for k in ZSEND]

    def tiles(count):
        return ags.at[pl.ds(0, count), pl.ds(0, SHARE)]

    def z_share():
        landed(tiles(3), got_in)
        for j in range(4):
            b = block(z, j // 2, c, j % 2)
            for to in sends:
                peer = at(to, x, c, y)
                remote(share(b), share(b), send_g, got_gz.at[z], peer).start()
            remote(share(b), share(b), send_g, got_gc, partner).start()

    def z_arrived(k):
        landed(tiles(4), got_gz.at[visits[k]])
        for j in range(4):
            b = block(visits[k], j // 2, c, j % 2)
            remote(share(b), share(b), send_g, got_gc, partner).start()

    for to in sends:
        forward(d, at(to, x, c, y))

    def column(k):
        b = block(visits[k], x, c, y)
        if k > 0:
            arrived(b)
        for way in COLUMN:
            if way == "x":
                forward(b, x_side)
            elif way == "y":
                forward(b, y_side)
            elif way == "p":
                forward(b, partner)
            elif k in DIRECT:
                forward(b, across)

    def from_y(k):
        b = block(visits[k], x, c, 1 - y)
        arrived(b)
        if k not in DIRECT:
            forward(b, x_side, 0, half_a)
        forward(b, partner)

    def from_x(k):
        b = block(visits[k], 1 - x, c, y)
        arrived(b)
        if k not in DIRECT:
            forward(b, y_side, half_a, half_b)
        forward(b, partner)

    def corner(k):
        b = block(visits[k], 1 - x, c, 1 - y)
        arrived(b)
        forward(b, partner)

    def edges():
        @pl.when(d > 0)
        def _():
            send_edge()

        @pl.when(d == n - 1)
        def _():
            age[0] = update(step)
            for q in range(1, n):
                remote(age, age, send_e, got_e, dev(d - q)).start()

    for op in AG:
        i = int(op[1:])
        if op[0] == "c":
            column(i)
        elif op[0] == "x":
            from_x(i)
        elif op[0] == "y":
            from_y(i)
        elif op[0] == "d":
            corner(i)
        elif op[0] == "g":
            z_share()
        elif op[0] == "h":
            z_arrived(i)
        elif op[0] == "e":
            edges()

    @pl.loop(0, n_out)
    def _(k):
        for xx in range(2):
            for yy in range(2):
                arrived(block(k, xx, 1 - c, yy))

    landed(tiles(4 * n_out), got_gc)

    @pl.when(d < n - 1)
    def _():
        landed(age, got_e)
        for i, ref in enumerate((nmw, nvw)):
            landed(ref.at[step], back_sem.at[2 + i])

    @pl.when(d == n - 1)
    def _():
        landed(ags.at[pl.ds(0, n - 1), 0], send_e)

    @pl.when(d > 0)
    def _():
        for i, ref in enumerate((nmw, nvw)):
            landed(ref.at[step], back_sem.at[i])

    @pl.when((z != last) | (c != 1))
    def _():
        landed(re1.at[pl.ds(0, 1)], send_e1)

    @pl.when((z == last) & (c == 1) & (x * 2 + y < 3))
    def _():
        landed(ze, send_e2)

    for ref, sem in (
        (r1x, send1x),
        (r1y, send1y),
        (r2x, send2x),
        (r2y, send2y),
        (rz1.at[pl.ds(0, 2 * n_out - 1)], sendz1),
        (rz2, sendz2),
        (recv3.at[pl.ds(0, n_out - 1)], send3),
        (stats.at[pl.ds(0, n - 1)], send_s),
        (ags.at[pl.ds(0, n - 1), pl.ds(0, main)], send4),
        (tiles(n - 1), send_g),
    ):
        landed(ref, sem)


def finish(
    plan,
    ags,
    age,
    nmw,
    nvw,
    out_ref,
    nm_ref,
    nv_ref,
    nm_out,
    nv_out,
    out_sem,
    own_sem,
):
    n, n_spa, shard, step, span = plan
    rows = span * 8
    whole = step * TILE
    part = n * step // PIECES
    copies = [
        pltpu.make_async_copy(
            ags.at[pl.ds(i * part, part)], out_ref.at[pl.ds(i * part, part)], out_sem.at[i]
        )
        for i in range(PIECES)
    ]
    copies.append(
        pltpu.make_async_copy(age, out_ref.at[pl.ds(n * step, 1)], out_sem.at[PIECES])
    )
    for copy in copies:
        copy.start()
    d = lax.axis_index("replica") * n_spa + lax.axis_index("spatial")
    off = d * (shard - whole)
    shift_l = off % 128
    shift_r = off // 128
    back_l = 128 - shift_l
    lane = lax.broadcasted_iota(jnp.int32, (rows, 128), 1)
    for j, (src, buf, ref) in enumerate(((nmw, nm_out, nm_ref), (nvw, nv_out, nv_ref))):
        x = src[...].reshape(rows, 128)
        x = pltpu.roll(x, (rows - shift_r) % rows, 0)
        x = pltpu.roll(x, back_l % 128, 1)
        x = jnp.where(lane < back_l, x, pltpu.roll(x, rows - 1, 0))
        buf[pl.ds(0, whole)] = x[: step * 8].reshape(whole)
        buf[pl.ds(whole, shard - whole)] = x[step * 8, : shard - whole].reshape(shard - whole)
        copy = pltpu.make_async_copy(buf, ref, own_sem.at[j])
        copy.start()
        copies.append(copy)
    for copy in copies:
        copy.wait()


def windowed(n_rep, n_spa, grads, master, velocity, layer_offsets, layer_sizes, lars_skip):
    shard = master.shape[0]
    params = grads.shape[2]
    layers = layer_offsets.shape[0]
    plane = 8
    n = n_rep * n_spa
    n_out = n // plane
    step = shard // TILE
    span = params // TILE - (n - 1) * step
    chunk = (plane - 1) * step + span
    tiles = params // TILE
    hz = ZTILES
    hx = (step - hz + 1) // 2
    hy = step - hz - hx
    plan = (n_out, shard, step, span, layers, hx, hy, hz)
    vmem = pl.BlockSpec(memory_space=pltpu.VMEM)
    anywhere = pl.BlockSpec(memory_space=pltpu.HBM)
    f32, bf16 = jnp.float32, jnp.bfloat16
    dma = pltpu.SemaphoreType.DMA
    ags, age, nmw, nvw = pl.pallas_call(
        functools.partial(kernel, plan),
        out_shape=(
            pltpu.VMEM((n, step, 8, 128), bf16),
            pltpu.VMEM((1, 8, 128), bf16),
            pltpu.VMEM((span, 8, 128), f32),
            pltpu.VMEM((span, 8, 128), f32),
        ),
        in_specs=[anywhere] * 6,
        out_specs=(vmem,) * 4,
        scratch_shapes=[
            pltpu.SMEM((layers,), jnp.int32),
            pltpu.SMEM((layers,), jnp.int32),
            pltpu.SMEM((layers,), jnp.int32),
            pltpu.VMEM((shard,), f32),
            pltpu.VMEM((shard,), f32),
            pltpu.VMEM((n_out, 1, chunk * TILE), bf16),
            pltpu.VMEM((n_out, chunk, 8, 128), bf16),
            pltpu.VMEM((2, n_out, 3, hx, 8, 128), bf16),
            pltpu.VMEM((2, n_out, 3, hy, 8, 128), bf16),
            pltpu.VMEM((n_out, hx, 8, 128), f32),
            pltpu.VMEM((n_out, hy, 8, 128), f32),
            pltpu.VMEM((n_out, hx, 8, 128), f32),
            pltpu.VMEM((n_out, hy, 8, 128), f32),
            pltpu.VMEM((2 * n_out, 4, hz, 8, 128), bf16),
            pltpu.VMEM((4, hz, 8, 128), f32),
            pltpu.VMEM((3, hz, 8, 128), f32),
            pltpu.VMEM((2 * n_out, 8, 128), bf16),
            pltpu.VMEM((1, 8, 128), f32),
            pltpu.VMEM((3, 8, 128), f32),
            pltpu.VMEM((n_out, hx + hy, 8, 128), f32),
            pltpu.VMEM((n_out, hx + hy, 8, 128), f32),
            pltpu.VMEM((span, 2, 8, 128), f32),
            pltpu.VMEM((2, 8, 128), f32),
            pltpu.VMEM((span, 8, 128), f32),
            pltpu.VMEM((span, 8, 128), jnp.int32),
            pltpu.VMEM((span, 8, 128), f32),
            pltpu.VMEM((span, 8, 128), f32),
            pltpu.VMEM((1, 128), f32),
            pltpu.VMEM((n, 1, 128), f32),
            dma((n_out,)),
            dma((2,)),
            dma((3,)),
            pltpu.SemaphoreType.REGULAR((n_out,)),
            dma(()),
            dma((2, n_out)),
            dma(()),
            dma((2, n_out)),
            dma(()),
            dma((n_out,)),
            dma(()),
            dma((n_out,)),
            dma(()),
            dma(()),
            dma(()),
            dma(()),
            dma(()),
            dma(()),
            dma(()),
            dma(()),
            dma(()),
            dma(()),
            dma((2,)),
            dma(()),
            dma(()),
            dma(()),
            dma((n,)),
            dma(()),
            dma(()),
            dma((n_out,)),
            dma(()),
            dma(()),
            dma(()),
            dma((4,)),
        ],
        compiler_params=pltpu.CompilerParams(
            collective_id=0, has_side_effects=True, vmem_limit_bytes=61 * 2**20
        ),
    )(grads, master, velocity, layer_offsets, layer_sizes, lars_skip)
    weights, nm, nv = pl.pallas_call(
        functools.partial(finish, (n, n_spa, shard, step, span)),
        out_shape=(
            jax.ShapeDtypeStruct((tiles, 8, 128), bf16),
            jax.ShapeDtypeStruct((shard,), f32),
            jax.ShapeDtypeStruct((shard,), f32),
        ),
        in_specs=[vmem] * 4,
        out_specs=(anywhere, anywhere, anywhere),
        scratch_shapes=[
            pltpu.VMEM((shard,), f32),
            pltpu.VMEM((shard,), f32),
            dma((PIECES + 1,)),
            dma((2,)),
        ],
        compiler_params=pltpu.CompilerParams(vmem_limit_bytes=16 * 2**20),
    )(ags.reshape(n * step, 8, 128), age, nmw, nvw)
    return weights.reshape(params), nm, nv


def tiled(n_rep, n_spa, params):
    n = n_rep * n_spa
    shard = params // n
    rest = shard % TILE
    n_out = n_rep // 4
    return (
        n_spa == 2
        and n_rep % 4 == 0
        and n_out == 4
        and params % TILE == 0
        and shard >= TILE
        and 0 < n * rest <= TILE
        and rest <= 128
    )


def step_fn(n_rep, n_spa, grads, *rest):
    if tiled(n_rep, n_spa, grads.shape[2]):
        return windowed(n_rep, n_spa, grads, *rest)
    return shards(grads, *rest)


def shards(grads, master, velocity, layer_offsets, layer_sizes, lars_skip):
    n_rep = lax.axis_size("replica")
    n_spa = lax.axis_size("spatial")
    shard = master.shape[0]
    position = lax.axis_index(("replica", "spatial")) * shard + jnp.arange(shard, dtype=jnp.int32)
    inside = (position[None, :] >= layer_offsets[:, None]) & (
        position[None, :] < (layer_offsets + layer_sizes)[:, None]
    )
    onehot = inside.astype(jnp.float32)
    received = lax.all_to_all(
        grads[0, 0].reshape(n_rep, n_spa * shard),
        "replica",
        split_axis=0,
        concat_axis=0,
        tiled=True,
    )
    first = jnp.sum(received.astype(jnp.float32), axis=0)
    summed = lax.psum_scatter(
        first.reshape(n_spa, shard), "spatial", scatter_dimension=0, tiled=True
    )
    grad = summed.reshape(shard) / (n_rep * n_spa)
    gsq_local = jnp.dot(onehot, grad * grad, precision=lax.Precision.HIGHEST)
    wsq_local = jnp.dot(onehot, master * master, precision=lax.Precision.HIGHEST)
    wsq, gsq = lax.psum((wsq_local, gsq_local), ("replica", "spatial"))
    wnorm = jnp.sqrt(wsq)
    gnorm = jnp.sqrt(gsq)
    skipped = lars_skip.astype(jnp.float32)
    ratio = 0.02 * wnorm / (gnorm + 0.001 * wnorm + 1e-06)
    trust = skipped + (1.0 - skipped) * ratio
    decay = (1.0 - skipped) * 0.001
    trust_pos = jnp.dot(trust, onehot, precision=lax.Precision.HIGHEST)
    decay_pos = jnp.dot(decay, onehot, precision=lax.Precision.HIGHEST)
    new_velocity = 0.9 * velocity + 8.0 * trust_pos * (grad + decay_pos * master)
    new_master = master - new_velocity
    new_weights = lax.all_gather(
        new_master.astype(jnp.bfloat16), ("replica", "spatial"), axis=0, tiled=True
    )
    return (new_weights, new_master, new_velocity)


def solution(mesh):
    return jax.shard_map(
        functools.partial(step_fn, mesh.shape["replica"], mesh.shape["spatial"]),
        mesh=mesh,
        in_specs=(
            P("replica", "spatial", None),
            P(("replica", "spatial")),
            P(("replica", "spatial")),
            P(),
            P(),
            P(),
        ),
        out_specs=(P(), P(("replica", "spatial")), P(("replica", "spatial"))),
        check_vma=False,
    )
```

```python
import functools

import jax
import jax.numpy as jnp
from jax import lax
from jax.experimental import pallas as pl
from jax.experimental.pallas import tpu as pltpu
from jax.sharding import PartitionSpec as P

MESH = pl.DeviceIdType.MESH
TILE = 1024
ZTILES = 4
SHARE = 6
PIECES = 8
RS = (
    "k1", "bar", "A1", "B1", "k2", "A2", "B2", "k3", "k4", "z1", "z2", "z3", "mv", "s1", "A3",
    "s2", "p1", "B3", "A4", "s3", "p2", "B4", "s4", "Z", "p3", "p4",
)
ZSEND = "mfn"
VISIT = "mnf"
COLUMN = "axyp"
AG = (
    "c0", "c1", "g0", "c2", "c3", "x0", "y0", "e0", "x1", "y1", "d0", "x2", "y2", "x3", "y3",
    "d1", "d2", "h1", "h2", "d3", "h3",
)
DIRECT = (0, 1, 2, 3)


def flip(i, k):
    out, bit = 0, 1
    while bit <= k:
        b = (i // bit) % 2
        out = out + bit * (1 - 2 * b) * ((k // bit) % 2)
        bit *= 2
    return i + out


def kernel(
    plan,
    grads_ref,
    m_ref,
    v_ref,
    offsets_in,
    sizes_in,
    skip_in,
    ags,
    age,
    nmw,
    nvw,
    offsets_ref,
    sizes_ref,
    skip_ref,
    m_in,
    v_in,
    gin,
    packed,
    r1x,
    r1y,
    sx,
    sy,
    r2x,
    r2y,
    rz1,
    zs,
    rz2,
    re1,
    ze,
    re2,
    part,
    recv3,
    mv,
    halo,
    grad_buf,
    layer_of,
    nvw_pre,
    step_pre,
    wrow,
    stats,
    in_sem,
    mv_sem,
    table_sem,
    ready,
    send1x,
    got1x,
    send1y,
    got1y,
    send2x,
    got2x,
    send2y,
    got2y,
    sendz1,
    gotz1,
    sendz2,
    gotz2,
    send_e1,
    got_e1,
    send_e2,
    got_e2,
    send3,
    got3,
    halo_sem,
    send_s,
    got_s,
    send4,
    got4,
    send_g,
    got_in,
    got_gz,
    got_gc,
    send_e,
    got_e,
    back_sem,
):
    n_out, shard, step, span, layers, hx, hy, hz = plan
    plane = 8
    n = n_out * plane
    chunk = (plane - 1) * step + span
    rows = span * 8
    hxy = hx + hy
    last = n_out - 1
    main = step - SHARE
    half_a = (main + 1) // 2
    half_b = main - half_a
    r = lax.axis_index("replica")
    y = lax.axis_index("spatial")
    d = r * 2 + y
    z = d // plane
    p = d % plane
    x = p // 4
    c = (p // 2) % 2
    base = d * (step * TILE)
    off = d * (shard - step * TILE)

    def dev(flat):
        return (flat // 2, flat % 2)

    def at(zz, xx, cc, yy):
        return ((zz * 2 + xx) * 2 + cc, yy)

    barrier = pltpu.get_barrier_semaphore()

    def load(zt):
        start = pl.multiple_of(zt * (plane * step * TILE), TILE)
        return pltpu.make_async_copy(
            grads_ref.at[0, :, pl.ds(start, chunk * TILE)], gin.at[zt], in_sem.at[zt]
        )

    h = z // 2
    order = [3 - 3 * h, 2 - h, flip(z, 1), z]
    for zt in order:
        load(zt).start()
    mv_loads = [
        pltpu.make_async_copy(ref, buf, mv_sem.at[j])
        for j, (ref, buf) in enumerate(((m_ref, m_in), (v_ref, v_in)))
    ]
    tables = [
        pltpu.make_async_copy(ref, buf, table_sem.at[j])
        for j, (ref, buf) in enumerate(
            ((offsets_in, offsets_ref), (sizes_in, sizes_ref), (skip_in, skip_ref))
        )
    ]
    for copy in mv_loads + tables:
        copy.start()

    def signal(sem, device):
        pl.semaphore_signal(sem, inc=1, device_id=device, device_id_type=MESH)

    def signal_z(sem, cores):
        @pl.when(z > 0)
        def _():
            for cc in cores:
                signal(sem, at(z - 1, x, cc, y))

        @pl.when(z < n_out - 1)
        def _():
            for cc in cores:
                signal(sem, at(z + 1, x, cc, y))

    n_z = jnp.where(z > 0, 1, 0) + jnp.where(z < n_out - 1, 1, 0)
    for device in (
        at(z, x, 1 - c, y),
        at(z, 1 - x, c, y),
        at(z, x, c, 1 - y),
        at(z, 1 - x, 1 - c, y),
        at(z, x, 1 - c, 1 - y),
    ):
        signal(barrier, device)
    signal_z(barrier, (c, 1 - c))

    group = max(g for g in range(1, 33) if chunk % g == 0)

    def pack(k):
        zt = order[k - 1]
        load(zt).wait()
        @pl.loop(0, chunk // group)
        def _(i):
            first = pl.multiple_of(i * (group * TILE), group * TILE)
            v = gin[zt, :, pl.ds(first, group * TILE)].astype(jnp.float32)
            packed[zt, pl.ds(i * group, group)] = v.reshape(group, 8, 128).astype(jnp.bfloat16)

    def remote(src, dst, send, recv, device):
        return pltpu.make_async_remote_copy(
            src_ref=src,
            dst_ref=dst,
            send_sem=send,
            recv_sem=recv,
            device_id=device,
            device_id_type=MESH,
        )

    def landed(ref, sem):
        pltpu.make_async_copy(ref, ref, sem).wait()

    def first(xx, cc, yy):
        return (xx * 4 + cc * 2 + yy) * step

    def send_raw(zt, h):
        yb, xb = (y, x) if h else (1 - y, 1 - x)
        for m in (3, 2, 1):
            xx, cc = (1 - x if m >= 2 else x), (1 - c if m % 2 else c)
            remote(
                packed.at[zt, pl.ds(first(xx, cc, yb), hx)],
                r1x.at[h, zt, m - 1],
                send1x,
                got1x.at[h, zt],
                at(z, xx, cc, y),
            ).start()
            yy = 1 - y if m >= 2 else y
            remote(
                packed.at[zt, pl.ds(first(xb, cc, yy) + hx, hy)],
                r1y.at[h, zt, m - 1],
                send1y,
                got1y.at[h, zt],
                at(z, x, cc, yy),
            ).start()

    def raws(zt, h, t, r1, own):
        v = packed[zt, own + t].astype(jnp.float32) + r1[h, zt, 0, t].astype(jnp.float32)
        return v + (r1[h, zt, 1, t].astype(jnp.float32) + r1[h, zt, 2, t].astype(jnp.float32))

    def sum_raw(zt):
        landed(r1x.at[0, zt], got1x.at[0, zt])
        own = first(x, c, 1 - y)

        @pl.loop(0, hx, unroll=2)
        def _(t):
            sx[zt, t] = raws(zt, 0, t, r1x, own)

        remote(sx.at[zt], r2x.at[zt], send2x, got2x.at[zt], at(z, x, c, 1 - y)).start()
        landed(r1y.at[0, zt], got1y.at[0, zt])
        own2 = first(1 - x, c, y) + hx

        @pl.loop(0, hy, unroll=2)
        def _(t):
            sy[zt, t] = raws(zt, 0, t, r1y, own2)

        remote(sy.at[zt], r2y.at[zt], send2y, got2y.at[zt], at(z, 1 - x, c, y)).start()

    def pass_on(zt, lo, size):
        rows = pl.ds(lo, size)
        to = at(zt, x, c, y)
        remote(part.at[zt, rows], recv3.at[z, rows], send3, got3, to).start()

    def sum_plane(zt, send):
        own = first(x, c, y)
        landed(r1x.at[1, zt], got1x.at[1, zt])
        landed(r2x.at[zt], got2x.at[zt])

        @pl.loop(0, hx, unroll=2)
        def _(t):
            part[zt, t] = raws(zt, 1, t, r1x, own) + r2x[zt, t]

        if send:
            pass_on(zt, 0, hx)
        landed(r1y.at[1, zt], got1y.at[1, zt])
        landed(r2y.at[zt], got2y.at[zt])

        @pl.loop(0, hy, unroll=2)
        def _(t):
            part[zt, hx + t] = raws(zt, 1, t, r1y, own + hx) + r2y[zt, t]

        if send:
            pass_on(zt, hx, hy)

    def send_far(zt, other):
        cc = 1 - c if other else c
        for j in range(4):
            remote(
                packed.at[zt, pl.ds(first(j // 2, cc, j % 2) + hxy, hz)],
                rz1.at[other * n_out + z, j],
                sendz1,
                gotz1,
                at(zt, x, cc, y),
            ).start()

        @pl.when((zt == last) & (cc == 1))
        def _():
            remote(
                packed.at[last, pl.ds(chunk - 1, 1)],
                re1.at[pl.ds(z * 2 + c, 1)],
                send_e1,
                got_e1,
                at(zt, x, cc, y),
            ).start()

    def send_distance(j):
        @pl.when(z >= j)
        def _():
            for other in (0, 1):
                send_far(z - j, other)

        @pl.when(z < n_out - j)
        def _():
            for other in (0, 1):
                send_far(z + j, other)

    def sum_far():
        landed(rz1.at[pl.ds(0, 2 * n_out - 1)], gotz1)

        @pl.loop(0, 4)
        def _(j):
            own = first(j // 2, c, j % 2) + hxy
            for t in range(hz):
                acc = packed[z, own + t].astype(jnp.float32)
                acc = acc + rz1[n_out + z, j, t].astype(jnp.float32)
                for k in range(1, n_out):
                    zz = (z + k) % n_out
                    two = rz1[zz, j, t].astype(jnp.float32)
                    acc = acc + (two + rz1[n_out + zz, j, t].astype(jnp.float32))
                zs[j, t] = acc

        for m in (3, 2, 1):
            xx, yy = (1 - x if m >= 2 else x), (1 - y if m % 2 else y)
            remote(zs.at[xx * 2 + yy], rz2.at[m - 1], sendz2, gotz2, at(z, xx, c, yy)).start()

        @pl.when((z == last) & (c == 1))
        def _():
            landed(re1.at[pl.ds(0, 2 * n_out - 1)], got_e1)
            acc = packed[last, chunk - 1].astype(jnp.float32)
            for j in range(2 * n_out - 1):
                acc = acc + re1[j].astype(jnp.float32)
            ze[0] = acc

            @pl.when(x * 2 + y < 3)
            def _():
                remote(
                    ze, re2.at[pl.ds(x * 2 + y, 1)], send_e2, got_e2, at(z, 1, 1, 1)
                ).start()

    lane = lax.broadcasted_iota(jnp.int32, (rows, 128), 1)
    shift_l = off % 128
    shift_r = off // 128
    whole = step * TILE

    def window(j, ref):
        mv_loads[j].wait()
        edge = jnp.pad(ref[pl.ds(whole, shard - whole)], (0, 128 - (shard - whole)))
        edge = jnp.broadcast_to(edge.reshape(1, 128), (8, 128))
        w = jnp.concatenate([ref[pl.ds(0, whole)].reshape(step * 8, 128), edge], 0)
        w = pltpu.roll(w, shift_l, 1)
        w = jnp.where(lane < shift_l, pltpu.roll(w, 1, 0), w)
        w = pltpu.roll(w, shift_r, 0)
        mv[:, j] = w.reshape(span, 8, 128)

    place = lax.broadcasted_iota(jnp.int32, (8, 128), 0) * 128 + lax.broadcasted_iota(
        jnp.int32, (8, 128), 1
    )
    low, high, own_low, own_high = [], [], [], []

    def bounds():
        for copy in tables:
            copy.wait()
        for l in range(layers):
            low.append(offsets_ref[l] - base)
            high.append(offsets_ref[l] + sizes_ref[l] - base)
            own_low.append(jnp.maximum(low[l], off))
            own_high.append(jnp.minimum(high[l], off + shard))

    lane1 = lax.broadcasted_iota(jnp.int32, (1, 128), 1)

    def squares(value, start, stop, lows, highs, sums=None):
        def add(t, accs):
            pos = place + t * TILE
            v = value(t)
            v = v * v
            return tuple(
                acc + jnp.where((pos >= lo) & (pos < hi), v, 0.0)
                for acc, lo, hi in zip(accs, lows, highs)
            )

        if sums is None:
            sums = tuple(jnp.zeros((8, 128), jnp.float32) for _ in range(layers))
        return lax.fori_loop(start, stop, add, sums)

    sub8 = lax.broadcasted_iota(jnp.int32, (8, 128), 0)
    lane8 = lax.broadcasted_iota(jnp.int32, (8, 128), 1)

    def as_row(sums, first):
        rows8 = jnp.zeros((8, 128), jnp.float32)
        for l, acc in enumerate(sums):
            rows8 = jnp.where(sub8 == l, jnp.sum(acc, axis=0, keepdims=True), rows8)
        totals = jnp.sum(rows8, axis=1, keepdims=True)
        return jnp.sum(jnp.where(lane8 == sub8 + first, totals, 0.0), axis=0, keepdims=True)

    def step_z(j):
        if j == 1:
            send_distance(1)
            send_far(z, 1)
            return
        pl.semaphore_wait(ready.at[j - 2], n_z)
        if j < n_out - 1:
            signal_z(ready.at[j - 1], (c,))
        send_distance(j)

    for op in RS:
        i = int(op[1:] or 0) if op != "bar" and op != "mv" else 0
        zt = order[i - 1]
        if op == "bar":
            pl.semaphore_wait(barrier, 5 + 2 * n_z)
            signal_z(ready.at[0], (c,))
        elif op == "mv":
            bounds()
            for j, ref in enumerate((m_in, v_in)):
                window(j, ref)
            wrow[...] = as_row(squares(lambda t: mv[t, 0], 0, span, own_low, own_high), 0)
        elif op[0] == "k":
            pack(i)
        elif op[0] == "A":
            send_raw(zt, 0)
        elif op[0] == "B":
            send_raw(zt, 1)
        elif op[0] == "z":
            step_z(i)
        elif op[0] == "Z":
            sum_far()
        elif op[0] == "s":
            sum_raw(zt)
        elif op[0] == "p":
            sum_plane(zt, i < n_out)

    landed(recv3.at[pl.ds(0, n_out - 1)], got3)
    halo_copy = remote(mv.at[span - 1], halo, halo_sem.at[0], halo_sem.at[1], dev((d + 1) % n))
    halo_copy.start()
    landed(rz2, gotz2)
    for t in range(hz):
        acc = zs[x * 2 + y, t] + rz2[0, t]
        grad_buf[hxy + t] = (acc + (rz2[1, t] + rz2[2, t])) / n
    grad_buf[step] = jnp.zeros((8, 128), jnp.float32)

    @pl.when(d == n - 1)
    def _():
        landed(re2, got_e2)
        grad_buf[step] = (ze[0] + re2[0] + (re2[1] + re2[2])) / n

    def total_grad(t):
        acc = part[z, t]
        for k in range(1, n_out):
            acc = acc + recv3[(z + k) % n_out, t]
        acc = acc / n
        grad_buf[t] = acc
        return acc

    sums = squares(total_grad, 0, hxy, low, high)
    sums = squares(lambda t: grad_buf[t], hxy, span, low, high, sums)
    stats[d] = as_row(sums, layers) + wrow[...]

    for k in range(n_out - 1, -1, -1):
        for q in range(plane - 1, -1, -1):
            if k + q > 0:
                peer = flip(z, k) * plane + flip(p, q)
                remote(stats.at[d], stats.at[d], send_s, got_s, dev(peer)).start()

    skip_row = jnp.zeros((1, 128), jnp.float32)
    for l in range(layers):
        skip_row = jnp.where(lane1 == l, skip_ref[l].astype(jnp.float32), skip_row)

    def prepare(t):
        pos = place + t * TILE
        which = jnp.zeros((8, 128), jnp.int32)
        decay = jnp.zeros((8, 128), jnp.float32)
        for l in range(layers):
            inside = (pos >= low[l]) & (pos < high[l])
            which = jnp.where(inside, l, which)
            decay = jnp.where(inside, (1.0 - skip_ref[l].astype(jnp.float32)) * 0.001, decay)
        layer_of[t] = which
        nvw_pre[t] = 0.9 * mv[t, 1]
        step_pre[t] = 8.0 * (grad_buf[t] + decay * mv[t, 0])

    @pl.loop(1, span)
    def _(t):
        prepare(t)

    halo_copy.wait()
    for j in range(2):
        mv[0, j] = jnp.where(place < off, halo[j], mv[0, j])
    prepare(0)

    landed(stats.at[pl.ds(0, n - 1)], got_s)
    norms = jnp.sqrt(jnp.sum(stats[...], axis=0))
    wnorm = jnp.broadcast_to(norms, (8, 128))
    gnorm = pltpu.roll(wnorm, 128 - layers, 1)
    ratio = 0.02 * wnorm / (gnorm + 0.001 * wnorm + 1e-06)
    trust_row = skip_row + (1.0 - skip_row) * ratio
    trust = [
        jnp.sum(jnp.where(lane1 == l, trust_row, 0.0), axis=1, keepdims=True)
        for l in range(layers)
    ]

    def update(t):
        which = layer_of[t]
        trust_pos = jnp.broadcast_to(trust[0], (8, 128))
        for l in range(1, layers):
            trust_pos = jnp.where(which == l, trust[l], trust_pos)
        nv = nvw_pre[t] + trust_pos * step_pre[t]
        nm = mv[t, 0] - nv
        nvw[t] = nv
        nmw[t] = nm
        return nm.astype(jnp.bfloat16)

    x_side = at(z, 1 - x, c, y)
    y_side = at(z, x, c, 1 - y)
    across = at(z, 1 - x, c, 1 - y)
    partner = at(z, x, 1 - c, y)

    def share(b):
        return ags.at[b, pl.ds(main, SHARE)]

    for t in range(main, step):
        ags[d, t] = update(t)
    for device in (across, x_side, y_side):
        remote(share(d), share(d), send_g, got_in, device).start()

    @pl.loop(0, main)
    def _(t):
        ags[d, t] = update(t)

    def send_edge():
        for i, ref in enumerate((nmw, nvw)):
            remote(ref.at[0], ref.at[step], back_sem.at[i], back_sem.at[2 + i], dev(d - 1)).start()

    def block(zz, xx, cc, yy):
        return zz * plane + xx * 4 + cc * 2 + yy

    def forward(b, device, lo=0, size=main):
        piece = ags.at[b, pl.ds(lo, size)]
        remote(piece, piece, send4, got4.at[b], device).start()

    def arrived(b):
        landed(ags.at[b, pl.ds(0, main)], got4.at[b])

    zone = {"m": flip(z, 1), "n": 2 - h, "f": 3 - 3 * h}
    visits = [z] + [zone[k] for k in VISIT]
    sends = [zone[k] for k in ZSEND]

    def tiles(count):
        return ags.at[pl.ds(0, count), pl.ds(0, SHARE)]

    def z_share():
        landed(tiles(3), got_in)
        for j in range(4):
            b = block(z, j // 2, c, j % 2)
            for to in sends:
                peer = at(to, x, c, y)
                remote(share(b), share(b), send_g, got_gz.at[z], peer).start()
            remote(share(b), share(b), send_g, got_gc, partner).start()

    def z_arrived(k):
        landed(tiles(4), got_gz.at[visits[k]])
        for j in range(4):
            b = block(visits[k], j // 2, c, j % 2)
            remote(share(b), share(b), send_g, got_gc, partner).start()

    for to in sends:
        forward(d, at(to, x, c, y))

    def column(k):
        b = block(visits[k], x, c, y)
        if k > 0:
            arrived(b)
        for way in COLUMN:
            if way == "x":
                forward(b, x_side)
            elif way == "y":
                forward(b, y_side)
            elif way == "p":
                forward(b, partner)
            elif k in DIRECT:
                forward(b, across)

    def from_y(k):
        b = block(visits[k], x, c, 1 - y)
        arrived(b)
        if k not in DIRECT:
            forward(b, x_side, 0, half_a)
        forward(b, partner)

    def from_x(k):
        b = block(visits[k], 1 - x, c, y)
        arrived(b)
        if k not in DIRECT:
            forward(b, y_side, half_a, half_b)
        forward(b, partner)

    def corner(k):
        b = block(visits[k], 1 - x, c, 1 - y)
        arrived(b)
        forward(b, partner)

    def edges():
        @pl.when(d > 0)
        def _():
            send_edge()

        @pl.when(d == n - 1)
        def _():
            age[0] = update(step)
            for q in range(1, n):
                remote(age, age, send_e, got_e, dev(d - q)).start()

    for op in AG:
        i = int(op[1:])
        if op[0] == "c":
            column(i)
        elif op[0] == "x":
            from_x(i)
        elif op[0] == "y":
            from_y(i)
        elif op[0] == "d":
            corner(i)
        elif op[0] == "g":
            z_share()
        elif op[0] == "h":
            z_arrived(i)
        elif op[0] == "e":
            edges()

    @pl.loop(0, n_out)
    def _(k):
        for xx in range(2):
            for yy in range(2):
                arrived(block(k, xx, 1 - c, yy))

    landed(tiles(4 * n_out), got_gc)

    @pl.when(d < n - 1)
    def _():
        landed(age, got_e)
        for i, ref in enumerate((nmw, nvw)):
            landed(ref.at[step], back_sem.at[2 + i])

    @pl.when(d == n - 1)
    def _():
        landed(ags.at[pl.ds(0, n - 1), 0], send_e)

    @pl.when(d > 0)
    def _():
        for i, ref in enumerate((nmw, nvw)):
            landed(ref.at[step], back_sem.at[i])

    @pl.when((z != last) | (c != 1))
    def _():
        landed(re1.at[pl.ds(0, 1)], send_e1)

    @pl.when((z == last) & (c == 1) & (x * 2 + y < 3))
    def _():
        landed(ze, send_e2)

    for ref, sem in (
        (r1x, send1x),
        (r1y, send1y),
        (r2x, send2x),
        (r2y, send2y),
        (rz1.at[pl.ds(0, 2 * n_out - 1)], sendz1),
        (rz2, sendz2),
        (recv3.at[pl.ds(0, n_out - 1)], send3),
        (stats.at[pl.ds(0, n - 1)], send_s),
        (ags.at[pl.ds(0, n - 1), pl.ds(0, main)], send4),
        (tiles(n - 1), send_g),
    ):
        landed(ref, sem)


def finish(
    plan,
    ags,
    age,
    nmw,
    nvw,
    out_ref,
    nm_ref,
    nv_ref,
    nm_out,
    nv_out,
    out_sem,
    own_sem,
):
    n, n_spa, shard, step, span = plan
    rows = span * 8
    whole = step * TILE
    part = n * step // PIECES
    copies = [
        pltpu.make_async_copy(
            ags.at[pl.ds(i * part, part)], out_ref.at[pl.ds(i * part, part)], out_sem.at[i]
        )
        for i in range(PIECES)
    ]
    copies.append(
        pltpu.make_async_copy(age, out_ref.at[pl.ds(n * step, 1)], out_sem.at[PIECES])
    )
    for copy in copies:
        copy.start()
    d = lax.axis_index("replica") * n_spa + lax.axis_index("spatial")
    off = d * (shard - whole)
    shift_l = off % 128
    shift_r = off // 128
    back_l = 128 - shift_l
    lane = lax.broadcasted_iota(jnp.int32, (rows, 128), 1)
    for j, (src, buf, ref) in enumerate(((nmw, nm_out, nm_ref), (nvw, nv_out, nv_ref))):
        x = src[...].reshape(rows, 128)
        x = pltpu.roll(x, (rows - shift_r) % rows, 0)
        x = pltpu.roll(x, back_l % 128, 1)
        x = jnp.where(lane < back_l, x, pltpu.roll(x, rows - 1, 0))
        buf[pl.ds(0, whole)] = x[: step * 8].reshape(whole)
        buf[pl.ds(whole, shard - whole)] = x[step * 8, : shard - whole].reshape(shard - whole)
        copy = pltpu.make_async_copy(buf, ref, own_sem.at[j])
        copy.start()
        copies.append(copy)
    for copy in copies:
        copy.wait()


def windowed(n_rep, n_spa, grads, master, velocity, layer_offsets, layer_sizes, lars_skip):
    shard = master.shape[0]
    params = grads.shape[2]
    layers = layer_offsets.shape[0]
    plane = 8
    n = n_rep * n_spa
    n_out = n // plane
    step = shard // TILE
    span = params // TILE - (n - 1) * step
    chunk = (plane - 1) * step + span
    tiles = params // TILE
    hz = ZTILES
    hx = (step - hz + 1) // 2
    hy = step - hz - hx
    plan = (n_out, shard, step, span, layers, hx, hy, hz)
    vmem = pl.BlockSpec(memory_space=pltpu.VMEM)
    anywhere = pl.BlockSpec(memory_space=pltpu.HBM)
    f32, bf16 = jnp.float32, jnp.bfloat16
    dma = pltpu.SemaphoreType.DMA
    ags, age, nmw, nvw = pl.pallas_call(
        functools.partial(kernel, plan),
        out_shape=(
            pltpu.VMEM((n, step, 8, 128), bf16),
            pltpu.VMEM((1, 8, 128), bf16),
            pltpu.VMEM((span, 8, 128), f32),
            pltpu.VMEM((span, 8, 128), f32),
        ),
        in_specs=[anywhere] * 6,
        out_specs=(vmem,) * 4,
        scratch_shapes=[
            pltpu.SMEM((layers,), jnp.int32),
            pltpu.SMEM((layers,), jnp.int32),
            pltpu.SMEM((layers,), jnp.int32),
            pltpu.VMEM((shard,), f32),
            pltpu.VMEM((shard,), f32),
            pltpu.VMEM((n_out, 1, chunk * TILE), bf16),
            pltpu.VMEM((n_out, chunk, 8, 128), bf16),
            pltpu.VMEM((2, n_out, 3, hx, 8, 128), bf16),
            pltpu.VMEM((2, n_out, 3, hy, 8, 128), bf16),
            pltpu.VMEM((n_out, hx, 8, 128), f32),
            pltpu.VMEM((n_out, hy, 8, 128), f32),
            pltpu.VMEM((n_out, hx, 8, 128), f32),
            pltpu.VMEM((n_out, hy, 8, 128), f32),
            pltpu.VMEM((2 * n_out, 4, hz, 8, 128), bf16),
            pltpu.VMEM((4, hz, 8, 128), f32),
            pltpu.VMEM((3, hz, 8, 128), f32),
            pltpu.VMEM((2 * n_out, 8, 128), bf16),
            pltpu.VMEM((1, 8, 128), f32),
            pltpu.VMEM((3, 8, 128), f32),
            pltpu.VMEM((n_out, hx + hy, 8, 128), f32),
            pltpu.VMEM((n_out, hx + hy, 8, 128), f32),
            pltpu.VMEM((span, 2, 8, 128), f32),
            pltpu.VMEM((2, 8, 128), f32),
            pltpu.VMEM((span, 8, 128), f32),
            pltpu.VMEM((span, 8, 128), jnp.int32),
            pltpu.VMEM((span, 8, 128), f32),
            pltpu.VMEM((span, 8, 128), f32),
            pltpu.VMEM((1, 128), f32),
            pltpu.VMEM((n, 1, 128), f32),
            dma((n_out,)),
            dma((2,)),
            dma((3,)),
            pltpu.SemaphoreType.REGULAR((n_out,)),
            dma(()),
            dma((2, n_out)),
            dma(()),
            dma((2, n_out)),
            dma(()),
            dma((n_out,)),
            dma(()),
            dma((n_out,)),
            dma(()),
            dma(()),
            dma(()),
            dma(()),
            dma(()),
            dma(()),
            dma(()),
            dma(()),
            dma(()),
            dma(()),
            dma((2,)),
            dma(()),
            dma(()),
            dma(()),
            dma((n,)),
            dma(()),
            dma(()),
            dma((n_out,)),
            dma(()),
            dma(()),
            dma(()),
            dma((4,)),
        ],
        compiler_params=pltpu.CompilerParams(
            collective_id=0, has_side_effects=True, vmem_limit_bytes=61 * 2**20
        ),
    )(grads, master, velocity, layer_offsets, layer_sizes, lars_skip)
    weights, nm, nv = pl.pallas_call(
        functools.partial(finish, (n, n_spa, shard, step, span)),
        out_shape=(
            jax.ShapeDtypeStruct((tiles, 8, 128), bf16),
            jax.ShapeDtypeStruct((shard,), f32),
            jax.ShapeDtypeStruct((shard,), f32),
        ),
        in_specs=[vmem] * 4,
        out_specs=(anywhere, anywhere, anywhere),
        scratch_shapes=[
            pltpu.VMEM((shard,), f32),
            pltpu.VMEM((shard,), f32),
            dma((PIECES + 1,)),
            dma((2,)),
        ],
        compiler_params=pltpu.CompilerParams(vmem_limit_bytes=16 * 2**20),
    )(ags.reshape(n * step, 8, 128), age, nmw, nvw)
    return weights.reshape(params), nm, nv


def tiled(n_rep, n_spa, params, layers):
    n = n_rep * n_spa
    shard = params // n
    rest = shard % TILE
    n_out = n_rep // 4
    return (
        n_spa == 2
        and n_rep % 4 == 0
        and n_out == 4
        and layers <= 8
        and params % TILE == 0
        and shard >= TILE
        and 0 < n * rest <= TILE
        and rest <= 128
    )


def step_fn(n_rep, n_spa, grads, *rest):
    if tiled(n_rep, n_spa, grads.shape[2], rest[2].shape[0]):
        return windowed(n_rep, n_spa, grads, *rest)
    return shards(grads, *rest)


def shards(grads, master, velocity, layer_offsets, layer_sizes, lars_skip):
    n_rep = lax.axis_size("replica")
    n_spa = lax.axis_size("spatial")
    shard = master.shape[0]
    position = lax.axis_index(("replica", "spatial")) * shard + jnp.arange(shard, dtype=jnp.int32)
    inside = (position[None, :] >= layer_offsets[:, None]) & (
        position[None, :] < (layer_offsets + layer_sizes)[:, None]
    )
    onehot = inside.astype(jnp.float32)
    received = lax.all_to_all(
        grads[0, 0].reshape(n_rep, n_spa * shard),
        "replica",
        split_axis=0,
        concat_axis=0,
        tiled=True,
    )
    first = jnp.sum(received.astype(jnp.float32), axis=0)
    summed = lax.psum_scatter(
        first.reshape(n_spa, shard), "spatial", scatter_dimension=0, tiled=True
    )
    grad = summed.reshape(shard) / (n_rep * n_spa)
    gsq_local = jnp.dot(onehot, grad * grad, precision=lax.Precision.HIGHEST)
    wsq_local = jnp.dot(onehot, master * master, precision=lax.Precision.HIGHEST)
    wsq, gsq = lax.psum((wsq_local, gsq_local), ("replica", "spatial"))
    wnorm = jnp.sqrt(wsq)
    gnorm = jnp.sqrt(gsq)
    skipped = lars_skip.astype(jnp.float32)
    ratio = 0.02 * wnorm / (gnorm + 0.001 * wnorm + 1e-06)
    trust = skipped + (1.0 - skipped) * ratio
    decay = (1.0 - skipped) * 0.001
    trust_pos = jnp.dot(trust, onehot, precision=lax.Precision.HIGHEST)
    decay_pos = jnp.dot(decay, onehot, precision=lax.Precision.HIGHEST)
    new_velocity = 0.9 * velocity + 8.0 * trust_pos * (grad + decay_pos * master)
    new_master = master - new_velocity
    new_weights = lax.all_gather(
        new_master.astype(jnp.bfloat16), ("replica", "spatial"), axis=0, tiled=True
    )
    return (new_weights, new_master, new_velocity)


def solution(mesh):
    return jax.shard_map(
        functools.partial(step_fn, mesh.shape["replica"], mesh.shape["spatial"]),
        mesh=mesh,
        in_specs=(
            P("replica", "spatial", None),
            P(("replica", "spatial")),
            P(("replica", "spatial")),
            P(),
            P(),
            P(),
        ),
        out_specs=(P(), P(("replica", "spatial")), P(("replica", "spatial"))),
        check_vma=False,
    )
```

```python
import functools

import jax
import jax.numpy as jnp
from jax import lax
from jax.experimental import pallas as pl
from jax.experimental.pallas import tpu as pltpu
from jax.sharding import PartitionSpec as P

MESH = pl.DeviceIdType.MESH
TILE = 1024
ZTILES = 4
SHARE = 6
PIECES = 8
RS = (
    "k1", "bar", "A1", "B1", "k2", "A2", "B2", "k3", "k4", "z1", "z2", "z3", "mv", "s1", "A3",
    "s2", "p1", "B3", "A4", "s3", "p2", "B4", "s4", "Z", "p3", "p4",
)
ZSEND = "mfn"
VISIT = "mnf"
COLUMN = "axyp"
AG = (
    "c0", "c1", "g0", "c2", "c3", "x0", "y0", "e0", "x1", "y1", "d0", "x2", "y2", "x3", "y3",
    "d1", "d2", "h1", "h2", "n0", "d3", "h3",
)
DIRECT = (0, 1, 2, 3)


def flip(i, k):
    out, bit = 0, 1
    while bit <= k:
        b = (i // bit) % 2
        out = out + bit * (1 - 2 * b) * ((k // bit) % 2)
        bit *= 2
    return i + out


def kernel(
    plan,
    grads_ref,
    m_ref,
    v_ref,
    offsets_in,
    sizes_in,
    skip_in,
    ags,
    age,
    nm_out,
    nv_out,
    nmw,
    nvw,
    offsets_ref,
    sizes_ref,
    skip_ref,
    m_in,
    v_in,
    gin,
    packed,
    r1x,
    r1y,
    sx,
    sy,
    r2x,
    r2y,
    rz1,
    zs,
    rz2,
    re1,
    ze,
    re2,
    part,
    recv3,
    mv,
    halo,
    grad_buf,
    layer_of,
    nvw_pre,
    step_pre,
    wrow,
    stats,
    in_sem,
    mv_sem,
    table_sem,
    ready,
    send1x,
    got1x,
    send1y,
    got1y,
    send2x,
    got2x,
    send2y,
    got2y,
    sendz1,
    gotz1,
    sendz2,
    gotz2,
    send_e1,
    got_e1,
    send_e2,
    got_e2,
    send3,
    got3,
    halo_sem,
    send_s,
    got_s,
    send4,
    got4,
    send_g,
    got_in,
    got_gz,
    got_gc,
    send_e,
    got_e,
    back_sem,
):
    n_out, shard, step, span, layers, hx, hy, hz = plan
    plane = 8
    n = n_out * plane
    chunk = (plane - 1) * step + span
    rows = span * 8
    hxy = hx + hy
    last = n_out - 1
    main = step - SHARE
    half_a = (main + 1) // 2
    half_b = main - half_a
    r = lax.axis_index("replica")
    y = lax.axis_index("spatial")
    d = r * 2 + y
    z = d // plane
    p = d % plane
    x = p // 4
    c = (p // 2) % 2
    base = d * (step * TILE)
    off = d * (shard - step * TILE)

    def dev(flat):
        return (flat // 2, flat % 2)

    def at(zz, xx, cc, yy):
        return ((zz * 2 + xx) * 2 + cc, yy)

    barrier = pltpu.get_barrier_semaphore()

    def load(zt):
        start = pl.multiple_of(zt * (plane * step * TILE), TILE)
        return pltpu.make_async_copy(
            grads_ref.at[0, :, pl.ds(start, chunk * TILE)], gin.at[zt], in_sem.at[zt]
        )

    h = z // 2
    order = [3 - 3 * h, 2 - h, flip(z, 1), z]
    for zt in order:
        load(zt).start()
    mv_loads = [
        pltpu.make_async_copy(ref, buf, mv_sem.at[j])
        for j, (ref, buf) in enumerate(((m_ref, m_in), (v_ref, v_in)))
    ]
    tables = [
        pltpu.make_async_copy(ref, buf, table_sem.at[j])
        for j, (ref, buf) in enumerate(
            ((offsets_in, offsets_ref), (sizes_in, sizes_ref), (skip_in, skip_ref))
        )
    ]
    for copy in mv_loads + tables:
        copy.start()

    def signal(sem, device):
        pl.semaphore_signal(sem, inc=1, device_id=device, device_id_type=MESH)

    def signal_z(sem, cores):
        @pl.when(z > 0)
        def _():
            for cc in cores:
                signal(sem, at(z - 1, x, cc, y))

        @pl.when(z < n_out - 1)
        def _():
            for cc in cores:
                signal(sem, at(z + 1, x, cc, y))

    n_z = jnp.where(z > 0, 1, 0) + jnp.where(z < n_out - 1, 1, 0)
    for device in (
        at(z, x, 1 - c, y),
        at(z, 1 - x, c, y),
        at(z, x, c, 1 - y),
        at(z, 1 - x, 1 - c, y),
        at(z, x, 1 - c, 1 - y),
    ):
        signal(barrier, device)
    signal_z(barrier, (c, 1 - c))

    group = max(g for g in range(1, 33) if chunk % g == 0)

    def pack(k):
        zt = order[k - 1]
        load(zt).wait()
        @pl.loop(0, chunk // group)
        def _(i):
            first = pl.multiple_of(i * (group * TILE), group * TILE)
            v = gin[zt, :, pl.ds(first, group * TILE)].astype(jnp.float32)
            packed[zt, pl.ds(i * group, group)] = v.reshape(group, 8, 128).astype(jnp.bfloat16)

    def remote(src, dst, send, recv, device):
        return pltpu.make_async_remote_copy(
            src_ref=src,
            dst_ref=dst,
            send_sem=send,
            recv_sem=recv,
            device_id=device,
            device_id_type=MESH,
        )

    def landed(ref, sem):
        pltpu.make_async_copy(ref, ref, sem).wait()

    def first(xx, cc, yy):
        return (xx * 4 + cc * 2 + yy) * step

    def send_raw(zt, h):
        yb, xb = (y, x) if h else (1 - y, 1 - x)
        for m in (3, 2, 1):
            xx, cc = (1 - x if m >= 2 else x), (1 - c if m % 2 else c)
            remote(
                packed.at[zt, pl.ds(first(xx, cc, yb), hx)],
                r1x.at[h, zt, m - 1],
                send1x,
                got1x.at[h, zt],
                at(z, xx, cc, y),
            ).start()
            yy = 1 - y if m >= 2 else y
            remote(
                packed.at[zt, pl.ds(first(xb, cc, yy) + hx, hy)],
                r1y.at[h, zt, m - 1],
                send1y,
                got1y.at[h, zt],
                at(z, x, cc, yy),
            ).start()

    def raws(zt, h, t, r1, own):
        v = packed[zt, own + t].astype(jnp.float32) + r1[h, zt, 0, t].astype(jnp.float32)
        return v + (r1[h, zt, 1, t].astype(jnp.float32) + r1[h, zt, 2, t].astype(jnp.float32))

    def sum_raw(zt):
        landed(r1x.at[0, zt], got1x.at[0, zt])
        own = first(x, c, 1 - y)

        @pl.loop(0, hx, unroll=2)
        def _(t):
            sx[zt, t] = raws(zt, 0, t, r1x, own)

        remote(sx.at[zt], r2x.at[zt], send2x, got2x.at[zt], at(z, x, c, 1 - y)).start()
        landed(r1y.at[0, zt], got1y.at[0, zt])
        own2 = first(1 - x, c, y) + hx

        @pl.loop(0, hy, unroll=2)
        def _(t):
            sy[zt, t] = raws(zt, 0, t, r1y, own2)

        remote(sy.at[zt], r2y.at[zt], send2y, got2y.at[zt], at(z, 1 - x, c, y)).start()

    def pass_on(zt, lo, size):
        rows = pl.ds(lo, size)
        to = at(zt, x, c, y)
        remote(part.at[zt, rows], recv3.at[z, rows], send3, got3, to).start()

    def sum_plane(zt, send):
        own = first(x, c, y)
        landed(r1x.at[1, zt], got1x.at[1, zt])
        landed(r2x.at[zt], got2x.at[zt])

        @pl.loop(0, hx, unroll=2)
        def _(t):
            part[zt, t] = raws(zt, 1, t, r1x, own) + r2x[zt, t]

        if send:
            pass_on(zt, 0, hx)
        landed(r1y.at[1, zt], got1y.at[1, zt])
        landed(r2y.at[zt], got2y.at[zt])

        @pl.loop(0, hy, unroll=2)
        def _(t):
            part[zt, hx + t] = raws(zt, 1, t, r1y, own + hx) + r2y[zt, t]

        if send:
            pass_on(zt, hx, hy)

    def send_far(zt, other):
        cc = 1 - c if other else c
        for j in range(4):
            remote(
                packed.at[zt, pl.ds(first(j // 2, cc, j % 2) + hxy, hz)],
                rz1.at[other * n_out + z, j],
                sendz1,
                gotz1,
                at(zt, x, cc, y),
            ).start()

        @pl.when((zt == last) & (cc == 1))
        def _():
            remote(
                packed.at[last, pl.ds(chunk - 1, 1)],
                re1.at[pl.ds(z * 2 + c, 1)],
                send_e1,
                got_e1,
                at(zt, x, cc, y),
            ).start()

    def send_distance(j):
        @pl.when(z >= j)
        def _():
            for other in (0, 1):
                send_far(z - j, other)

        @pl.when(z < n_out - j)
        def _():
            for other in (0, 1):
                send_far(z + j, other)

    def sum_far():
        landed(rz1.at[pl.ds(0, 2 * n_out - 1)], gotz1)

        @pl.loop(0, 4)
        def _(j):
            own = first(j // 2, c, j % 2) + hxy
            for t in range(hz):
                acc = packed[z, own + t].astype(jnp.float32)
                acc = acc + rz1[n_out + z, j, t].astype(jnp.float32)
                for k in range(1, n_out):
                    zz = (z + k) % n_out
                    two = rz1[zz, j, t].astype(jnp.float32)
                    acc = acc + (two + rz1[n_out + zz, j, t].astype(jnp.float32))
                zs[j, t] = acc

        for m in (3, 2, 1):
            xx, yy = (1 - x if m >= 2 else x), (1 - y if m % 2 else y)
            remote(zs.at[xx * 2 + yy], rz2.at[m - 1], sendz2, gotz2, at(z, xx, c, yy)).start()

        @pl.when((z == last) & (c == 1))
        def _():
            landed(re1.at[pl.ds(0, 2 * n_out - 1)], got_e1)
            acc = packed[last, chunk - 1].astype(jnp.float32)
            for j in range(2 * n_out - 1):
                acc = acc + re1[j].astype(jnp.float32)
            ze[0] = acc

            @pl.when(x * 2 + y < 3)
            def _():
                remote(
                    ze, re2.at[pl.ds(x * 2 + y, 1)], send_e2, got_e2, at(z, 1, 1, 1)
                ).start()

    lane = lax.broadcasted_iota(jnp.int32, (rows, 128), 1)
    shift_l = off % 128
    shift_r = off // 128
    whole = step * TILE

    def window(j, ref):
        mv_loads[j].wait()
        edge = jnp.pad(ref[pl.ds(whole, shard - whole)], (0, 128 - (shard - whole)))
        edge = jnp.broadcast_to(edge.reshape(1, 128), (8, 128))
        w = jnp.concatenate([ref[pl.ds(0, whole)].reshape(step * 8, 128), edge], 0)
        w = pltpu.roll(w, shift_l, 1)
        w = jnp.where(lane < shift_l, pltpu.roll(w, 1, 0), w)
        w = pltpu.roll(w, shift_r, 0)
        mv[:, j] = w.reshape(span, 8, 128)

    place = lax.broadcasted_iota(jnp.int32, (8, 128), 0) * 128 + lax.broadcasted_iota(
        jnp.int32, (8, 128), 1
    )
    low, high, own_low, own_high = [], [], [], []

    def bounds():
        for copy in tables:
            copy.wait()
        for l in range(layers):
            low.append(offsets_ref[l] - base)
            high.append(offsets_ref[l] + sizes_ref[l] - base)
            own_low.append(jnp.maximum(low[l], off))
            own_high.append(jnp.minimum(high[l], off + shard))

    lane1 = lax.broadcasted_iota(jnp.int32, (1, 128), 1)

    def squares(value, start, stop, lows, highs, sums=None):
        def add(t, accs):
            pos = place + t * TILE
            v = value(t)
            v = v * v
            return tuple(
                acc + jnp.where((pos >= lo) & (pos < hi), v, 0.0)
                for acc, lo, hi in zip(accs, lows, highs)
            )

        if sums is None:
            sums = tuple(jnp.zeros((8, 128), jnp.float32) for _ in range(layers))
        return lax.fori_loop(start, stop, add, sums)

    sub8 = lax.broadcasted_iota(jnp.int32, (8, 128), 0)
    lane8 = lax.broadcasted_iota(jnp.int32, (8, 128), 1)

    def as_row(sums, first):
        rows8 = jnp.zeros((8, 128), jnp.float32)
        for l, acc in enumerate(sums):
            rows8 = jnp.where(sub8 == l, jnp.sum(acc, axis=0, keepdims=True), rows8)
        totals = jnp.sum(rows8, axis=1, keepdims=True)
        return jnp.sum(jnp.where(lane8 == sub8 + first, totals, 0.0), axis=0, keepdims=True)

    def step_z(j):
        if j == 1:
            send_distance(1)
            send_far(z, 1)
            return
        pl.semaphore_wait(ready.at[j - 2], n_z)
        if j < n_out - 1:
            signal_z(ready.at[j - 1], (c,))
        send_distance(j)

    for op in RS:
        i = int(op[1:] or 0) if op != "bar" and op != "mv" else 0
        zt = order[i - 1]
        if op == "bar":
            pl.semaphore_wait(barrier, 5 + 2 * n_z)
            signal_z(ready.at[0], (c,))
        elif op == "mv":
            bounds()
            for j, ref in enumerate((m_in, v_in)):
                window(j, ref)
            wrow[...] = as_row(squares(lambda t: mv[t, 0], 0, span, own_low, own_high), 0)
        elif op[0] == "k":
            pack(i)
        elif op[0] == "A":
            send_raw(zt, 0)
        elif op[0] == "B":
            send_raw(zt, 1)
        elif op[0] == "z":
            step_z(i)
        elif op[0] == "Z":
            sum_far()
        elif op[0] == "s":
            sum_raw(zt)
        elif op[0] == "p":
            sum_plane(zt, i < n_out)

    landed(recv3.at[pl.ds(0, n_out - 1)], got3)
    halo_copy = remote(mv.at[span - 1], halo, halo_sem.at[0], halo_sem.at[1], dev((d + 1) % n))
    halo_copy.start()
    landed(rz2, gotz2)
    for t in range(hz):
        acc = zs[x * 2 + y, t] + rz2[0, t]
        grad_buf[hxy + t] = (acc + (rz2[1, t] + rz2[2, t])) / n
    grad_buf[step] = jnp.zeros((8, 128), jnp.float32)

    @pl.when(d == n - 1)
    def _():
        landed(re2, got_e2)
        grad_buf[step] = (ze[0] + re2[0] + (re2[1] + re2[2])) / n

    def total_grad(t):
        acc = part[z, t]
        for k in range(1, n_out):
            acc = acc + recv3[(z + k) % n_out, t]
        acc = acc / n
        grad_buf[t] = acc
        return acc

    sums = squares(total_grad, 0, hxy, low, high)
    sums = squares(lambda t: grad_buf[t], hxy, span, low, high, sums)
    stats[d] = as_row(sums, layers) + wrow[...]

    for k in range(n_out - 1, -1, -1):
        for q in range(plane - 1, -1, -1):
            if k + q > 0:
                peer = flip(z, k) * plane + flip(p, q)
                remote(stats.at[d], stats.at[d], send_s, got_s, dev(peer)).start()

    skip_row = jnp.zeros((1, 128), jnp.float32)
    for l in range(layers):
        skip_row = jnp.where(lane1 == l, skip_ref[l].astype(jnp.float32), skip_row)

    def prepare(t):
        pos = place + t * TILE
        which = jnp.zeros((8, 128), jnp.int32)
        decay = jnp.zeros((8, 128), jnp.float32)
        for l in range(layers):
            inside = (pos >= low[l]) & (pos < high[l])
            which = jnp.where(inside, l, which)
            decay = jnp.where(inside, (1.0 - skip_ref[l].astype(jnp.float32)) * 0.001, decay)
        layer_of[t] = which
        nvw_pre[t] = 0.9 * mv[t, 1]
        step_pre[t] = 8.0 * (grad_buf[t] + decay * mv[t, 0])

    @pl.loop(1, span)
    def _(t):
        prepare(t)

    halo_copy.wait()
    for j in range(2):
        mv[0, j] = jnp.where(place < off, halo[j], mv[0, j])
    prepare(0)

    landed(stats.at[pl.ds(0, n - 1)], got_s)
    norms = jnp.sqrt(jnp.sum(stats[...], axis=0))
    wnorm = jnp.broadcast_to(norms, (8, 128))
    gnorm = pltpu.roll(wnorm, 128 - layers, 1)
    ratio = 0.02 * wnorm / (gnorm + 0.001 * wnorm + 1e-06)
    trust_row = skip_row + (1.0 - skip_row) * ratio
    trust = [
        jnp.sum(jnp.where(lane1 == l, trust_row, 0.0), axis=1, keepdims=True)
        for l in range(layers)
    ]

    def update(t):
        which = layer_of[t]
        trust_pos = jnp.broadcast_to(trust[0], (8, 128))
        for l in range(1, layers):
            trust_pos = jnp.where(which == l, trust[l], trust_pos)
        nv = nvw_pre[t] + trust_pos * step_pre[t]
        nm = mv[t, 0] - nv
        nvw[t] = nv
        nmw[t] = nm
        return nm.astype(jnp.bfloat16)

    x_side = at(z, 1 - x, c, y)
    y_side = at(z, x, c, 1 - y)
    across = at(z, 1 - x, c, 1 - y)
    partner = at(z, x, 1 - c, y)

    def share(b):
        return ags.at[b, pl.ds(main, SHARE)]

    for t in range(main, step):
        ags[d, t] = update(t)
    for device in (across, x_side, y_side):
        remote(share(d), share(d), send_g, got_in, device).start()

    @pl.loop(0, main)
    def _(t):
        ags[d, t] = update(t)

    def send_edge():
        for i, ref in enumerate((nmw, nvw)):
            remote(ref.at[0], ref.at[step], back_sem.at[i], back_sem.at[2 + i], dev(d - 1)).start()

    def block(zz, xx, cc, yy):
        return zz * plane + xx * 4 + cc * 2 + yy

    def forward(b, device, lo=0, size=main):
        piece = ags.at[b, pl.ds(lo, size)]
        remote(piece, piece, send4, got4.at[b], device).start()

    def arrived(b):
        landed(ags.at[b, pl.ds(0, main)], got4.at[b])

    zone = {"m": flip(z, 1), "n": 2 - h, "f": 3 - 3 * h}
    visits = [z] + [zone[k] for k in VISIT]
    sends = [zone[k] for k in ZSEND]

    def tiles(count):
        return ags.at[pl.ds(0, count), pl.ds(0, SHARE)]

    def z_share():
        landed(tiles(3), got_in)
        for j in range(4):
            b = block(z, j // 2, c, j % 2)
            for to in sends:
                peer = at(to, x, c, y)
                remote(share(b), share(b), send_g, got_gz.at[z], peer).start()
            remote(share(b), share(b), send_g, got_gc, partner).start()

    def z_arrived(k):
        landed(tiles(4), got_gz.at[visits[k]])
        for j in range(4):
            b = block(visits[k], j // 2, c, j % 2)
            remote(share(b), share(b), send_g, got_gc, partner).start()

    for to in sends:
        forward(d, at(to, x, c, y))

    def column(k):
        b = block(visits[k], x, c, y)
        if k > 0:
            arrived(b)
        for way in COLUMN:
            if way == "x":
                forward(b, x_side)
            elif way == "y":
                forward(b, y_side)
            elif way == "p":
                forward(b, partner)
            elif k in DIRECT:
                forward(b, across)

    def from_y(k):
        b = block(visits[k], x, c, 1 - y)
        arrived(b)
        if k not in DIRECT:
            forward(b, x_side, 0, half_a)
        forward(b, partner)

    def from_x(k):
        b = block(visits[k], 1 - x, c, y)
        arrived(b)
        if k not in DIRECT:
            forward(b, y_side, half_a, half_b)
        forward(b, partner)

    def corner(k):
        b = block(visits[k], 1 - x, c, 1 - y)
        arrived(b)
        forward(b, partner)

    def edges():
        @pl.when(d > 0)
        def _():
            send_edge()

        @pl.when(d == n - 1)
        def _():
            age[0] = update(step)
            for q in range(1, n):
                remote(age, age, send_e, got_e, dev(d - q)).start()

    def own_rows():
        @pl.when(d < n - 1)
        def _():
            for i, ref in enumerate((nmw, nvw)):
                landed(ref.at[step], back_sem.at[2 + i])

        back_l = 128 - shift_l
        for src, buf in ((nmw, nm_out), (nvw, nv_out)):
            w = src[...].reshape(rows, 128)
            w = pltpu.roll(w, (rows - shift_r) % rows, 0)
            w = pltpu.roll(w, back_l % 128, 1)
            w = jnp.where(lane < back_l, w, pltpu.roll(w, rows - 1, 0))
            buf[pl.ds(0, whole)] = w[: step * 8].reshape(whole)
            buf[pl.ds(whole, shard - whole)] = w[step * 8, : shard - whole].reshape(shard - whole)

    for op in AG:
        i = int(op[1:])
        if op[0] == "c":
            column(i)
        elif op[0] == "x":
            from_x(i)
        elif op[0] == "y":
            from_y(i)
        elif op[0] == "d":
            corner(i)
        elif op[0] == "g":
            z_share()
        elif op[0] == "h":
            z_arrived(i)
        elif op[0] == "e":
            edges()
        elif op[0] == "n":
            own_rows()

    @pl.loop(0, n_out)
    def _(k):
        for xx in range(2):
            for yy in range(2):
                arrived(block(k, xx, 1 - c, yy))

    landed(tiles(4 * n_out), got_gc)

    @pl.when(d < n - 1)
    def _():
        landed(age, got_e)

    @pl.when(d == n - 1)
    def _():
        landed(ags.at[pl.ds(0, n - 1), 0], send_e)

    @pl.when(d > 0)
    def _():
        for i, ref in enumerate((nmw, nvw)):
            landed(ref.at[step], back_sem.at[i])

    @pl.when((z != last) | (c != 1))
    def _():
        landed(re1.at[pl.ds(0, 1)], send_e1)

    @pl.when((z == last) & (c == 1) & (x * 2 + y < 3))
    def _():
        landed(ze, send_e2)

    for ref, sem in (
        (r1x, send1x),
        (r1y, send1y),
        (r2x, send2x),
        (r2y, send2y),
        (rz1.at[pl.ds(0, 2 * n_out - 1)], sendz1),
        (rz2, sendz2),
        (recv3.at[pl.ds(0, n_out - 1)], send3),
        (stats.at[pl.ds(0, n - 1)], send_s),
        (ags.at[pl.ds(0, n - 1), pl.ds(0, main)], send4),
        (tiles(n - 1), send_g),
    ):
        landed(ref, sem)


def finish(plan, ags, age, nm, nv, out_ref, nm_ref, nv_ref, sem):
    part, last = plan
    copies = [
        (ags.at[pl.ds(i * part, part)], out_ref.at[pl.ds(i * part, part)]) for i in range(PIECES)
    ]
    copies += [(nm, nm_ref), (nv, nv_ref), (age, out_ref.at[pl.ds(last, 1)])]
    copies = [
        pltpu.make_async_copy(src, dst, sem.at[i]) for i, (src, dst) in enumerate(copies)
    ]
    for copy in copies:
        copy.start()
    for copy in copies:
        copy.wait()


def windowed(n_rep, n_spa, grads, master, velocity, layer_offsets, layer_sizes, lars_skip):
    shard = master.shape[0]
    params = grads.shape[2]
    layers = layer_offsets.shape[0]
    plane = 8
    n = n_rep * n_spa
    n_out = n // plane
    step = shard // TILE
    span = params // TILE - (n - 1) * step
    chunk = (plane - 1) * step + span
    tiles = params // TILE
    hz = ZTILES
    hx = (step - hz + 1) // 2
    hy = step - hz - hx
    plan = (n_out, shard, step, span, layers, hx, hy, hz)
    vmem = pl.BlockSpec(memory_space=pltpu.VMEM)
    anywhere = pl.BlockSpec(memory_space=pltpu.HBM)
    f32, bf16 = jnp.float32, jnp.bfloat16
    dma = pltpu.SemaphoreType.DMA
    ags, age, nmw, nvw = pl.pallas_call(
        functools.partial(kernel, plan),
        out_shape=(
            pltpu.VMEM((n, step, 8, 128), bf16),
            pltpu.VMEM((1, 8, 128), bf16),
            pltpu.VMEM((shard,), f32),
            pltpu.VMEM((shard,), f32),
        ),
        in_specs=[anywhere] * 6,
        out_specs=(vmem,) * 4,
        scratch_shapes=[
            pltpu.VMEM((span, 8, 128), f32),
            pltpu.VMEM((span, 8, 128), f32),
            pltpu.SMEM((layers,), jnp.int32),
            pltpu.SMEM((layers,), jnp.int32),
            pltpu.SMEM((layers,), jnp.int32),
            pltpu.VMEM((shard,), f32),
            pltpu.VMEM((shard,), f32),
            pltpu.VMEM((n_out, 1, chunk * TILE), bf16),
            pltpu.VMEM((n_out, chunk, 8, 128), bf16),
            pltpu.VMEM((2, n_out, 3, hx, 8, 128), bf16),
            pltpu.VMEM((2, n_out, 3, hy, 8, 128), bf16),
            pltpu.VMEM((n_out, hx, 8, 128), f32),
            pltpu.VMEM((n_out, hy, 8, 128), f32),
            pltpu.VMEM((n_out, hx, 8, 128), f32),
            pltpu.VMEM((n_out, hy, 8, 128), f32),
            pltpu.VMEM((2 * n_out, 4, hz, 8, 128), bf16),
            pltpu.VMEM((4, hz, 8, 128), f32),
            pltpu.VMEM((3, hz, 8, 128), f32),
            pltpu.VMEM((2 * n_out, 8, 128), bf16),
            pltpu.VMEM((1, 8, 128), f32),
            pltpu.VMEM((3, 8, 128), f32),
            pltpu.VMEM((n_out, hx + hy, 8, 128), f32),
            pltpu.VMEM((n_out, hx + hy, 8, 128), f32),
            pltpu.VMEM((span, 2, 8, 128), f32),
            pltpu.VMEM((2, 8, 128), f32),
            pltpu.VMEM((span, 8, 128), f32),
            pltpu.VMEM((span, 8, 128), jnp.int32),
            pltpu.VMEM((span, 8, 128), f32),
            pltpu.VMEM((span, 8, 128), f32),
            pltpu.VMEM((1, 128), f32),
            pltpu.VMEM((n, 1, 128), f32),
            dma((n_out,)),
            dma((2,)),
            dma((3,)),
            pltpu.SemaphoreType.REGULAR((n_out,)),
            dma(()),
            dma((2, n_out)),
            dma(()),
            dma((2, n_out)),
            dma(()),
            dma((n_out,)),
            dma(()),
            dma((n_out,)),
            dma(()),
            dma(()),
            dma(()),
            dma(()),
            dma(()),
            dma(()),
            dma(()),
            dma(()),
            dma(()),
            dma(()),
            dma((2,)),
            dma(()),
            dma(()),
            dma(()),
            dma((n,)),
            dma(()),
            dma(()),
            dma((n_out,)),
            dma(()),
            dma(()),
            dma(()),
            dma((4,)),
        ],
        compiler_params=pltpu.CompilerParams(
            collective_id=0, has_side_effects=True, vmem_limit_bytes=61 * 2**20
        ),
    )(grads, master, velocity, layer_offsets, layer_sizes, lars_skip)
    weights, nm, nv = pl.pallas_call(
        functools.partial(finish, (n * step // PIECES, n * step)),
        out_shape=(
            jax.ShapeDtypeStruct((tiles, 8, 128), bf16),
            jax.ShapeDtypeStruct((shard,), f32),
            jax.ShapeDtypeStruct((shard,), f32),
        ),
        in_specs=[vmem] * 4,
        out_specs=(anywhere, anywhere, anywhere),
        scratch_shapes=[
            dma((PIECES + 3,)),
        ],
        compiler_params=pltpu.CompilerParams(vmem_limit_bytes=16 * 2**20),
    )(ags.reshape(n * step, 8, 128), age, nmw, nvw)
    return weights.reshape(params), nm, nv


def tiled(n_rep, n_spa, params, layers):
    n = n_rep * n_spa
    shard = params // n
    rest = shard % TILE
    n_out = n_rep // 4
    return (
        n_spa == 2
        and n_rep % 4 == 0
        and n_out == 4
        and layers <= 8
        and params % TILE == 0
        and shard >= TILE
        and 0 < n * rest <= TILE
        and rest <= 128
    )


def step_fn(n_rep, n_spa, grads, *rest):
    if tiled(n_rep, n_spa, grads.shape[2], rest[2].shape[0]):
        return windowed(n_rep, n_spa, grads, *rest)
    return shards(grads, *rest)


def shards(grads, master, velocity, layer_offsets, layer_sizes, lars_skip):
    n_rep = lax.axis_size("replica")
    n_spa = lax.axis_size("spatial")
    shard = master.shape[0]
    position = lax.axis_index(("replica", "spatial")) * shard + jnp.arange(shard, dtype=jnp.int32)
    inside = (position[None, :] >= layer_offsets[:, None]) & (
        position[None, :] < (layer_offsets + layer_sizes)[:, None]
    )
    onehot = inside.astype(jnp.float32)
    received = lax.all_to_all(
        grads[0, 0].reshape(n_rep, n_spa * shard),
        "replica",
        split_axis=0,
        concat_axis=0,
        tiled=True,
    )
    first = jnp.sum(received.astype(jnp.float32), axis=0)
    summed = lax.psum_scatter(
        first.reshape(n_spa, shard), "spatial", scatter_dimension=0, tiled=True
    )
    grad = summed.reshape(shard) / (n_rep * n_spa)
    gsq_local = jnp.dot(onehot, grad * grad, precision=lax.Precision.HIGHEST)
    wsq_local = jnp.dot(onehot, master * master, precision=lax.Precision.HIGHEST)
    wsq, gsq = lax.psum((wsq_local, gsq_local), ("replica", "spatial"))
    wnorm = jnp.sqrt(wsq)
    gnorm = jnp.sqrt(gsq)
    skipped = lars_skip.astype(jnp.float32)
    ratio = 0.02 * wnorm / (gnorm + 0.001 * wnorm + 1e-06)
    trust = skipped + (1.0 - skipped) * ratio
    decay = (1.0 - skipped) * 0.001
    trust_pos = jnp.dot(trust, onehot, precision=lax.Precision.HIGHEST)
    decay_pos = jnp.dot(decay, onehot, precision=lax.Precision.HIGHEST)
    new_velocity = 0.9 * velocity + 8.0 * trust_pos * (grad + decay_pos * master)
    new_master = master - new_velocity
    new_weights = lax.all_gather(
        new_master.astype(jnp.bfloat16), ("replica", "spatial"), axis=0, tiled=True
    )
    return (new_weights, new_master, new_velocity)


def solution(mesh):
    return jax.shard_map(
        functools.partial(step_fn, mesh.shape["replica"], mesh.shape["spatial"]),
        mesh=mesh,
        in_specs=(
            P("replica", "spatial", None),
            P(("replica", "spatial")),
            P(("replica", "spatial")),
            P(),
            P(),
            P(),
        ),
        out_specs=(P(), P(("replica", "spatial")), P(("replica", "spatial"))),
        check_vma=False,
    )
```
